32 devices in a mesh: traj: 8 (over z, core), amp: 4 (over y, x).
Axes of the slice: x: 2, y: 2, z: 4, core: 2. Of those that a mesh axis runs over, the one named last changes fastest.
Arguments:
- amplitudes: float32 [8, 2, 524288], P('traj', None, 'amp'), parts along dimension 0, may hold values from -6 to 6
- couplings: float32 [18], replicated, may hold values from 0.5 to 2
- fields: float32 [19], replicated, may hold values from 0.5 to 2
- decays: float32 [19], replicated, may hold values from 0.2 to 2
- channel: int32 [8], P('traj'), parts along dimension 0, may hold values from 0 to 19
Outputs:
- evolved_state: float32 [8, 2, 524288], P('traj', None, 'amp'), parts along dimension 0
The draws below stay inside these ranges and needn't reach their ends.
There are 8 independent parts, one for each index of `traj`. The reference program is written for one: setup_inputs(seed, part) draws one part's arguments, and reference() takes and returns one part's arrays. A program takes and returns all parts, laid end to end along the dimension named above; an argument that names none is the same for every part. Nothing has to cross between parts.
Inputs may be any that keep to these rules, and one draw needn't show every extreme that they name: `channel`: the value 19 means that the trajectory does not jump.
All inputs are finite; a program needn't handle non-finite values.
Results may differ from the reference program's by a relative error of at most 0.0003.
Values sent between devices are 32-bit elements; how exact they have to be, the bound alone decides.
A program may use at most 256 MiB of HBM per device.

```python
import math
import jax
import jax.numpy as jnp
from jax import lax

SPINS = 19
KRYLOV = 8
TRAJ = 1
AMPS = 524288


def steps_of(rng, dims, cuts, smallest, largest):
    def one(dim, shards_of):
        steps = jax.random.uniform(jax.random.fold_in(jax.random.fold_in(rng, 6), dim), (shards_of,), jnp.float32, smallest / len(cuts), largest / len(cuts))
        return jnp.repeat(jnp.exp(steps), dims[dim] // shards_of).reshape((-1,) + (1,) * (len(dims) - dim - 1))

    factor_of = one(*cuts[0])
    for cut in cuts[1:]:
        factor_of = factor_of * one(*cut)
    return factor_of


def noise(stream_key, dims, deviation, most, pieces=(), kind=jnp.bfloat16):
    drawn = jax.random.normal(stream_key, dims, jnp.float32) * deviation
    if len(pieces) > 0:
        drawn = steps_of(stream_key, dims, pieces, -0.22, 0.18) * drawn
    return jnp.clip(drawn, min=-most, max=most).astype(kind)


def setup_inputs(seed: int = 0, part: int = 0) -> dict:
    streams_of = jax.random.split(jax.random.key(seed), 6)
    own_keys = jax.random.split(jax.random.fold_in(streams_of[5], part), 6)
    amplitudes = noise(own_keys[0], (TRAJ, 2, AMPS), 1.0, 6.0, ((2, 4),), jnp.float32)
    couplings = jnp.clip(jnp.exp(jax.random.uniform(streams_of[1], (SPINS - 1,), jnp.float32, math.log(0.5), math.log(2.0))), 0.5, 2.0)
    fields = jnp.clip(jnp.exp(jax.random.uniform(streams_of[2], (SPINS,), jnp.float32, math.log(0.5), math.log(2.0))), 0.5, 2.0)
    decays = jnp.clip(jnp.exp(jax.random.uniform(streams_of[3], (SPINS,), jnp.float32, math.log(0.2), math.log(2.0))), 0.2, 2.0)
    channel = jax.random.randint(own_keys[4], (TRAJ,), 0, SPINS + 1).astype(jnp.int32)
    return dict(amplitudes=amplitudes, couplings=couplings, fields=fields, decays=decays, channel=channel)


time_step = 0.7
squarings = 8
taylor_order = 10
highest = lax.Precision.HIGHEST

def flip_spin(vector, spin_pos):
    leading = vector.shape[:-1]
    length = vector.shape[-1]
    parted = vector.reshape(leading + (length >> spin_pos + 1, 2, 1 << spin_pos))
    return jnp.flip(parted, axis=len(leading) + 1).reshape(vector.shape)

def apply_heff(vector, fields, diag_real, diag_imag):
    flipped = jnp.zeros_like(vector)
    for spin_pos in range(SPINS):
        flipped = flipped + fields[spin_pos] * flip_spin(vector, spin_pos)
    real_part = vector[:, 0]
    imag_part = vector[:, 1]
    out_real = diag_real * real_part - diag_imag * imag_part - flipped[:, 0]
    out_imag = diag_real * imag_part + diag_imag * real_part - flipped[:, 1]
    return jnp.stack([out_real, out_imag], axis=1)

def krylov_weights(scale_norm, hess_real, hess_imag):
    a_real = time_step * hess_imag
    a_imag = -time_step * hess_real
    upper_half = jnp.concatenate([a_real, -a_imag], axis=2)
    lower_half = jnp.concatenate([a_imag, a_real], axis=2)
    scaled = jnp.concatenate([upper_half, lower_half], axis=1) / 2.0 ** squarings
    identity = jnp.broadcast_to(jnp.eye(2 * KRYLOV, dtype=jnp.float32), scaled.shape)
    series = identity
    for degree in range(taylor_order, 0, -1):
        series = identity + jnp.einsum('tij,tjk->tik', scaled, series, precision=highest) / degree
    for repeat in range(squarings):
        series = jnp.einsum('tij,tjk->tik', series, series, precision=highest)
    first_column = series[:, :, 0] * scale_norm[:, None]
    return (first_column[:, :KRYLOV], first_column[:, KRYLOV:])

def reference(amplitudes, couplings, fields, decays, channel):
    traj_count = amplitudes.shape[0]
    position = jnp.arange(AMPS, dtype=jnp.int32)
    occupation = [(position >> spin_pos & 1).astype(jnp.float32) for spin_pos in range(SPINS)]
    diag_real = jnp.zeros((AMPS,), jnp.float32)
    for spin_pos in range(SPINS - 1):
        diag_real = diag_real - couplings[spin_pos] * (1.0 - 2.0 * occupation[spin_pos]) * (1.0 - 2.0 * occupation[spin_pos + 1])
    diag_imag = jnp.zeros((AMPS,), jnp.float32)
    for spin_pos in range(SPINS):
        diag_imag = diag_imag - 0.5 * decays[spin_pos] * occupation[spin_pos]
    scale_norm = jnp.sqrt(lax.optimization_barrier(jnp.sum(amplitudes * amplitudes, axis=(1, 2))))
    krylov_basis = [amplitudes / scale_norm[:, None, None]]
    hess_real = jnp.zeros((traj_count, KRYLOV, KRYLOV), jnp.float32)
    hess_imag = jnp.zeros((traj_count, KRYLOV, KRYLOV), jnp.float32)
    for column in range(KRYLOV):
        applied = apply_heff(krylov_basis[column], fields, diag_real, diag_imag)
        stacked = jnp.stack(krylov_basis, axis=1)
        swapped = jnp.stack([applied[:, 1], -applied[:, 0]], axis=1)
        proj_real = jnp.einsum('tkca,tca->tk', stacked, applied, precision=highest)
        proj_imag = jnp.einsum('tkca,tca->tk', stacked, swapped, precision=highest)
        hess_real = hess_real.at[:, :column + 1, column].set(proj_real)
        hess_imag = hess_imag.at[:, :column + 1, column].set(proj_imag)
        if column + 1 < KRYLOV:
            comb_real = jnp.einsum('tk,tka->ta', proj_real, stacked[:, :, 0], precision=highest) - jnp.einsum('tk,tka->ta', proj_imag, stacked[:, :, 1], precision=highest)
            comb_imag = jnp.einsum('tk,tka->ta', proj_real, stacked[:, :, 1], precision=highest) + jnp.einsum('tk,tka->ta', proj_imag, stacked[:, :, 0], precision=highest)
            residual = applied - jnp.stack([comb_real, comb_imag], axis=1)
            column_norm = jnp.sqrt(lax.optimization_barrier(jnp.sum(residual * residual, axis=(1, 2))))
            hess_real = hess_real.at[:, column + 1, column].set(column_norm)
            krylov_basis.append(residual / column_norm[:, None, None])
    weights_real, weights_imag = krylov_weights(scale_norm, hess_real, hess_imag)
    stacked = jnp.stack(krylov_basis, axis=1)
    new_real = jnp.einsum('tk,tka->ta', weights_real, stacked[:, :, 0], precision=highest) - jnp.einsum('tk,tka->ta', weights_imag, stacked[:, :, 1], precision=highest)
    new_imag = jnp.einsum('tk,tka->ta', weights_real, stacked[:, :, 1], precision=highest) + jnp.einsum('tk,tka->ta', weights_imag, stacked[:, :, 0], precision=highest)
    propagated = jnp.stack([new_real, new_imag], axis=1)
    lowered = jnp.zeros_like(propagated)
    for spin_pos in range(SPINS):
        vacant = occupation[spin_pos] == 0.0
        lowered_term = jnp.where(vacant[None, None, :], flip_spin(propagated, spin_pos), 0.0)
        lowered = jnp.where((channel == spin_pos)[:, None, None], lowered_term, lowered)
    jumped = channel < SPINS
    squared_sum = jnp.where(jumped, lax.optimization_barrier(jnp.sum(lowered * lowered, axis=(1, 2))), jnp.float32(AMPS))
    lowered = lowered * jnp.sqrt(AMPS / squared_sum)[:, None, None]
    return jnp.where(jumped[:, None, None], lowered, propagated)
```

```python
import jax
import jax.numpy as jnp
from jax import lax
from jax.experimental import pallas as pl
from jax.experimental.pallas import tpu as pltpu
from jax.sharding import PartitionSpec as P

SPINS = 19
KRYLOV = 8
LANES = 128
LANE_BITS = 7

time_step = 0.7
squarings = 8
taylor_order = 10
highest = lax.Precision.HIGHEST

CHUNK_BITS = 8
CHUNK = 1 << CHUNK_BITS
SUB = 32


def split(x):
    hi = x.astype(jnp.bfloat16)
    lo = (x - hi.astype(jnp.float32)).astype(jnp.bfloat16)
    return hi, lo


def dot(a, b):
    return jnp.dot(a, b, preferred_element_type=jnp.float32)


def fold(x):
    return jnp.sum(x.reshape(x.shape[0] // 8, 8, x.shape[1]), axis=0)


def scalar_sqrt(value):
    root = jnp.sqrt(jnp.full((8, LANES), value, jnp.float32))
    return jnp.max(root), jnp.max(1.0 / root)


def krylov_weights(a_matrix):
    size = a_matrix.shape[0]
    pad = jnp.zeros((LANES - size, LANES), jnp.float32)
    scaled = jnp.concatenate([a_matrix, pad], axis=0) * (1.0 / 2.0**squarings)
    rows = lax.broadcasted_iota(jnp.int32, (LANES, LANES), 0)
    cols = lax.broadcasted_iota(jnp.int32, (LANES, LANES), 1)
    identity = jnp.where(rows == cols, 1.0, 0.0).astype(jnp.float32)
    series = identity
    for degree in range(taylor_order, 0, -1):
        product = jnp.dot(
            scaled, series, precision=highest, preferred_element_type=jnp.float32
        )
        series = identity + product * (1.0 / degree)
    for repeat in range(squarings):
        series = jnp.dot(
            series, series, precision=highest, preferred_element_type=jnp.float32
        )
    return series


def kernel(
    channel_ref,
    couplings,
    fields,
    decays,
    state,
    out,
    basis,
    work,
    flips,
    row_table,
    lane_table,
    diag_low,
):
    node_count, _, block_rows, _ = state.shape
    rows = node_count * block_rows
    chunks = rows // CHUNK
    subs = CHUNK // SUB
    channel = channel_ref[0]
    device = lax.axis_index("amp")
    zero_tile = jnp.zeros((8, LANES), jnp.float32)
    per_block = block_rows // CHUNK

    table_shape = (CHUNK, CHUNK)
    crossed = lax.broadcasted_iota(jnp.int32, table_shape, 0)
    crossed = crossed ^ lax.broadcasted_iota(jnp.int32, table_shape, 1)
    for table, first_spin, bits in (
        (row_table, LANE_BITS, CHUNK_BITS),
        (lane_table, 0, LANE_BITS),
    ):
        value = jnp.zeros(table_shape, jnp.float32)
        for bit in range(bits):
            value = jnp.where(crossed == 1 << bit, fields[first_spin + bit], value)
        table[0], table[1] = split(value)

    low_shape = (CHUNK, LANES)
    low_pos = lax.broadcasted_iota(jnp.int32, low_shape, 0) * LANES
    low_pos = low_pos + lax.broadcasted_iota(jnp.int32, low_shape, 1)
    low_bits = LANE_BITS + CHUNK_BITS
    before = None
    low_real = jnp.zeros(low_shape, jnp.float32)
    low_imag = jnp.zeros(low_shape, jnp.float32)
    for spin in range(low_bits):
        occupied = (lax.shift_right_logical(low_pos, spin) & 1).astype(jnp.float32)
        sign = 1.0 - 2.0 * occupied
        low_imag = low_imag - 0.5 * decays[spin] * occupied
        if spin > 0:
            low_real = low_real - couplings[spin - 1] * (before * sign)
        before = sign
    diag_low[0] = low_real
    diag_low[1] = low_imag

    def high_diagonal(i):
        bits = [
            (lax.shift_right_logical(i, b) & 1).astype(jnp.float32)
            for b in range(SPINS - low_bits)
        ]
        signs = [1.0 - 2.0 * bit for bit in bits]
        real = jnp.float32(0.0)
        imag = jnp.float32(0.0)
        for b in range(len(bits)):
            imag = imag - 0.5 * decays[low_bits + b] * bits[b]
            if b > 0:
                real = real - couplings[low_bits + b - 1] * signs[b - 1] * signs[b]
        edge = couplings[low_bits - 1] * signs[0]
        return real - edge, real + edge, imag

    def start_norm(i, acc):
        node = i // per_block
        first = (i % per_block) * CHUNK
        for part in range(2):
            x = state[node, part, pl.ds(first, CHUNK), :]
            acc = acc + fold(x * x)
        return acc

    start_sq = jnp.sum(lax.fori_loop(0, chunks, start_norm, zero_tile))
    beta, inv_beta = scalar_sqrt(start_sq)

    def start_vector(i, carry):
        node = i // per_block
        first = (i % per_block) * CHUNK
        for part in range(2):
            basis[0, pl.ds(i * CHUNK, CHUNK), part * LANES : (part + 1) * LANES] = (
                state[node, part, pl.ds(first, CHUNK), :] * inv_beta
            )
        return carry

    lax.fori_loop(0, chunks, start_vector, 0)

    mat_rows = lax.broadcasted_iota(jnp.int32, (2 * KRYLOV, LANES), 0)
    mat_cols = lax.broadcasted_iota(jnp.int32, (2 * KRYLOV, LANES), 1)
    a_matrix = jnp.zeros((2 * KRYLOV, LANES), jnp.float32)

    def put(matrix, k, j, real, imag):
        a_real = time_step * imag
        a_imag = -time_step * real
        for r, c, value in (
            (k, j, a_real),
            (k, j + KRYLOV, -a_imag),
            (k + KRYLOV, j, a_imag),
            (k + KRYLOV, j + KRYLOV, a_real),
        ):
            matrix = jnp.where((mat_rows == r) & (mat_cols == c), value, matrix)
        return matrix

    high_fields = [
        fields[LANE_BITS + CHUNK_BITS + b] for b in range(SPINS - LANE_BITS - CHUNK_BITS)
    ]

    for j in range(KRYLOV):
        last = j + 1 == KRYLOV

        def apply_chunk(i, acc, j=j):
            base = pl.multiple_of(i * CHUNK, CHUNK)
            hi, lo = split(basis[j, pl.ds(base, CHUNK), :])
            flips[...] = (
                dot(row_table[0], hi)
                + dot(row_table[1], hi)
                + dot(row_table[0], lo)
                + dot(hi, lane_table[0])
                + dot(lo, lane_table[0])
                + dot(hi, lane_table[1])
            )
            acc = list(acc)
            real_vacant, real_occupied, imag_high = high_diagonal(i)
            for s in range(subs):
                here = pl.ds(base + s * SUB, SUB)
                x = basis[j, here, :]
                f = flips[s * SUB : (s + 1) * SUB, :]
                for b, field in enumerate(high_fields):
                    there = pl.multiple_of((i ^ (1 << b)) * CHUNK, CHUNK)
                    f = f + field * basis[j, pl.ds(there + s * SUB, SUB), :]
                part = slice(s * SUB, (s + 1) * SUB)
                dr = diag_low[0, part, :] + (real_vacant if s < subs // 2 else real_occupied)
                di = diag_low[1, part, :] + imag_high
                xr, xi = x[:, :LANES], x[:, LANES:]
                wr = dr * xr - di * xi - f[:, :LANES]
                wi = dr * xi + di * xr - f[:, LANES:]
                work[here, :LANES] = wr
                work[here, LANES:] = wi
                for k in range(j + 1):
                    vr = basis[k, here, :LANES]
                    vi = basis[k, here, LANES:]
                    acc[2 * k] = acc[2 * k] + fold(vr * wr + vi * wi)
                    acc[2 * k + 1] = acc[2 * k + 1] + fold(vr * wi - vi * wr)
                acc[-1] = acc[-1] + fold(wr * wr + wi * wi)
            return tuple(acc)

        sums = lax.fori_loop(0, chunks, apply_chunk, (zero_tile,) * (2 * j + 3))
        coeffs = [jnp.sum(t) for t in sums]
        for k in range(j + 1):
            a_matrix = put(a_matrix, k, j, coeffs[2 * k], coeffs[2 * k + 1])
        if last:
            break
        left = coeffs[-1]
        for value in coeffs[:-1]:
            left = left - value * value
        norm, inv_norm = scalar_sqrt(left)
        a_matrix = put(a_matrix, j + 1, j, norm, jnp.float32(0.0))

        def subtract_chunk(i, carry, j=j, coeffs=coeffs, inv_norm=inv_norm):
            base = pl.multiple_of(i * CHUNK, CHUNK)
            for s in range(subs):
                here = pl.ds(base + s * SUB, SUB)
                rr = work[here, :LANES]
                ri = work[here, LANES:]
                for k in range(j + 1):
                    vr = basis[k, here, :LANES]
                    vi = basis[k, here, LANES:]
                    hr, hm = coeffs[2 * k], coeffs[2 * k + 1]
                    rr = rr - (hr * vr - hm * vi)
                    ri = ri - (hr * vi + hm * vr)
                basis[j + 1, here, :LANES] = rr * inv_norm
                basis[j + 1, here, LANES:] = ri * inv_norm
            return carry

        lax.fori_loop(0, chunks, subtract_chunk, 0)

    series = krylov_weights(a_matrix)
    first = series[: 2 * KRYLOV, :] * beta
    weights = [
        jnp.sum(jnp.where((mat_rows == k) & (mat_cols == 0), first, 0.0))
        for k in range(2 * KRYLOV)
    ]
    sub_pos = lax.broadcasted_iota(jnp.int32, (SUB, LANES), 0) * LANES
    sub_pos = sub_pos + lax.broadcasted_iota(jnp.int32, (SUB, LANES), 1)

    def combine(i, acc):
        base = pl.multiple_of(i * CHUNK, CHUNK)
        for s in range(subs):
            here = pl.ds(base + s * SUB, SUB)
            pr = jnp.zeros((SUB, LANES), jnp.float32)
            pi = jnp.zeros((SUB, LANES), jnp.float32)
            for k in range(KRYLOV):
                vr = basis[k, here, :LANES]
                vi = basis[k, here, LANES:]
                cr, ci = weights[k], weights[k + KRYLOV]
                pr = pr + (cr * vr - ci * vi)
                pi = pi + (cr * vi + ci * vr)
            work[here, :LANES] = pr
            work[here, LANES:] = pi
            position = sub_pos + (base + s * SUB) * LANES
            occupied = lax.shift_right_logical(position, channel) & 1
            acc = acc + fold(jnp.where(occupied == 1, pr * pr + pi * pi, 0.0))
        return acc

    total = jnp.sum(lax.fori_loop(0, chunks, combine, zero_tile))
    jumped = channel < SPINS
    size = jnp.float32(rows * LANES)
    total = jnp.where(jumped, total, size)
    root = jnp.sqrt(size / jnp.full((8, LANES), total, jnp.float32))
    scale = jnp.max(root)
    in_lanes = channel < LANE_BITS
    lane_shift = jnp.where(in_lanes, lax.shift_left(1, channel), 0)
    row_shift = jnp.where(
        in_lanes | (channel >= SPINS),
        0,
        lax.shift_left(1, jnp.maximum(channel - LANE_BITS, 0)),
    )
    in_sublanes = row_shift < 8
    near = jnp.where(in_sublanes, row_shift, 0)
    far = jnp.where(in_sublanes, 0, row_shift)
    lane_turn = (LANES - lane_shift) % LANES
    row_turn = (SUB - near) % SUB

    def jump(i, carry):
        local = pl.multiple_of(i * SUB, SUB)
        base = device * block_rows + local
        source = pl.multiple_of(base + far, 8)
        position = sub_pos + base * LANES
        vacant = (lax.shift_right_logical(position, channel) & 1) == 0
        for part in range(2):
            x = work[pl.ds(source, SUB), part * LANES : (part + 1) * LANES]
            x = pltpu.roll(x, row_turn, 0)
            x = pltpu.roll(x, lane_turn, 1)
            out[part, pl.ds(local, SUB), :] = jnp.where(vacant, x * scale, 0.0)
        return carry

    lax.fori_loop(0, block_rows // SUB, jump, 0)


def gather_kernel(block, out, send_sem, recv_sem):
    me = lax.axis_index("amp")
    near = (me ^ 1, me ^ 2)
    barrier = pltpu.get_barrier_semaphore()
    for partner in near:
        pl.semaphore_signal(
            barrier, inc=1, device_id={"amp": partner}, device_id_type=pl.DeviceIdType.MESH
        )
    pl.semaphore_wait(barrier, 2)

    def copy(source, owner, part, axis, slot):
        return pltpu.make_async_remote_copy(
            src_ref=source,
            dst_ref=out.at[owner, part],
            send_sem=send_sem.at[slot],
            recv_sem=recv_sem.at[slot],
            device_id={"amp": near[axis]},
            device_id_type=pl.DeviceIdType.MESH,
        )

    direct = {}
    for turn in range(2):
        for axis in range(2):
            part = axis ^ turn
            direct[axis, part] = copy(block.at[part], me, part, axis, 2 * axis + part)
            direct[axis, part].start()
    out[me] = block[...]
    forwards = []
    for axis in range(2):
        direct[axis, axis].wait_recv()
        owner = near[axis]
        forward = copy(out.at[owner, axis], owner, axis, 1 - axis, 4 + axis)
        forward.start()
        forwards.append(forward)
    for axis in range(2):
        direct[axis, 1 - axis].wait_recv()
    for forward in forwards:
        forward.wait_recv()
    for sent in list(direct.values()) + forwards:
        sent.wait_send()


def gather(block):
    node_count = lax.axis_size("amp")
    if node_count != 4:
        return lax.all_gather(block, "amp")
    vmem = pl.BlockSpec(memory_space=pltpu.VMEM)
    return pl.pallas_call(
        gather_kernel,
        out_shape=jax.ShapeDtypeStruct((node_count,) + block.shape, block.dtype),
        in_specs=[vmem],
        out_specs=vmem,
        scratch_shapes=[pltpu.SemaphoreType.DMA((6,)), pltpu.SemaphoreType.DMA((6,))],
        compiler_params=pltpu.CompilerParams(collective_id=0, has_side_effects=True),
        name="gather",
    )(block)


def body(amplitudes, couplings, fields, decays, channel):
    node_count = lax.axis_size("amp")
    local_len = amplitudes.shape[2]
    block_rows = local_len // LANES
    rows = node_count * block_rows
    vmem = pl.BlockSpec(memory_space=pltpu.VMEM)
    smem = pl.BlockSpec(memory_space=pltpu.SMEM)
    call = pl.pallas_call(
        kernel,
        out_shape=jax.ShapeDtypeStruct((2, block_rows, LANES), jnp.float32),
        in_specs=[smem] * 4 + [vmem],
        out_specs=vmem,
        scratch_shapes=[
            pltpu.VMEM((KRYLOV, rows, 2 * LANES), jnp.float32),
            pltpu.VMEM((rows + rows // 2, 2 * LANES), jnp.float32),
            pltpu.VMEM((CHUNK, 2 * LANES), jnp.float32),
            pltpu.VMEM((2, CHUNK, CHUNK), jnp.bfloat16),
            pltpu.VMEM((2, CHUNK, CHUNK), jnp.bfloat16),
            pltpu.VMEM((2, CHUNK, LANES), jnp.float32),
        ],
        compiler_params=pltpu.CompilerParams(vmem_limit_bytes=62 * 1024 * 1024),
        name="trajectory",
    )
    results = []
    for t in range(amplitudes.shape[0]):
        block = amplitudes[t].reshape(2, block_rows, LANES)
        state = gather(block)
        results.append(call(channel[t : t + 1], couplings, fields, decays, state))
    return jnp.stack(results).reshape(amplitudes.shape)


BLOCK = 256
BLOCK_BITS = 8


def pair_kernel(
    channel_ref,
    couplings,
    fields,
    decays,
    block,
    pieces,
    scale_out,
    landing,
    basis,
    work,
    mate,
    flips_even,
    flips_odd,
    row_table,
    lane_table,
    diag_low,
    own_sums,
    other_sums,
    own_channel,
    other_channel,
    parcel,
    gather_send,
    gather_recv,
    sums_send,
    sums_recv,
    mate_send,
    mate_recv,
    channel_sem,
    parcel_send,
    parcel_recv,
    scale_sem,
):
    quarters = landing.shape[0]
    piece_rows = landing.shape[1]
    traj = lax.axis_index("traj")
    me = lax.axis_index("amp")
    core = traj & 1
    first_traj = traj - core
    held = (me ^ (me >> 1)) & 1
    stays = core == held
    split_spin = LANE_BITS + BLOCK_BITS + 1
    side_spin = split_spin - 1
    zero_tile = jnp.zeros((8, LANES), jnp.float32)
    tiles = [(s, side) for s in range(BLOCK // SUB) for side in range(2)]

    def device(core_index, chip):
        return {"traj": first_traj + core_index, "amp": chip}

    def remote(source, target, send, recv, where):
        return pltpu.make_async_remote_copy(
            src_ref=source,
            dst_ref=target,
            send_sem=send,
            recv_sem=recv,
            device_id=where,
            device_id_type=pl.DeviceIdType.MESH,
        )

    other = device(1 - core, me)
    barrier = pltpu.get_barrier_semaphore()
    for flip_core in range(2):
        for flip_chip in range(quarters):
            if flip_core or flip_chip:
                pl.semaphore_signal(
                    barrier,
                    inc=1,
                    device_id=device(core ^ flip_core, me ^ flip_chip),
                    device_id_type=pl.DeviceIdType.MESH,
                )
    own_channel[...] = jnp.full(own_channel.shape, channel_ref[0], jnp.int32)
    pl.semaphore_wait(barrier, 2 * quarters - 1)

    near_chip = me ^ (held ^ core)
    far_chip = near_chip ^ 3

    def piece(core_index, chip, slot):
        source = block.at[pl.ds(pl.multiple_of(core_index * piece_rows, piece_rows), piece_rows)]
        return remote(
            source,
            landing.at[me],
            gather_send.at[slot],
            gather_recv.at[me],
            device(core_index, chip),
        )

    sends = [piece(core, far_chip, 0), piece(1 - core, far_chip, 1), piece(1 - core, near_chip, 2)]
    for send in sends:
        send.start()

    @pl.when(jnp.logical_not(stays))
    def _():
        piece(core, near_chip, 3).start()

    channel_copy = remote(
        own_channel, other_channel, channel_sem.at[0], channel_sem.at[1], other
    )
    channel_copy.start()

    crossed = lax.broadcasted_iota(jnp.int32, (BLOCK, BLOCK), 0)
    crossed = crossed ^ lax.broadcasted_iota(jnp.int32, (BLOCK, BLOCK), 1)
    for table, spins, axis in (
        (row_table, [LANE_BITS + b for b in range(BLOCK_BITS)], 1),
        (lane_table, [*range(LANE_BITS), side_spin], 0),
    ):
        value = jnp.zeros((BLOCK, BLOCK), jnp.float32)
        for bit, spin in enumerate(spins):
            value = jnp.where(crossed == 1 << bit, fields[spin], value)
        hi, lo = split(value)
        table[...] = jnp.concatenate([hi, hi, lo], axis=axis)

    core_sign = (1 - 2 * core).astype(jnp.float32)
    for side in range(2):
        low_shape = (BLOCK, LANES)
        low_pos = lax.broadcasted_iota(jnp.int32, low_shape, 0) * LANES
        low_pos = low_pos + lax.broadcasted_iota(jnp.int32, low_shape, 1)
        side_sign = 1.0 - 2.0 * side
        low_real = jnp.zeros(low_shape, jnp.float32)
        low_imag = jnp.zeros(low_shape, jnp.float32)
        before = None
        for spin in range(side_spin):
            occupied = (lax.shift_right_logical(low_pos, spin) & 1).astype(jnp.float32)
            sign = 1.0 - 2.0 * occupied
            low_imag = low_imag - 0.5 * decays[spin] * occupied
            if spin > 0:
                low_real = low_real - couplings[spin - 1] * (before * sign)
            before = sign
        low_real = low_real - couplings[side_spin - 1] * side_sign * before
        low_real = low_real - couplings[side_spin] * side_sign * core_sign
        low_imag = low_imag - 0.5 * side * decays[side_spin]
        low_imag = low_imag - 0.5 * core.astype(jnp.float32) * decays[split_spin]
        diag_low[0, side] = low_real
        diag_low[1, side] = low_imag

    def high_diagonal(q):
        signs = [core_sign]
        real = jnp.float32(0.0)
        imag = jnp.float32(0.0)
        for b in range(SPINS - 1 - split_spin):
            bit = (lax.shift_right_logical(q, b) & 1).astype(jnp.float32)
            signs.append(1.0 - 2.0 * bit)
            imag = imag - 0.5 * decays[split_spin + 1 + b] * bit
            real = real - couplings[split_spin + b] * signs[b] * signs[b + 1]
        return real, imag

    def window(ref, lead, part, s, side):
        return ref.at[(*lead, part, pl.ds(s * SUB, SUB), pl.ds(side * LANES, LANES))]

    def total(values, slot):
        count = len(values)
        for k, value in enumerate(values):
            own_sums[slot, 8 * k : 8 * k + 8] = value
        copy = remote(
            own_sums.at[slot, pl.ds(0, 8 * count)],
            other_sums.at[slot, pl.ds(0, 8 * count)],
            sums_send.at[slot],
            sums_recv.at[slot],
            other,
        )
        copy.start()
        copy.wait()
        return [
            own_sums[slot, 8 * k : 8 * k + 8] + other_sums[slot, 8 * k : 8 * k + 8]
            for k in range(count)
        ]

    def mate_copy(j, q):
        return remote(basis.at[j, q], mate.at[q], mate_send.at[q], mate_recv.at[q], other)

    @pl.when(stays)
    def _():
        def keep(i, carry):
            rows = pl.multiple_of(i * SUB, SUB)
            landing[me, pl.ds(rows, SUB), :] = block[
                pl.ds(pl.multiple_of(core * piece_rows, piece_rows) + rows, SUB), :
            ]
            return carry

        lax.fori_loop(0, piece_rows // SUB, keep, 0)

    def arrival(chip):
        return remote(
            block.at[pl.ds(0, piece_rows)],
            landing.at[chip],
            gather_send.at[0],
            gather_recv.at[chip],
            other,
        )

    @pl.when(jnp.logical_not(stays))
    def _():
        arrival(me).wait_recv()

    start_sq = zero_tile
    for flip_chip in range(quarters):
        q = me ^ flip_chip
        if flip_chip:
            arrival(q).wait_recv()

        def start_norm(i, acc, q=q):
            x = landing[q, pl.ds(pl.multiple_of(i * 128, 128), 128), :]
            return acc + fold(x * x)

        start_sq = lax.fori_loop(0, piece_rows // 128, start_norm, start_sq)
    beta, inv_beta = scalar_sqrt(jnp.sum(total([start_sq], 1)[0]))

    def start_vector(q, carry):
        for s, side in tiles:
            for part in range(2):
                first = (side * BLOCK + s * SUB) * 2 + part
                x = landing[q, pl.ds(first, SUB, stride=2), :]
                window(basis, (0, q), part, s, side)[...] = x * inv_beta
        mate_copy(0, q).start()
        return carry

    lax.fori_loop(0, quarters, start_vector, 0)

    mat_rows = lax.broadcasted_iota(jnp.int32, (2 * KRYLOV, LANES), 0)
    mat_cols = lax.broadcasted_iota(jnp.int32, (2 * KRYLOV, LANES), 1)
    a_matrix = jnp.zeros((2 * KRYLOV, LANES), jnp.float32)

    def put(matrix, k, j, real, imag):
        a_real = time_step * imag
        a_imag = -time_step * real
        for r, c, value in (
            (k, j, a_real),
            (k, j + KRYLOV, -a_imag),
            (k + KRYLOV, j, a_imag),
            (k + KRYLOV, j + KRYLOV, a_real),
        ):
            matrix = jnp.where((mat_rows == r) & (mat_cols == c), value, matrix)
        return matrix

    high_fields = [fields[split_spin + 1 + b] for b in range(SPINS - 1 - split_spin)]
    split_field = fields[split_spin]

    for j in range(KRYLOV):
        last = j + 1 == KRYLOV

        def issue(q, flips, j=j):
            for part in range(2):
                hi, lo = split(basis[j, q, part])
                flips[part] = dot(
                    jnp.concatenate([row_table[...], hi, lo, hi], axis=1),
                    jnp.concatenate([hi, lo, hi, lane_table[...]], axis=0),
                )

        def consume(q, flips, acc, j=j):
            acc = list(acc)
            real_high, imag_high = high_diagonal(q)
            for s, side in tiles:
                x = [window(basis, (j, q), part, s, side)[...] for part in range(2)]
                f = [window(flips, (), part, s, side)[...] for part in range(2)]
                for part in range(2):
                    f[part] = f[part] + split_field * window(mate, (q,), part, s, side)[...]
                    for b, field in enumerate(high_fields):
                        f[part] = (
                            f[part]
                            + field * window(basis, (j, q ^ (1 << b)), part, s, side)[...]
                        )
                dr = window(diag_low, (0,), side, s, 0)[...] + real_high
                di = window(diag_low, (1,), side, s, 0)[...] + imag_high
                wr = dr * x[0] - di * x[1] - f[0]
                wi = dr * x[1] + di * x[0] - f[1]
                window(work, (q,), 0, s, side)[...] = wr
                window(work, (q,), 1, s, side)[...] = wi
                for k in range(j + 1):
                    vr = window(basis, (k, q), 0, s, side)[...]
                    vi = window(basis, (k, q), 1, s, side)[...]
                    acc[2 * k] = acc[2 * k] + fold(vr * wr + vi * wi)
                    acc[2 * k + 1] = acc[2 * k + 1] + fold(vr * wi - vi * wr)
                acc[-1] = acc[-1] + fold(wr * wr + wi * wi)
            return tuple(acc)

        def apply_pair(i, acc, j=j):
            even = 2 * i
            odd = even + 1
            mate_copy(j, even).wait()
            mate_copy(j, odd).wait()
            issue(odd, flips_odd)
            acc = consume(even, flips_even, acc)
            issue((even + 2) % quarters, flips_even)
            return consume(odd, flips_odd, acc)

        issue(0, flips_even)
        sums = lax.fori_loop(0, quarters // 2, apply_pair, (zero_tile,) * (2 * j + 3))
        coeffs = [jnp.sum(t) for t in total(sums, j % 2)]
        for k in range(j + 1):
            a_matrix = put(a_matrix, k, j, coeffs[2 * k], coeffs[2 * k + 1])
        if last:
            break
        left = coeffs[-1]
        for value in coeffs[:-1]:
            left = left - value * value
        norm, inv_norm = scalar_sqrt(left)
        a_matrix = put(a_matrix, j + 1, j, norm, jnp.float32(0.0))

        def subtract(q, carry, j=j, coeffs=coeffs, inv_norm=inv_norm):
            for s, side in tiles:
                rr = window(work, (q,), 0, s, side)[...]
                ri = window(work, (q,), 1, s, side)[...]
                for k in range(j + 1):
                    vr = window(basis, (k, q), 0, s, side)[...]
                    vi = window(basis, (k, q), 1, s, side)[...]
                    hr, hm = coeffs[2 * k], coeffs[2 * k + 1]
                    rr = rr - (hr * vr - hm * vi)
                    ri = ri - (hr * vi + hm * vr)
                window(basis, (j + 1, q), 0, s, side)[...] = rr * inv_norm
                window(basis, (j + 1, q), 1, s, side)[...] = ri * inv_norm
            mate_copy(j + 1, q).start()
            return carry

        lax.fori_loop(0, quarters, subtract, 0)

    series = krylov_weights(a_matrix)
    first = series[: 2 * KRYLOV, :] * beta
    weights = [
        jnp.sum(jnp.where((mat_rows == k) & (mat_cols == 0), first, 0.0))
        for k in range(2 * KRYLOV)
    ]
    channel_copy.wait()
    channel = jnp.where(stays, own_channel[...], other_channel[...])
    sub_pos = lax.broadcasted_iota(jnp.int32, (SUB, LANES), 0) * LANES
    sub_pos = sub_pos + lax.broadcasted_iota(jnp.int32, (SUB, LANES), 1)

    def combine(q, acc):
        high = (core << split_spin) + (q << (split_spin + 1))
        for s, side in tiles:
            pr = jnp.zeros((SUB, LANES), jnp.float32)
            pi = jnp.zeros((SUB, LANES), jnp.float32)
            for k in range(KRYLOV):
                vr = window(basis, (k, q), 0, s, side)[...]
                vi = window(basis, (k, q), 1, s, side)[...]
                cr, ci = weights[k], weights[k + KRYLOV]
                pr = pr + (cr * vr - ci * vi)
                pi = pi + (cr * vi + ci * vr)
            window(work, (q,), 0, s, side)[...] = pr
            window(work, (q,), 1, s, side)[...] = pi
            position = sub_pos + (high + (side << side_spin) + s * SUB * LANES)
            occupied = lax.shift_right_logical(position, channel) & 1
            acc = acc + fold(jnp.where(occupied == 1, pr * pr + pi * pi, 0.0))
        return acc

    jumped_sq = lax.fori_loop(0, quarters, combine, zero_tile)

    def pack(target, q, part):
        for s, side in tiles:
            value = window(work, (q,), part, s, side)[...]
            for b in range(SPINS - 1 - split_spin):
                flipped = window(work, (q | (1 << b),), part, s, side)[...]
                value = jnp.where(channel == split_spin + 1 + b, flipped, value)
            target[s * SUB : (s + 1) * SUB, side * LANES : (side + 1) * LANES] = value

    parcels = []
    for part in range(2):
        q = me ^ (1 << part)
        pack(parcel.at[part], q, part)
        copy = remote(
            parcel.at[part],
            pieces.at[core, part],
            parcel_send.at[part],
            parcel_recv.at[core, part],
            device(held, q),
        )
        copy.start()
        parcels.append(copy)
    for part in range(2):
        pack(parcel.at[2 + part], me, part)
    home = remote(
        parcel.at[pl.ds(2, 2)], pieces.at[core], parcel_send.at[2], parcel_recv.at[2, 0], other
    )

    @pl.when(jnp.logical_not(stays))
    def _():
        home.start()

    @pl.when(stays)
    def _():
        for part in range(2):
            pieces[core, part] = parcel[2 + part]

    all_sq = jnp.sum(total([jumped_sq], 0)[0])
    size = jnp.float32(quarters * 2 * piece_rows // 2 * LANES)
    ratio = jnp.where(channel[:8] < SPINS, size / jnp.full((8, LANES), all_sq, jnp.float32), 1.0)
    own_scale = jnp.sqrt(ratio)
    own_sums[1, 0:8] = own_scale
    scale_copy = remote(
        own_sums.at[1, pl.ds(0, 8)], scale_out, scale_sem.at[0], scale_sem.at[1],
        device(core, me ^ 1),
    )

    @pl.when(stays)
    def _():
        scale_copy.start()
        scale_out[...] = own_scale
        remote(
            parcel.at[pl.ds(2, 2)], pieces.at[1 - core], parcel_send.at[2],
            parcel_recv.at[2, 0], other,
        ).wait_recv()
        scale_copy.wait_send()

    @pl.when(jnp.logical_not(stays))
    def _():
        for sender in range(2):
            for part in range(2):
                remote(
                    parcel.at[part], pieces.at[sender, part], parcel_send.at[part],
                    parcel_recv.at[sender, part], other,
                ).wait_recv()
        scale_copy.wait_recv()
        home.wait_send()
        piece(core, near_chip, 3).wait_send()

    for copy in parcels:
        copy.wait_send()
    for send in sends:
        send.wait_send()


def lower_kernel(channel_ref, pieces, scale, out):
    channel = channel_ref[0]
    me = lax.axis_index("amp")
    side_spin = LANE_BITS + BLOCK_BITS
    in_lanes = channel < LANE_BITS
    in_rows = jnp.logical_not(in_lanes) & (channel < side_spin)
    lane_shift = jnp.where(in_lanes, lax.shift_left(1, channel), 0)
    row_shift = jnp.where(in_rows, lax.shift_left(1, jnp.maximum(channel - LANE_BITS, 0)), 0)
    near = jnp.where(row_shift < 8, row_shift, 0)
    far = jnp.where(row_shift < 8, 0, row_shift)
    lane_turn = (LANES - lane_shift) % LANES
    row_turn = (8 - near) % 8
    sub_pos = lax.broadcasted_iota(jnp.int32, (8, LANES), 0) * LANES
    sub_pos = sub_pos + lax.broadcasted_iota(jnp.int32, (8, LANES), 1)
    own = me * (4 * BLOCK * LANES)
    factor = scale[...]

    for half in range(2):
        from_half = jnp.where(channel == side_spin + 1, 1, half)
        for side in range(2):
            from_side = jnp.where(channel == side_spin, 1, side)
            columns = pl.ds(pl.multiple_of(from_side * LANES, LANES), LANES)

            def lower(i, carry, half=half, side=side, from_half=from_half, columns=columns):
                for t in range(8):
                    local = i * 64 + t * 8
                    base = (half * 2 + side) * BLOCK + local
                    rows = pl.ds(pl.multiple_of(local | far, 8), 8)
                    position = sub_pos + (own + base * LANES)
                    vacant = (lax.shift_right_logical(position, channel) & 1) == 0
                    for part in range(2):
                        x = pieces[from_half, part, rows, columns]
                        x = pltpu.roll(x, row_turn, 0)
                        x = pltpu.roll(x, lane_turn, 1)
                        x = jnp.where(vacant, x * factor, 0.0)
                        out[pl.ds(base * 2 + part, 8, stride=2), :] = x
                return carry

            lax.fori_loop(0, BLOCK // 64, lower, 0)


def paired_body(amplitudes, couplings, fields, decays, channel):
    quarters = lax.axis_size("amp")
    local_len = amplitudes.shape[2]
    block_rows = local_len // LANES
    vmem = pl.BlockSpec(memory_space=pltpu.VMEM)
    smem = pl.BlockSpec(memory_space=pltpu.SMEM)
    f32 = jnp.float32
    dma = pltpu.SemaphoreType.DMA
    sums_rows = 8 * (2 * KRYLOV + 1)
    state = amplitudes.reshape(2, block_rows, LANES).transpose(1, 0, 2)
    state = state.reshape(2 * block_rows, LANES)
    pieces, scale = pl.pallas_call(
        pair_kernel,
        out_shape=(
            jax.ShapeDtypeStruct((2, 2, BLOCK, BLOCK), f32),
            jax.ShapeDtypeStruct((8, LANES), f32),
        ),
        in_specs=[smem] * 4 + [vmem],
        out_specs=(vmem, vmem),
        scratch_shapes=[
            pltpu.VMEM((quarters, block_rows, LANES), f32),
            pltpu.VMEM((KRYLOV, quarters, 2, BLOCK, BLOCK), f32),
            pltpu.VMEM((quarters, 2, BLOCK, BLOCK), f32),
            pltpu.VMEM((quarters, 2, BLOCK, BLOCK), f32),
            pltpu.VMEM((2, BLOCK, BLOCK), f32),
            pltpu.VMEM((2, BLOCK, BLOCK), f32),
            pltpu.VMEM((BLOCK, 3 * BLOCK), jnp.bfloat16),
            pltpu.VMEM((3 * BLOCK, BLOCK), jnp.bfloat16),
            pltpu.VMEM((2, 2, BLOCK, LANES), f32),
            pltpu.VMEM((2, sums_rows, LANES), f32),
            pltpu.VMEM((2, sums_rows, LANES), f32),
            pltpu.VMEM((SUB, LANES), jnp.int32),
            pltpu.VMEM((SUB, LANES), jnp.int32),
            pltpu.VMEM((4, BLOCK, BLOCK), f32),
            dma((4,)),
            dma((quarters,)),
            dma((2,)),
            dma((2,)),
            dma((quarters,)),
            dma((quarters,)),
            dma((2,)),
            dma((3,)),
            dma((3, 2)),
            dma((2,)),
        ],
        compiler_params=pltpu.CompilerParams(
            collective_id=1, has_side_effects=True, vmem_limit_bytes=62 * 1024 * 1024
        ),
        name="pair",
    )(channel, couplings, fields, decays, state)
    lowered = pl.pallas_call(
        lower_kernel,
        out_shape=jax.ShapeDtypeStruct((2 * block_rows, LANES), f32),
        in_specs=[smem, vmem, vmem],
        out_specs=vmem,
        name="lower",
    )(channel, pieces, scale)
    lowered = lowered.reshape(block_rows, 2, LANES).transpose(1, 0, 2)
    return lowered.reshape(amplitudes.shape)


def solution(mesh):
    placed = (P("traj", None, "amp"), P(), P(), P(), P("traj"))

    def step(amplitudes, *rest):
        trajectories = mesh.shape["traj"]
        low_rows = amplitudes.shape[2] // mesh.shape["amp"] // LANES
        paired = (
            mesh.shape["amp"] == 4
            and trajectories % 2 == 0
            and amplitudes.shape[0] == trajectories
            and low_rows == 4 * BLOCK
        )
        return jax.shard_map(
            paired_body if paired else body,
            mesh=mesh,
            in_specs=placed,
            out_specs=P("traj", None, "amp"),
            check_vma=False,
        )(amplitudes, *rest)

    return step
```

```python
import math

import jax
import jax.numpy as jnp
from jax import lax
from jax.experimental import pallas as pl
from jax.experimental.pallas import tpu as pltpu
from jax.sharding import PartitionSpec as P

SPINS = 19
KRYLOV = 8
LANES = 128
LANE_BITS = 7

time_step = 0.7
squarings = 8
taylor_order = 10
highest = lax.Precision.HIGHEST

CHUNK_BITS = 8
CHUNK = 1 << CHUNK_BITS
SUB = 32


def split(x):
    hi = x.astype(jnp.bfloat16)
    lo = (x - hi.astype(jnp.float32)).astype(jnp.bfloat16)
    return hi, lo


def dot(a, b):
    return jnp.dot(a, b, preferred_element_type=jnp.float32)


def fold(x):
    return jnp.sum(x.reshape(x.shape[0] // 8, 8, x.shape[1]), axis=0)


def scalar_sqrt(value):
    root = jnp.sqrt(jnp.full((8, LANES), value, jnp.float32))
    return jnp.max(root), jnp.max(1.0 / root)


def krylov_weights(a_matrix):
    size = a_matrix.shape[0]
    pad = jnp.zeros((LANES - size, LANES), jnp.float32)
    scaled = jnp.concatenate([a_matrix, pad], axis=0) * (1.0 / 2.0**squarings)
    rows = lax.broadcasted_iota(jnp.int32, (LANES, LANES), 0)
    cols = lax.broadcasted_iota(jnp.int32, (LANES, LANES), 1)
    identity = jnp.where(rows == cols, 1.0, 0.0).astype(jnp.float32)
    series = identity
    for degree in range(taylor_order, 0, -1):
        product = jnp.dot(
            scaled, series, precision=highest, preferred_element_type=jnp.float32
        )
        series = identity + product * (1.0 / degree)
    for repeat in range(squarings):
        series = jnp.dot(
            series, series, precision=highest, preferred_element_type=jnp.float32
        )
    return series


def kernel(
    channel_ref,
    couplings,
    fields,
    decays,
    state,
    out,
    basis,
    work,
    flips,
    row_table,
    lane_table,
    diag_low,
):
    node_count, _, block_rows, _ = state.shape
    rows = node_count * block_rows
    chunks = rows // CHUNK
    subs = CHUNK // SUB
    channel = channel_ref[0]
    device = lax.axis_index("amp")
    zero_tile = jnp.zeros((8, LANES), jnp.float32)
    per_block = block_rows // CHUNK

    table_shape = (CHUNK, CHUNK)
    crossed = lax.broadcasted_iota(jnp.int32, table_shape, 0)
    crossed = crossed ^ lax.broadcasted_iota(jnp.int32, table_shape, 1)
    for table, first_spin, bits in (
        (row_table, LANE_BITS, CHUNK_BITS),
        (lane_table, 0, LANE_BITS),
    ):
        value = jnp.zeros(table_shape, jnp.float32)
        for bit in range(bits):
            value = jnp.where(crossed == 1 << bit, fields[first_spin + bit], value)
        table[0], table[1] = split(value)

    low_shape = (CHUNK, LANES)
    low_pos = lax.broadcasted_iota(jnp.int32, low_shape, 0) * LANES
    low_pos = low_pos + lax.broadcasted_iota(jnp.int32, low_shape, 1)
    low_bits = LANE_BITS + CHUNK_BITS
    before = None
    low_real = jnp.zeros(low_shape, jnp.float32)
    low_imag = jnp.zeros(low_shape, jnp.float32)
    for spin in range(low_bits):
        occupied = (lax.shift_right_logical(low_pos, spin) & 1).astype(jnp.float32)
        sign = 1.0 - 2.0 * occupied
        low_imag = low_imag - 0.5 * decays[spin] * occupied
        if spin > 0:
            low_real = low_real - couplings[spin - 1] * (before * sign)
        before = sign
    diag_low[0] = low_real
    diag_low[1] = low_imag

    def high_diagonal(i):
        bits = [
            (lax.shift_right_logical(i, b) & 1).astype(jnp.float32)
            for b in range(SPINS - low_bits)
        ]
        signs = [1.0 - 2.0 * bit for bit in bits]
        real = jnp.float32(0.0)
        imag = jnp.float32(0.0)
        for b in range(len(bits)):
            imag = imag - 0.5 * decays[low_bits + b] * bits[b]
            if b > 0:
                real = real - couplings[low_bits + b - 1] * signs[b - 1] * signs[b]
        edge = couplings[low_bits - 1] * signs[0]
        return real - edge, real + edge, imag

    def start_norm(i, acc):
        node = i // per_block
        first = (i % per_block) * CHUNK
        for part in range(2):
            x = state[node, part, pl.ds(first, CHUNK), :]
            acc = acc + fold(x * x)
        return acc

    start_sq = jnp.sum(lax.fori_loop(0, chunks, start_norm, zero_tile))
    beta, inv_beta = scalar_sqrt(start_sq)

    def start_vector(i, carry):
        node = i // per_block
        first = (i % per_block) * CHUNK
        for part in range(2):
            basis[0, pl.ds(i * CHUNK, CHUNK), part * LANES : (part + 1) * LANES] = (
                state[node, part, pl.ds(first, CHUNK), :] * inv_beta
            )
        return carry

    lax.fori_loop(0, chunks, start_vector, 0)

    mat_rows = lax.broadcasted_iota(jnp.int32, (2 * KRYLOV, LANES), 0)
    mat_cols = lax.broadcasted_iota(jnp.int32, (2 * KRYLOV, LANES), 1)
    a_matrix = jnp.zeros((2 * KRYLOV, LANES), jnp.float32)

    def put(matrix, k, j, real, imag):
        a_real = time_step * imag
        a_imag = -time_step * real
        for r, c, value in (
            (k, j, a_real),
            (k, j + KRYLOV, -a_imag),
            (k + KRYLOV, j, a_imag),
            (k + KRYLOV, j + KRYLOV, a_real),
        ):
            matrix = jnp.where((mat_rows == r) & (mat_cols == c), value, matrix)
        return matrix

    high_fields = [
        fields[LANE_BITS + CHUNK_BITS + b] for b in range(SPINS - LANE_BITS - CHUNK_BITS)
    ]

    for j in range(KRYLOV):
        last = j + 1 == KRYLOV

        def apply_chunk(i, acc, j=j):
            base = pl.multiple_of(i * CHUNK, CHUNK)
            hi, lo = split(basis[j, pl.ds(base, CHUNK), :])
            flips[...] = (
                dot(row_table[0], hi)
                + dot(row_table[1], hi)
                + dot(row_table[0], lo)
                + dot(hi, lane_table[0])
                + dot(lo, lane_table[0])
                + dot(hi, lane_table[1])
            )
            acc = list(acc)
            real_vacant, real_occupied, imag_high = high_diagonal(i)
            for s in range(subs):
                here = pl.ds(base + s * SUB, SUB)
                x = basis[j, here, :]
                f = flips[s * SUB : (s + 1) * SUB, :]
                for b, field in enumerate(high_fields):
                    there = pl.multiple_of((i ^ (1 << b)) * CHUNK, CHUNK)
                    f = f + field * basis[j, pl.ds(there + s * SUB, SUB), :]
                part = slice(s * SUB, (s + 1) * SUB)
                dr = diag_low[0, part, :] + (real_vacant if s < subs // 2 else real_occupied)
                di = diag_low[1, part, :] + imag_high
                xr, xi = x[:, :LANES], x[:, LANES:]
                wr = dr * xr - di * xi - f[:, :LANES]
                wi = dr * xi + di * xr - f[:, LANES:]
                work[here, :LANES] = wr
                work[here, LANES:] = wi
                for k in range(j + 1):
                    vr = basis[k, here, :LANES]
                    vi = basis[k, here, LANES:]
                    acc[2 * k] = acc[2 * k] + fold(vr * wr + vi * wi)
                    acc[2 * k + 1] = acc[2 * k + 1] + fold(vr * wi - vi * wr)
                acc[-1] = acc[-1] + fold(wr * wr + wi * wi)
            return tuple(acc)

        sums = lax.fori_loop(0, chunks, apply_chunk, (zero_tile,) * (2 * j + 3))
        coeffs = [jnp.sum(t) for t in sums]
        for k in range(j + 1):
            a_matrix = put(a_matrix, k, j, coeffs[2 * k], coeffs[2 * k + 1])
        if last:
            break
        left = coeffs[-1]
        for value in coeffs[:-1]:
            left = left - value * value
        norm, inv_norm = scalar_sqrt(left)
        a_matrix = put(a_matrix, j + 1, j, norm, jnp.float32(0.0))

        def subtract_chunk(i, carry, j=j, coeffs=coeffs, inv_norm=inv_norm):
            base = pl.multiple_of(i * CHUNK, CHUNK)
            for s in range(subs):
                here = pl.ds(base + s * SUB, SUB)
                rr = work[here, :LANES]
                ri = work[here, LANES:]
                for k in range(j + 1):
                    vr = basis[k, here, :LANES]
                    vi = basis[k, here, LANES:]
                    hr, hm = coeffs[2 * k], coeffs[2 * k + 1]
                    rr = rr - (hr * vr - hm * vi)
                    ri = ri - (hr * vi + hm * vr)
                basis[j + 1, here, :LANES] = rr * inv_norm
                basis[j + 1, here, LANES:] = ri * inv_norm
            return carry

        lax.fori_loop(0, chunks, subtract_chunk, 0)

    series = krylov_weights(a_matrix)
    first = series[: 2 * KRYLOV, :] * beta
    weights = [
        jnp.sum(jnp.where((mat_rows == k) & (mat_cols == 0), first, 0.0))
        for k in range(2 * KRYLOV)
    ]
    sub_pos = lax.broadcasted_iota(jnp.int32, (SUB, LANES), 0) * LANES
    sub_pos = sub_pos + lax.broadcasted_iota(jnp.int32, (SUB, LANES), 1)

    def combine(i, acc):
        base = pl.multiple_of(i * CHUNK, CHUNK)
        for s in range(subs):
            here = pl.ds(base + s * SUB, SUB)
            pr = jnp.zeros((SUB, LANES), jnp.float32)
            pi = jnp.zeros((SUB, LANES), jnp.float32)
            for k in range(KRYLOV):
                vr = basis[k, here, :LANES]
                vi = basis[k, here, LANES:]
                cr, ci = weights[k], weights[k + KRYLOV]
                pr = pr + (cr * vr - ci * vi)
                pi = pi + (cr * vi + ci * vr)
            work[here, :LANES] = pr
            work[here, LANES:] = pi
            position = sub_pos + (base + s * SUB) * LANES
            occupied = lax.shift_right_logical(position, channel) & 1
            acc = acc + fold(jnp.where(occupied == 1, pr * pr + pi * pi, 0.0))
        return acc

    total = jnp.sum(lax.fori_loop(0, chunks, combine, zero_tile))
    jumped = channel < SPINS
    size = jnp.float32(rows * LANES)
    total = jnp.where(jumped, total, size)
    root = jnp.sqrt(size / jnp.full((8, LANES), total, jnp.float32))
    scale = jnp.max(root)
    in_lanes = channel < LANE_BITS
    lane_shift = jnp.where(in_lanes, lax.shift_left(1, channel), 0)
    row_shift = jnp.where(
        in_lanes | (channel >= SPINS),
        0,
        lax.shift_left(1, jnp.maximum(channel - LANE_BITS, 0)),
    )
    in_sublanes = row_shift < 8
    near = jnp.where(in_sublanes, row_shift, 0)
    far = jnp.where(in_sublanes, 0, row_shift)
    lane_turn = (LANES - lane_shift) % LANES
    row_turn = (SUB - near) % SUB

    def jump(i, carry):
        local = pl.multiple_of(i * SUB, SUB)
        base = device * block_rows + local
        source = pl.multiple_of(base + far, 8)
        position = sub_pos + base * LANES
        vacant = (lax.shift_right_logical(position, channel) & 1) == 0
        for part in range(2):
            x = work[pl.ds(source, SUB), part * LANES : (part + 1) * LANES]
            x = pltpu.roll(x, row_turn, 0)
            x = pltpu.roll(x, lane_turn, 1)
            out[part, pl.ds(local, SUB), :] = jnp.where(vacant, x * scale, 0.0)
        return carry

    lax.fori_loop(0, block_rows // SUB, jump, 0)


def gather_kernel(block, out, send_sem, recv_sem):
    me = lax.axis_index("amp")
    near = (me ^ 1, me ^ 2)
    barrier = pltpu.get_barrier_semaphore()
    for partner in near:
        pl.semaphore_signal(
            barrier, inc=1, device_id={"amp": partner}, device_id_type=pl.DeviceIdType.MESH
        )
    pl.semaphore_wait(barrier, 2)

    def copy(source, owner, part, axis, slot):
        return pltpu.make_async_remote_copy(
            src_ref=source,
            dst_ref=out.at[owner, part],
            send_sem=send_sem.at[slot],
            recv_sem=recv_sem.at[slot],
            device_id={"amp": near[axis]},
            device_id_type=pl.DeviceIdType.MESH,
        )

    direct = {}
    for turn in range(2):
        for axis in range(2):
            part = axis ^ turn
            direct[axis, part] = copy(block.at[part], me, part, axis, 2 * axis + part)
            direct[axis, part].start()
    out[me] = block[...]
    forwards = []
    for axis in range(2):
        direct[axis, axis].wait_recv()
        owner = near[axis]
        forward = copy(out.at[owner, axis], owner, axis, 1 - axis, 4 + axis)
        forward.start()
        forwards.append(forward)
    for axis in range(2):
        direct[axis, 1 - axis].wait_recv()
    for forward in forwards:
        forward.wait_recv()
    for sent in list(direct.values()) + forwards:
        sent.wait_send()


def gather(block):
    node_count = lax.axis_size("amp")
    if node_count != 4:
        return lax.all_gather(block, "amp")
    vmem = pl.BlockSpec(memory_space=pltpu.VMEM)
    return pl.pallas_call(
        gather_kernel,
        out_shape=jax.ShapeDtypeStruct((node_count,) + block.shape, block.dtype),
        in_specs=[vmem],
        out_specs=vmem,
        scratch_shapes=[pltpu.SemaphoreType.DMA((6,)), pltpu.SemaphoreType.DMA((6,))],
        compiler_params=pltpu.CompilerParams(collective_id=0, has_side_effects=True),
        name="gather",
    )(block)


def body(amplitudes, couplings, fields, decays, channel):
    node_count = lax.axis_size("amp")
    local_len = amplitudes.shape[2]
    block_rows = local_len // LANES
    rows = node_count * block_rows
    vmem = pl.BlockSpec(memory_space=pltpu.VMEM)
    smem = pl.BlockSpec(memory_space=pltpu.SMEM)
    call = pl.pallas_call(
        kernel,
        out_shape=jax.ShapeDtypeStruct((2, block_rows, LANES), jnp.float32),
        in_specs=[smem] * 4 + [vmem],
        out_specs=vmem,
        scratch_shapes=[
            pltpu.VMEM((KRYLOV, rows, 2 * LANES), jnp.float32),
            pltpu.VMEM((rows + rows // 2, 2 * LANES), jnp.float32),
            pltpu.VMEM((CHUNK, 2 * LANES), jnp.float32),
            pltpu.VMEM((2, CHUNK, CHUNK), jnp.bfloat16),
            pltpu.VMEM((2, CHUNK, CHUNK), jnp.bfloat16),
            pltpu.VMEM((2, CHUNK, LANES), jnp.float32),
        ],
        compiler_params=pltpu.CompilerParams(vmem_limit_bytes=62 * 1024 * 1024),
        name="trajectory",
    )
    results = []
    for t in range(amplitudes.shape[0]):
        block = amplitudes[t].reshape(2, block_rows, LANES)
        state = gather(block)
        results.append(call(channel[t : t + 1], couplings, fields, decays, state))
    return jnp.stack(results).reshape(amplitudes.shape)


BLOCK = 256
BLOCK_BITS = 8


def pair_kernel(
    channel_ref,
    couplings,
    fields,
    decays,
    block,
    pieces,
    scale_out,
    landing,
    mate_landing,
    basis,
    mate,
    work,
    mate_work,
    flips_even,
    flips_odd,
    row_table,
    lane_table,
    diagonal,
    own_sums,
    other_sums,
    own_rest,
    other_rest,
    scalars,
    own_channel,
    other_channel,
    parcel,
    gather_send,
    gather_recv,
    forward_send,
    forward_recv,
    sums_send,
    sums_recv,
    rest_sem,
    work_send,
    work_recv,
    channel_sem,
    parcel_send,
    parcel_recv,
    scale_sem,
):
    quarters = landing.shape[0]
    piece_rows = landing.shape[1]
    traj = lax.axis_index("traj")
    me = lax.axis_index("amp")
    core = traj & 1
    first_traj = traj - core
    held = (me ^ (me >> 1)) & 1
    stays = core == held
    split_spin = LANE_BITS + BLOCK_BITS + 1
    side_spin = split_spin - 1
    zero_tile = jnp.zeros((8, LANES), jnp.float32)
    tiles = [(s, side) for s in range(BLOCK // SUB) for side in range(2)]

    def device(core_index, chip):
        return {"traj": first_traj + core_index, "amp": chip}

    def remote(source, target, send, recv, where):
        return pltpu.make_async_remote_copy(
            src_ref=source,
            dst_ref=target,
            send_sem=send,
            recv_sem=recv,
            device_id=where,
            device_id_type=pl.DeviceIdType.MESH,
        )

    other = device(1 - core, me)
    barrier = pltpu.get_barrier_semaphore()
    for flip_core in range(2):
        for flip_chip in range(quarters):
            if flip_core or flip_chip:
                pl.semaphore_signal(
                    barrier,
                    inc=1,
                    device_id=device(core ^ flip_core, me ^ flip_chip),
                    device_id_type=pl.DeviceIdType.MESH,
                )
    own_channel[...] = jnp.full(own_channel.shape, channel_ref[0], jnp.int32)
    pl.semaphore_wait(barrier, 2 * quarters - 1)

    near_chip = me ^ (held ^ core)
    far_chip = near_chip ^ 3

    def piece(core_index, chip, slot):
        source = block.at[pl.ds(pl.multiple_of(core_index * piece_rows, piece_rows), piece_rows)]
        return remote(
            source,
            landing.at[me],
            gather_send.at[slot],
            gather_recv.at[me],
            device(core_index, chip),
        )

    sends = [piece(core, far_chip, 0), piece(1 - core, far_chip, 1), piece(1 - core, near_chip, 2)]
    for send in sends:
        send.start()

    @pl.when(jnp.logical_not(stays))
    def _():
        piece(core, near_chip, 3).start()

    channel_copy = remote(
        own_channel, other_channel, channel_sem.at[0], channel_sem.at[1], other
    )
    channel_copy.start()

    unit = fields[split_spin]
    inv_unit = jnp.max(1.0 / jnp.full((8, LANES), unit, jnp.float32))
    crossed = lax.broadcasted_iota(jnp.int32, (BLOCK, BLOCK), 0)
    crossed = crossed ^ lax.broadcasted_iota(jnp.int32, (BLOCK, BLOCK), 1)
    for table, spins, axis in (
        (row_table, [LANE_BITS + b for b in range(BLOCK_BITS)], 1),
        (lane_table, [*range(LANE_BITS), side_spin], 0),
    ):
        value = jnp.zeros((BLOCK, BLOCK), jnp.float32)
        for bit, spin in enumerate(spins):
            value = jnp.where(crossed == 1 << bit, fields[spin] * inv_unit, value)
        hi, lo = split(value)
        table[...] = jnp.concatenate([hi, hi, lo], axis=axis)

    core_bit = core.astype(jnp.float32)
    core_sign = 1.0 - 2.0 * core_bit
    bond = [couplings[spin] * inv_unit for spin in range(SPINS - 1)]
    loss = [0.5 * decays[spin] * inv_unit for spin in range(SPINS)]
    for side in range(2):
        low_shape = (BLOCK, LANES)
        low_pos = lax.broadcasted_iota(jnp.int32, low_shape, 0) * LANES
        low_pos = low_pos + lax.broadcasted_iota(jnp.int32, low_shape, 1)
        side_sign = 1.0 - 2.0 * side
        low_real = jnp.zeros(low_shape, jnp.float32)
        low_imag = jnp.zeros(low_shape, jnp.float32)
        before = None
        for spin in range(side_spin):
            occupied = (lax.shift_right_logical(low_pos, spin) & 1).astype(jnp.float32)
            sign = 1.0 - 2.0 * occupied
            low_imag = low_imag - loss[spin] * occupied
            if spin > 0:
                low_real = low_real - bond[spin - 1] * (before * sign)
            before = sign
        low_real = low_real - bond[side_spin - 1] * side_sign * before
        low_real = low_real - bond[side_spin] * side_sign * core_sign
        low_imag = low_imag - side * loss[side_spin] - core_bit * loss[split_spin]
        for q in range(quarters):
            bits = [(q >> b) & 1 for b in range(SPINS - 1 - split_spin)]
            signs = [core_sign] + [1.0 - 2.0 * bit for bit in bits]
            real, imag = low_real, low_imag
            for b, bit in enumerate(bits):
                real = real - bond[split_spin + b] * (signs[b] * signs[b + 1])
                imag = imag - bit * loss[split_spin + 1 + b]
            diagonal[q, 0, side] = real
            diagonal[q, 1, side] = imag

    def window(ref, lead, part, s, side):
        return ref.at[(*lead, part, pl.ds(s * SUB, SUB), pl.ds(side * LANES, LANES))]

    def sums_copy(count, slot):
        return remote(
            own_sums.at[slot, pl.ds(0, 8 * count)],
            other_sums.at[slot, pl.ds(0, 8 * count)],
            sums_send.at[slot],
            sums_recv.at[slot],
            other,
        )

    def start_sums(values, slot):
        for k, value in enumerate(values):
            own_sums[slot, 8 * k : 8 * k + 8] = value
        sums_copy(len(values), slot).start()

    def finish_sums(count, slot):
        sums_copy(count, slot).wait()
        both = [ref[slot, : 8 * count] for ref in (own_sums, other_sums)]
        both = both[0] + both[1]
        return [jnp.sum(both[8 * k : 8 * k + 8]) for k in range(count)]

    def work_copy(slot, q):
        return remote(
            work.at[slot, q],
            mate_work.at[slot, q],
            work_send.at[slot, q],
            work_recv.at[slot, q],
            other,
        )

    @pl.when(stays)
    def _():
        def keep(i, carry):
            rows = pl.multiple_of(i * SUB, SUB)
            landing[me, pl.ds(rows, SUB), :] = block[
                pl.ds(pl.multiple_of(core * piece_rows, piece_rows) + rows, SUB), :
            ]
            return carry

        lax.fori_loop(0, piece_rows // SUB, keep, 0)

    def arrival(chip):
        return remote(
            block.at[pl.ds(0, piece_rows)],
            landing.at[chip],
            gather_send.at[0],
            gather_recv.at[chip],
            other,
        )

    def forward(chip):
        return remote(
            landing.at[chip],
            mate_landing.at[chip],
            forward_send.at[chip],
            forward_recv.at[chip],
            other,
        )

    @pl.when(jnp.logical_not(stays))
    def _():
        arrival(me).wait_recv()

    def square(ref, q, acc):
        def add(i, acc):
            x = ref[q, pl.ds(pl.multiple_of(i * 128, 128), 128), :]
            return acc + fold(x * x)

        return lax.fori_loop(0, piece_rows // 128, add, acc)

    own_sq = zero_tile
    for flip_chip in range(quarters):
        q = me ^ flip_chip
        if flip_chip:
            arrival(q).wait_recv()
        forward(q).start()
        own_sq = square(landing, q, own_sq)
    mate_sq = zero_tile
    for flip_chip in range(quarters):
        q = me ^ flip_chip
        forward(q).wait()
        mate_sq = square(mate_landing, q, mate_sq)
    beta, inv_beta = scalar_sqrt(jnp.sum(own_sq + mate_sq))

    def start_vector(q, carry):
        for source, target in ((landing, basis), (mate_landing, mate)):
            for s, side in tiles:
                for part in range(2):
                    first = (side * BLOCK + s * SUB) * 2 + part
                    x = source[q, pl.ds(first, SUB, stride=2), :]
                    window(target, (0, q), part, s, side)[...] = x * inv_beta
        return carry

    lax.fori_loop(0, quarters, start_vector, 0)

    high_fields = [fields[split_spin + 1 + b] * inv_unit for b in range(SPINS - 1 - split_spin)]
    flips = (flips_even, flips_odd)

    def issue(j, q):
        for part in range(2):
            hi, lo = split(basis[j, q, part])
            flips[q % 2][part] = dot(
                jnp.concatenate([row_table[...], hi, lo, hi], axis=1),
                jnp.concatenate([hi, lo, hi, lane_table[...]], axis=0),
            )

    def inner(k, q, s, side, wr, wi):
        vr = window(basis, (k, q), 0, s, side)[...]
        vi = window(basis, (k, q), 1, s, side)[...]
        return fold(vr * wr + vi * wi), fold(vr * wi - vi * wr)

    def consume(j, q, acc, against, keep):
        slot = j % 2
        for s, side in tiles:
            x = [window(basis, (j, q), part, s, side)[...] for part in range(2)]
            f = []
            for part in range(2):
                value = window(flips[q % 2], (), part, s, side)[...]
                value = value + window(mate, (slot, q), part, s, side)[...]
                for b, field in enumerate(high_fields):
                    value = value + field * window(basis, (j, q ^ (1 << b)), part, s, side)[...]
                f.append(value)
            dr = window(diagonal, (q, 0), side, s, 0)[...]
            di = window(diagonal, (q, 1), side, s, 0)[...]
            wr = dr * x[0] - di * x[1] - f[0]
            wi = dr * x[1] + di * x[0] - f[1]
            for n, k in enumerate(against):
                real, imag = inner(k, q, s, side, wr, wi)
                acc[2 * n] = acc[2 * n] + real
                acc[2 * n + 1] = acc[2 * n + 1] + imag
            if keep:
                window(work, (slot, q), 0, s, side)[...] = wr
                window(work, (slot, q), 1, s, side)[...] = wi
                acc[-1] = acc[-1] + fold(wr * wr + wi * wi)

    def apply(j, against, keep):
        acc = [zero_tile] * (2 * len(against) + keep)
        for q in range(quarters):
            if q + 1 < quarters:
                issue(j, q + 1)
            consume(j, q, acc, against, keep)
            if keep:
                work_copy(j % 2, q).start()
        return acc

    def rest_inner(j):
        slot = j % 2

        def one(k, carry):
            def add(q, acc):
                real, imag = acc
                for s, side in tiles:
                    wr = window(work, (slot, q), 0, s, side)[...]
                    wi = window(work, (slot, q), 1, s, side)[...]
                    more = inner(k, q, s, side, wr, wi)
                    real, imag = real + more[0], imag + more[1]
                return real, imag

            real, imag = lax.fori_loop(0, quarters, add, (zero_tile, zero_tile))
            own_rest[j, k, 0] = real
            own_rest[j, k, 1] = imag
            return carry

        lax.fori_loop(0, j - 1, one, 0)

    def step(j, first):
        slot = j % 2
        against = [j] if first else [j, j - 1]
        count = 2 * len(against) + 1
        start_sums(apply(j, against, True), slot)
        if not first:
            rest_inner(j)
        coeffs = finish_sums(count, slot)
        left = coeffs[-1]
        for value in coeffs[:-1]:
            left = left - value * value
        norm, inv_norm = scalar_sqrt(left)
        for n, value in enumerate(coeffs[:-1]):
            scalars[j, n] = value
        scalars[j, 4] = norm
        scalars[j, 5] = inv_norm

        def subtract(q, w_ref, u_ref, now, before, after):
            for s, side in tiles:
                rr = window(w_ref, (slot, q), 0, s, side)[...]
                ri = window(w_ref, (slot, q), 1, s, side)[...]
                for n, lead in enumerate([now] if first else [now, before]):
                    vr = window(u_ref, (lead, q), 0, s, side)[...]
                    vi = window(u_ref, (lead, q), 1, s, side)[...]
                    hr, hm = coeffs[2 * n], coeffs[2 * n + 1]
                    rr = rr - (hr * vr - hm * vi)
                    ri = ri - (hr * vi + hm * vr)
                window(u_ref, (after, q), 0, s, side)[...] = rr * inv_norm
                window(u_ref, (after, q), 1, s, side)[...] = ri * inv_norm

        subtract(0, work, basis, j, j - 1, j + 1)
        issue(j + 1, 0)
        for q in range(1, quarters):
            subtract(q, work, basis, j, j - 1, j + 1)
        for q in range(quarters):
            work_copy(slot, q).wait()
        for q in range(quarters):
            subtract(q, mate_work, mate, slot, 1 - slot, 1 - slot)

    final = KRYLOV - 1
    issue(0, 0)
    step(0, True)

    def later(j, carry):
        step(j, False)
        return carry

    lax.fori_loop(1, final, later, 0)
    rest_copy = remote(own_rest, other_rest, rest_sem.at[0], rest_sem.at[1], other)
    rest_copy.start()
    start_sums(apply(final, list(range(KRYLOV)), False), final % 2)
    rest_copy.wait()
    sub = lax.broadcasted_iota(jnp.int32, (8, LANES), 0)
    lane = lax.broadcasted_iota(jnp.int32, (8, LANES), 1)

    def put(tile, where, value):
        return jnp.where(where, value, tile)

    gram = [jnp.where(sub == lane, 1.0, 0.0).astype(jnp.float32), zero_tile]
    projected = [zero_tile, zero_tile]
    column = {j: [zero_tile, zero_tile] for j in range(3)}
    across = {j: [zero_tile, zero_tile] for j in range(3)}
    for j in range(final):
        here = lane == j
        alpha = [scalars[j, 0], scalars[j, 1]]
        bravo = [scalars[j, 2], scalars[j, 3]]
        for part in range(2):
            projected[part] = put(projected[part], here & (sub == j), alpha[part])
            if j > 0:
                projected[part] = put(projected[part], here & (sub == j - 1), bravo[part])
        projected[0] = put(projected[0], here & (sub == j + 1), scalars[j, 4])
        if j < 2:
            continue
        down = [zero_tile, zero_tile]
        along = [zero_tile, zero_tile]
        for k in range(j - 1):
            for part in range(2):
                value = jnp.sum(own_rest[j, k, part] + other_rest[j, k, part])
                down[part] = put(down[part], sub == k, value)
                along[part] = put(along[part], lane == k, value)
        for made, new in ((column, down), (across, along)):
            for value, old in ((alpha, made[j]), (bravo, made[j - 1])):
                new[0] = new[0] - (value[0] * old[0] - value[1] * old[1])
                new[1] = new[1] - (value[0] * old[1] + value[1] * old[0])
            made[j + 1] = [part * scalars[j, 5] for part in new]
        gram[0] = gram[0] + jnp.where(lane == j + 1, column[j + 1][0], 0.0)
        gram[0] = gram[0] + jnp.where(sub == j + 1, across[j + 1][0], 0.0)
        gram[1] = gram[1] + jnp.where(lane == j + 1, column[j + 1][1], 0.0)
        gram[1] = gram[1] - jnp.where(sub == j + 1, across[j + 1][1], 0.0)

    targets = finish_sums(2 * KRYLOV, final % 2)
    for k in range(KRYLOV):
        for part in range(2):
            gram[part] = put(gram[part], (lane == KRYLOV) & (sub == k), targets[2 * k + part])

    def column_of(tile, k):
        return jnp.broadcast_to(tile[:, k : k + 1], tile.shape)

    def row_of(tile, k):
        return jnp.broadcast_to(tile[k : k + 1, :], tile.shape)

    for p in range(KRYLOV):
        row = [row_of(tile, p) for tile in gram]
        factor = [column_of(tile, p) for tile in gram]
        inverse = 1.0 / row_of(factor[0], p)
        row = [tile * inverse for tile in row]
        less = (
            factor[0] * row[0] - factor[1] * row[1],
            factor[0] * row[1] + factor[1] * row[0],
        )
        gram = [jnp.where(sub == p, row[n], gram[n] - less[n]) for n in range(2)]
    for part in range(2):
        projected[part] = put(projected[part], lane == final, column_of(gram[part], KRYLOV))

    def product(a, b):
        real, imag = zero_tile, zero_tile
        for k in range(KRYLOV):
            ar, ai = column_of(a[0], k), column_of(a[1], k)
            br, bi = row_of(b[0], k), row_of(b[1], k)
            real = real + (ar * br - ai * bi)
            imag = imag + (ar * bi + ai * br)
        return real, imag

    inside = lane < KRYLOV
    pace = unit * (time_step / 2.0**squarings)
    first = (
        jnp.where(inside, projected[1] * pace, 0.0),
        jnp.where(inside, projected[0] * -pace, 0.0),
    )
    second = product(first, first)
    third = product(second, first)
    identity = jnp.where(sub == lane, 1.0, 0.0).astype(jnp.float32)
    series = None
    for low in range(taylor_order // 3 * 3, -1, -3):
        terms = [identity * (1.0 / math.factorial(low)), zero_tile]
        for n, power in ((low + 1, first), (low + 2, second)):
            if n <= taylor_order:
                terms = [t + p * (1.0 / math.factorial(n)) for t, p in zip(terms, power)]
        if series is not None:
            terms = [t + p for t, p in zip(terms, product(third, series))]
        series = terms
    for repeat in range(squarings):
        series = product(series, series)
    weights = [
        jnp.sum(jnp.where((sub == k) & (lane == 0), tile * beta, 0.0))
        for tile in series
        for k in range(KRYLOV)
    ]
    channel_copy.wait()
    channel = jnp.where(stays, own_channel[...], other_channel[...])
    sub_pos = lax.broadcasted_iota(jnp.int32, (SUB, LANES), 0) * LANES
    sub_pos = sub_pos + lax.broadcasted_iota(jnp.int32, (SUB, LANES), 1)

    def combine(q, acc):
        high = (core << split_spin) + (q << (split_spin + 1))
        for s, side in tiles:
            pr = jnp.zeros((SUB, LANES), jnp.float32)
            pi = jnp.zeros((SUB, LANES), jnp.float32)
            for k in range(KRYLOV):
                vr = window(basis, (k, q), 0, s, side)[...]
                vi = window(basis, (k, q), 1, s, side)[...]
                cr, ci = weights[k], weights[k + KRYLOV]
                pr = pr + (cr * vr - ci * vi)
                pi = pi + (cr * vi + ci * vr)
            window(work, (0, q), 0, s, side)[...] = pr
            window(work, (0, q), 1, s, side)[...] = pi
            position = sub_pos + (high + (side << side_spin) + s * SUB * LANES)
            occupied = lax.shift_right_logical(position, channel) & 1
            acc = acc + fold(jnp.where(occupied == 1, pr * pr + pi * pi, 0.0))
        return acc

    jumped_sq = lax.fori_loop(0, quarters, combine, zero_tile)

    start_sums([jumped_sq], 0)

    def pack(target, q, part):
        for s, side in tiles:
            value = window(work, (0, q), part, s, side)[...]
            for b in range(SPINS - 1 - split_spin):
                flipped = window(work, (0, q | (1 << b)), part, s, side)[...]
                value = jnp.where(channel == split_spin + 1 + b, flipped, value)
            target[s * SUB : (s + 1) * SUB, side * LANES : (side + 1) * LANES] = value

    parcels = []
    for part in range(2):
        q = me ^ (1 << part)
        pack(parcel.at[part], q, part)
        copy = remote(
            parcel.at[part],
            pieces.at[core, part],
            parcel_send.at[part],
            parcel_recv.at[core, part],
            device(held, q),
        )
        copy.start()
        parcels.append(copy)
    for part in range(2):
        pack(parcel.at[2 + part], me, part)
    home = remote(
        parcel.at[pl.ds(2, 2)], pieces.at[core], parcel_send.at[2], parcel_recv.at[2, 0], other
    )

    @pl.when(jnp.logical_not(stays))
    def _():
        home.start()

    @pl.when(stays)
    def _():
        for part in range(2):
            pieces[core, part] = parcel[2 + part]

    all_sq = finish_sums(1, 0)[0]
    size = jnp.float32(quarters * 2 * piece_rows // 2 * LANES)
    ratio = jnp.where(channel[:8] < SPINS, size / jnp.full((8, LANES), all_sq, jnp.float32), 1.0)
    own_scale = jnp.sqrt(ratio)
    own_sums[1, 0:8] = own_scale
    scale_copy = remote(
        own_sums.at[1, pl.ds(0, 8)], scale_out, scale_sem.at[0], scale_sem.at[1],
        device(core, me ^ 1),
    )

    @pl.when(stays)
    def _():
        scale_copy.start()
        scale_out[...] = own_scale
        remote(
            parcel.at[pl.ds(2, 2)], pieces.at[1 - core], parcel_send.at[2],
            parcel_recv.at[2, 0], other,
        ).wait_recv()
        scale_copy.wait_send()

    @pl.when(jnp.logical_not(stays))
    def _():
        for sender in range(2):
            for part in range(2):
                remote(
                    parcel.at[part], pieces.at[sender, part], parcel_send.at[part],
                    parcel_recv.at[sender, part], other,
                ).wait_recv()
        scale_copy.wait_recv()
        home.wait_send()
        piece(core, near_chip, 3).wait_send()

    for copy in parcels:
        copy.wait_send()
    for send in sends:
        send.wait_send()


def lower_kernel(channel_ref, pieces, scale, out):
    channel = channel_ref[0]
    me = lax.axis_index("amp")
    side_spin = LANE_BITS + BLOCK_BITS
    in_lanes = channel < LANE_BITS
    in_rows = jnp.logical_not(in_lanes) & (channel < side_spin)
    lane_shift = jnp.where(in_lanes, lax.shift_left(1, channel), 0)
    row_shift = jnp.where(in_rows, lax.shift_left(1, jnp.maximum(channel - LANE_BITS, 0)), 0)
    near = jnp.where(row_shift < 8, row_shift, 0)
    far = jnp.where(row_shift < 8, 0, row_shift)
    lane_turn = (LANES - lane_shift) % LANES
    row_turn = (8 - near) % 8
    sub_pos = lax.broadcasted_iota(jnp.int32, (8, LANES), 0) * LANES
    sub_pos = sub_pos + lax.broadcasted_iota(jnp.int32, (8, LANES), 1)
    own = me * (4 * BLOCK * LANES)
    factor = scale[...]

    for half in range(2):
        from_half = jnp.where(channel == side_spin + 1, 1, half)
        for side in range(2):
            from_side = jnp.where(channel == side_spin, 1, side)
            columns = pl.ds(pl.multiple_of(from_side * LANES, LANES), LANES)

            def lower(i, carry, half=half, side=side, from_half=from_half, columns=columns):
                for t in range(8):
                    local = i * 64 + t * 8
                    base = (half * 2 + side) * BLOCK + local
                    rows = pl.ds(pl.multiple_of(local | far, 8), 8)
                    position = sub_pos + (own + base * LANES)
                    vacant = (lax.shift_right_logical(position, channel) & 1) == 0
                    for part in range(2):
                        x = pieces[from_half, part, rows, columns]
                        x = pltpu.roll(x, row_turn, 0)
                        x = pltpu.roll(x, lane_turn, 1)
                        x = jnp.where(vacant, x * factor, 0.0)
                        out[pl.ds(base * 2 + part, 8, stride=2), :] = x
                return carry

            lax.fori_loop(0, BLOCK // 64, lower, 0)


def paired_body(amplitudes, couplings, fields, decays, channel):
    quarters = lax.axis_size("amp")
    local_len = amplitudes.shape[2]
    block_rows = local_len // LANES
    vmem = pl.BlockSpec(memory_space=pltpu.VMEM)
    smem = pl.BlockSpec(memory_space=pltpu.SMEM)
    f32 = jnp.float32
    dma = pltpu.SemaphoreType.DMA
    sums_rows = 8 * (2 * KRYLOV + 1)
    state = amplitudes.reshape(2, block_rows, LANES).transpose(1, 0, 2)
    state = state.reshape(2 * block_rows, LANES)
    pieces, scale = pl.pallas_call(
        pair_kernel,
        out_shape=(
            jax.ShapeDtypeStruct((2, 2, BLOCK, BLOCK), f32),
            jax.ShapeDtypeStruct((8, LANES), f32),
        ),
        in_specs=[smem] * 4 + [vmem],
        out_specs=(vmem, vmem),
        scratch_shapes=[
            pltpu.VMEM((quarters, block_rows, LANES), f32),
            pltpu.VMEM((quarters, block_rows, LANES), f32),
            pltpu.VMEM((KRYLOV, quarters, 2, BLOCK, BLOCK), f32),
            pltpu.VMEM((2, quarters, 2, BLOCK, BLOCK), f32),
            pltpu.VMEM((2, quarters, 2, BLOCK, BLOCK), f32),
            pltpu.VMEM((2, quarters, 2, BLOCK, BLOCK), f32),
            pltpu.VMEM((2, BLOCK, BLOCK), f32),
            pltpu.VMEM((2, BLOCK, BLOCK), f32),
            pltpu.VMEM((BLOCK, 3 * BLOCK), jnp.bfloat16),
            pltpu.VMEM((3 * BLOCK, BLOCK), jnp.bfloat16),
            pltpu.VMEM((quarters, 2, 2, BLOCK, LANES), f32),
            pltpu.VMEM((2, sums_rows, LANES), f32),
            pltpu.VMEM((2, sums_rows, LANES), f32),
            pltpu.VMEM((KRYLOV - 1, KRYLOV - 3, 2, 8, LANES), f32),
            pltpu.VMEM((KRYLOV - 1, KRYLOV - 3, 2, 8, LANES), f32),
            pltpu.SMEM((KRYLOV - 1, 6), f32),
            pltpu.VMEM((SUB, LANES), jnp.int32),
            pltpu.VMEM((SUB, LANES), jnp.int32),
            pltpu.VMEM((4, BLOCK, BLOCK), f32),
            dma((4,)),
            dma((quarters,)),
            dma((quarters,)),
            dma((quarters,)),
            dma((2,)),
            dma((2,)),
            dma((2,)),
            dma((2, quarters)),
            dma((2, quarters)),
            dma((2,)),
            dma((3,)),
            dma((3, 2)),
            dma((2,)),
        ],
        compiler_params=pltpu.CompilerParams(
            collective_id=1, has_side_effects=True, vmem_limit_bytes=62 * 1024 * 1024
        ),
        name="pair",
    )(channel, couplings, fields, decays, state)
    lowered = pl.pallas_call(
        lower_kernel,
        out_shape=jax.ShapeDtypeStruct((2 * block_rows, LANES), f32),
        in_specs=[smem, vmem, vmem],
        out_specs=vmem,
        name="lower",
    )(channel, pieces, scale)
    lowered = lowered.reshape(block_rows, 2, LANES).transpose(1, 0, 2)
    return lowered.reshape(amplitudes.shape)


def solution(mesh):
    placed = (P("traj", None, "amp"), P(), P(), P(), P("traj"))

    def step(amplitudes, *rest):
        trajectories = mesh.shape["traj"]
        low_rows = amplitudes.shape[2] // mesh.shape["amp"] // LANES
        paired = (
            mesh.shape["amp"] == 4
            and trajectories % 2 == 0
            and amplitudes.shape[0] == trajectories
            and low_rows == 4 * BLOCK
        )
        return jax.shard_map(
            paired_body if paired else body,
            mesh=mesh,
            in_specs=placed,
            out_specs=P("traj", None, "amp"),
            check_vma=False,
        )(amplitudes, *rest)

    return step
```

```python
import math

import jax
import jax.numpy as jnp
from jax import lax
from jax.experimental import pallas as pl
from jax.experimental.pallas import tpu as pltpu
from jax.sharding import PartitionSpec as P

SPINS = 19
KRYLOV = 8
LANES = 128
LANE_BITS = 7

time_step = 0.7
squarings = 8
taylor_order = 10
highest = lax.Precision.HIGHEST

CHUNK_BITS = 8
CHUNK = 1 << CHUNK_BITS
SUB = 32


def split(x):
    hi = x.astype(jnp.bfloat16)
    lo = (x - hi.astype(jnp.float32)).astype(jnp.bfloat16)
    return hi, lo


def dot(a, b):
    return jnp.dot(a, b, preferred_element_type=jnp.float32)


def fold(x):
    return jnp.sum(x.reshape(x.shape[0] // 8, 8, x.shape[1]), axis=0)


def scalar_sqrt(value):
    root = jnp.sqrt(jnp.full((8, LANES), value, jnp.float32))
    return jnp.max(root), jnp.max(1.0 / root)


def krylov_weights(a_matrix):
    size = a_matrix.shape[0]
    pad = jnp.zeros((LANES - size, LANES), jnp.float32)
    scaled = jnp.concatenate([a_matrix, pad], axis=0) * (1.0 / 2.0**squarings)
    rows = lax.broadcasted_iota(jnp.int32, (LANES, LANES), 0)
    cols = lax.broadcasted_iota(jnp.int32, (LANES, LANES), 1)
    identity = jnp.where(rows == cols, 1.0, 0.0).astype(jnp.float32)
    series = identity
    for degree in range(taylor_order, 0, -1):
        product = jnp.dot(
            scaled, series, precision=highest, preferred_element_type=jnp.float32
        )
        series = identity + product * (1.0 / degree)
    for repeat in range(squarings):
        series = jnp.dot(
            series, series, precision=highest, preferred_element_type=jnp.float32
        )
    return series


def kernel(
    channel_ref,
    couplings,
    fields,
    decays,
    state,
    out,
    basis,
    work,
    flips,
    row_table,
    lane_table,
    diag_low,
):
    node_count, _, block_rows, _ = state.shape
    rows = node_count * block_rows
    chunks = rows // CHUNK
    subs = CHUNK // SUB
    channel = channel_ref[0]
    device = lax.axis_index("amp")
    zero_tile = jnp.zeros((8, LANES), jnp.float32)
    per_block = block_rows // CHUNK

    table_shape = (CHUNK, CHUNK)
    crossed = lax.broadcasted_iota(jnp.int32, table_shape, 0)
    crossed = crossed ^ lax.broadcasted_iota(jnp.int32, table_shape, 1)
    for table, first_spin, bits in (
        (row_table, LANE_BITS, CHUNK_BITS),
        (lane_table, 0, LANE_BITS),
    ):
        value = jnp.zeros(table_shape, jnp.float32)
        for bit in range(bits):
            value = jnp.where(crossed == 1 << bit, fields[first_spin + bit], value)
        table[0], table[1] = split(value)

    low_shape = (CHUNK, LANES)
    low_pos = lax.broadcasted_iota(jnp.int32, low_shape, 0) * LANES
    low_pos = low_pos + lax.broadcasted_iota(jnp.int32, low_shape, 1)
    low_bits = LANE_BITS + CHUNK_BITS
    before = None
    low_real = jnp.zeros(low_shape, jnp.float32)
    low_imag = jnp.zeros(low_shape, jnp.float32)
    for spin in range(low_bits):
        occupied = (lax.shift_right_logical(low_pos, spin) & 1).astype(jnp.float32)
        sign = 1.0 - 2.0 * occupied
        low_imag = low_imag - 0.5 * decays[spin] * occupied
        if spin > 0:
            low_real = low_real - couplings[spin - 1] * (before * sign)
        before = sign
    diag_low[0] = low_real
    diag_low[1] = low_imag

    def high_diagonal(i):
        bits = [
            (lax.shift_right_logical(i, b) & 1).astype(jnp.float32)
            for b in range(SPINS - low_bits)
        ]
        signs = [1.0 - 2.0 * bit for bit in bits]
        real = jnp.float32(0.0)
        imag = jnp.float32(0.0)
        for b in range(len(bits)):
            imag = imag - 0.5 * decays[low_bits + b] * bits[b]
            if b > 0:
                real = real - couplings[low_bits + b - 1] * signs[b - 1] * signs[b]
        edge = couplings[low_bits - 1] * signs[0]
        return real - edge, real + edge, imag

    def start_norm(i, acc):
        node = i // per_block
        first = (i % per_block) * CHUNK
        for part in range(2):
            x = state[node, part, pl.ds(first, CHUNK), :]
            acc = acc + fold(x * x)
        return acc

    start_sq = jnp.sum(lax.fori_loop(0, chunks, start_norm, zero_tile))
    beta, inv_beta = scalar_sqrt(start_sq)

    def start_vector(i, carry):
        node = i // per_block
        first = (i % per_block) * CHUNK
        for part in range(2):
            basis[0, pl.ds(i * CHUNK, CHUNK), part * LANES : (part + 1) * LANES] = (
                state[node, part, pl.ds(first, CHUNK), :] * inv_beta
            )
        return carry

    lax.fori_loop(0, chunks, start_vector, 0)

    mat_rows = lax.broadcasted_iota(jnp.int32, (2 * KRYLOV, LANES), 0)
    mat_cols = lax.broadcasted_iota(jnp.int32, (2 * KRYLOV, LANES), 1)
    a_matrix = jnp.zeros((2 * KRYLOV, LANES), jnp.float32)

    def put(matrix, k, j, real, imag):
        a_real = time_step * imag
        a_imag = -time_step * real
        for r, c, value in (
            (k, j, a_real),
            (k, j + KRYLOV, -a_imag),
            (k + KRYLOV, j, a_imag),
            (k + KRYLOV, j + KRYLOV, a_real),
        ):
            matrix = jnp.where((mat_rows == r) & (mat_cols == c), value, matrix)
        return matrix

    high_fields = [
        fields[LANE_BITS + CHUNK_BITS + b] for b in range(SPINS - LANE_BITS - CHUNK_BITS)
    ]

    for j in range(KRYLOV):
        last = j + 1 == KRYLOV

        def apply_chunk(i, acc, j=j):
            base = pl.multiple_of(i * CHUNK, CHUNK)
            hi, lo = split(basis[j, pl.ds(base, CHUNK), :])
            flips[...] = (
                dot(row_table[0], hi)
                + dot(row_table[1], hi)
                + dot(row_table[0], lo)
                + dot(hi, lane_table[0])
                + dot(lo, lane_table[0])
                + dot(hi, lane_table[1])
            )
            acc = list(acc)
            real_vacant, real_occupied, imag_high = high_diagonal(i)
            for s in range(subs):
                here = pl.ds(base + s * SUB, SUB)
                x = basis[j, here, :]
                f = flips[s * SUB : (s + 1) * SUB, :]
                for b, field in enumerate(high_fields):
                    there = pl.multiple_of((i ^ (1 << b)) * CHUNK, CHUNK)
                    f = f + field * basis[j, pl.ds(there + s * SUB, SUB), :]
                part = slice(s * SUB, (s + 1) * SUB)
                dr = diag_low[0, part, :] + (real_vacant if s < subs // 2 else real_occupied)
                di = diag_low[1, part, :] + imag_high
                xr, xi = x[:, :LANES], x[:, LANES:]
                wr = dr * xr - di * xi - f[:, :LANES]
                wi = dr * xi + di * xr - f[:, LANES:]
                work[here, :LANES] = wr
                work[here, LANES:] = wi
                for k in range(j + 1):
                    vr = basis[k, here, :LANES]
                    vi = basis[k, here, LANES:]
                    acc[2 * k] = acc[2 * k] + fold(vr * wr + vi * wi)
                    acc[2 * k + 1] = acc[2 * k + 1] + fold(vr * wi - vi * wr)
                acc[-1] = acc[-1] + fold(wr * wr + wi * wi)
            return tuple(acc)

        sums = lax.fori_loop(0, chunks, apply_chunk, (zero_tile,) * (2 * j + 3))
        coeffs = [jnp.sum(t) for t in sums]
        for k in range(j + 1):
            a_matrix = put(a_matrix, k, j, coeffs[2 * k], coeffs[2 * k + 1])
        if last:
            break
        left = coeffs[-1]
        for value in coeffs[:-1]:
            left = left - value * value
        norm, inv_norm = scalar_sqrt(left)
        a_matrix = put(a_matrix, j + 1, j, norm, jnp.float32(0.0))

        def subtract_chunk(i, carry, j=j, coeffs=coeffs, inv_norm=inv_norm):
            base = pl.multiple_of(i * CHUNK, CHUNK)
            for s in range(subs):
                here = pl.ds(base + s * SUB, SUB)
                rr = work[here, :LANES]
                ri = work[here, LANES:]
                for k in range(j + 1):
                    vr = basis[k, here, :LANES]
                    vi = basis[k, here, LANES:]
                    hr, hm = coeffs[2 * k], coeffs[2 * k + 1]
                    rr = rr - (hr * vr - hm * vi)
                    ri = ri - (hr * vi + hm * vr)
                basis[j + 1, here, :LANES] = rr * inv_norm
                basis[j + 1, here, LANES:] = ri * inv_norm
            return carry

        lax.fori_loop(0, chunks, subtract_chunk, 0)

    series = krylov_weights(a_matrix)
    first = series[: 2 * KRYLOV, :] * beta
    weights = [
        jnp.sum(jnp.where((mat_rows == k) & (mat_cols == 0), first, 0.0))
        for k in range(2 * KRYLOV)
    ]
    sub_pos = lax.broadcasted_iota(jnp.int32, (SUB, LANES), 0) * LANES
    sub_pos = sub_pos + lax.broadcasted_iota(jnp.int32, (SUB, LANES), 1)

    def combine(i, acc):
        base = pl.multiple_of(i * CHUNK, CHUNK)
        for s in range(subs):
            here = pl.ds(base + s * SUB, SUB)
            pr = jnp.zeros((SUB, LANES), jnp.float32)
            pi = jnp.zeros((SUB, LANES), jnp.float32)
            for k in range(KRYLOV):
                vr = basis[k, here, :LANES]
                vi = basis[k, here, LANES:]
                cr, ci = weights[k], weights[k + KRYLOV]
                pr = pr + (cr * vr - ci * vi)
                pi = pi + (cr * vi + ci * vr)
            work[here, :LANES] = pr
            work[here, LANES:] = pi
            position = sub_pos + (base + s * SUB) * LANES
            occupied = lax.shift_right_logical(position, channel) & 1
            acc = acc + fold(jnp.where(occupied == 1, pr * pr + pi * pi, 0.0))
        return acc

    total = jnp.sum(lax.fori_loop(0, chunks, combine, zero_tile))
    jumped = channel < SPINS
    size = jnp.float32(rows * LANES)
    total = jnp.where(jumped, total, size)
    root = jnp.sqrt(size / jnp.full((8, LANES), total, jnp.float32))
    scale = jnp.max(root)
    in_lanes = channel < LANE_BITS
    lane_shift = jnp.where(in_lanes, lax.shift_left(1, channel), 0)
    row_shift = jnp.where(
        in_lanes | (channel >= SPINS),
        0,
        lax.shift_left(1, jnp.maximum(channel - LANE_BITS, 0)),
    )
    in_sublanes = row_shift < 8
    near = jnp.where(in_sublanes, row_shift, 0)
    far = jnp.where(in_sublanes, 0, row_shift)
    lane_turn = (LANES - lane_shift) % LANES
    row_turn = (SUB - near) % SUB

    def jump(i, carry):
        local = pl.multiple_of(i * SUB, SUB)
        base = device * block_rows + local
        source = pl.multiple_of(base + far, 8)
        position = sub_pos + base * LANES
        vacant = (lax.shift_right_logical(position, channel) & 1) == 0
        for part in range(2):
            x = work[pl.ds(source, SUB), part * LANES : (part + 1) * LANES]
            x = pltpu.roll(x, row_turn, 0)
            x = pltpu.roll(x, lane_turn, 1)
            out[part, pl.ds(local, SUB), :] = jnp.where(vacant, x * scale, 0.0)
        return carry

    lax.fori_loop(0, block_rows // SUB, jump, 0)


def gather_kernel(block, out, send_sem, recv_sem):
    me = lax.axis_index("amp")
    near = (me ^ 1, me ^ 2)
    barrier = pltpu.get_barrier_semaphore()
    for partner in near:
        pl.semaphore_signal(
            barrier, inc=1, device_id={"amp": partner}, device_id_type=pl.DeviceIdType.MESH
        )
    pl.semaphore_wait(barrier, 2)

    def copy(source, owner, part, axis, slot):
        return pltpu.make_async_remote_copy(
            src_ref=source,
            dst_ref=out.at[owner, part],
            send_sem=send_sem.at[slot],
            recv_sem=recv_sem.at[slot],
            device_id={"amp": near[axis]},
            device_id_type=pl.DeviceIdType.MESH,
        )

    direct = {}
    for turn in range(2):
        for axis in range(2):
            part = axis ^ turn
            direct[axis, part] = copy(block.at[part], me, part, axis, 2 * axis + part)
            direct[axis, part].start()
    out[me] = block[...]
    forwards = []
    for axis in range(2):
        direct[axis, axis].wait_recv()
        owner = near[axis]
        forward = copy(out.at[owner, axis], owner, axis, 1 - axis, 4 + axis)
        forward.start()
        forwards.append(forward)
    for axis in range(2):
        direct[axis, 1 - axis].wait_recv()
    for forward in forwards:
        forward.wait_recv()
    for sent in list(direct.values()) + forwards:
        sent.wait_send()


def gather(block):
    node_count = lax.axis_size("amp")
    if node_count != 4:
        return lax.all_gather(block, "amp")
    vmem = pl.BlockSpec(memory_space=pltpu.VMEM)
    return pl.pallas_call(
        gather_kernel,
        out_shape=jax.ShapeDtypeStruct((node_count,) + block.shape, block.dtype),
        in_specs=[vmem],
        out_specs=vmem,
        scratch_shapes=[pltpu.SemaphoreType.DMA((6,)), pltpu.SemaphoreType.DMA((6,))],
        compiler_params=pltpu.CompilerParams(collective_id=0, has_side_effects=True),
        name="gather",
    )(block)


def body(amplitudes, couplings, fields, decays, channel):
    node_count = lax.axis_size("amp")
    local_len = amplitudes.shape[2]
    block_rows = local_len // LANES
    rows = node_count * block_rows
    vmem = pl.BlockSpec(memory_space=pltpu.VMEM)
    smem = pl.BlockSpec(memory_space=pltpu.SMEM)
    call = pl.pallas_call(
        kernel,
        out_shape=jax.ShapeDtypeStruct((2, block_rows, LANES), jnp.float32),
        in_specs=[smem] * 4 + [vmem],
        out_specs=vmem,
        scratch_shapes=[
            pltpu.VMEM((KRYLOV, rows, 2 * LANES), jnp.float32),
            pltpu.VMEM((rows + rows // 2, 2 * LANES), jnp.float32),
            pltpu.VMEM((CHUNK, 2 * LANES), jnp.float32),
            pltpu.VMEM((2, CHUNK, CHUNK), jnp.bfloat16),
            pltpu.VMEM((2, CHUNK, CHUNK), jnp.bfloat16),
            pltpu.VMEM((2, CHUNK, LANES), jnp.float32),
        ],
        compiler_params=pltpu.CompilerParams(vmem_limit_bytes=62 * 1024 * 1024),
        name="trajectory",
    )
    results = []
    for t in range(amplitudes.shape[0]):
        block = amplitudes[t].reshape(2, block_rows, LANES)
        state = gather(block)
        results.append(call(channel[t : t + 1], couplings, fields, decays, state))
    return jnp.stack(results).reshape(amplitudes.shape)


BLOCK = 256
BLOCK_BITS = 8
TILE = 16


def pair_kernel(
    channel_ref,
    couplings,
    fields,
    decays,
    block,
    pieces,
    scale_out,
    landing,
    mate_landing,
    basis,
    mate,
    work,
    mate_work,
    flips,
    splits,
    row_table,
    lane_table,
    diagonal,
    own_sums,
    other_sums,
    own_rest,
    other_rest,
    scalars,
    own_channel,
    other_channel,
    parcel,
    gather_send,
    gather_recv,
    forward_send,
    forward_recv,
    sums_send,
    sums_recv,
    rest_sem,
    work_send,
    work_recv,
    channel_sem,
    parcel_send,
    parcel_recv,
    scale_sem,
):
    quarters = landing.shape[0]
    piece_rows = landing.shape[1]
    traj = lax.axis_index("traj")
    me = lax.axis_index("amp")
    core = traj & 1
    first_traj = traj - core
    held = (me ^ (me >> 1)) & 1
    stays = core == held
    split_spin = LANE_BITS + BLOCK_BITS + 1
    side_spin = split_spin - 1
    zero_tile = jnp.zeros((8, LANES), jnp.float32)
    tiles = [(s, side) for s in range(BLOCK // TILE) for side in range(2)]
    half = BLOCK // 2

    def device(core_index, chip):
        return {"traj": first_traj + core_index, "amp": chip}

    def remote(source, target, send, recv, where):
        return pltpu.make_async_remote_copy(
            src_ref=source,
            dst_ref=target,
            send_sem=send,
            recv_sem=recv,
            device_id=where,
            device_id_type=pl.DeviceIdType.MESH,
        )

    other = device(1 - core, me)
    barrier = pltpu.get_barrier_semaphore()
    for flip_core in range(2):
        for flip_chip in range(quarters):
            if flip_core or flip_chip:
                pl.semaphore_signal(
                    barrier,
                    inc=1,
                    device_id=device(core ^ flip_core, me ^ flip_chip),
                    device_id_type=pl.DeviceIdType.MESH,
                )
    own_channel[...] = jnp.full(own_channel.shape, channel_ref[0], jnp.int32)
    pl.semaphore_wait(barrier, 2 * quarters - 1)

    near_chip = me ^ (held ^ core)
    far_chip = near_chip ^ 3

    def piece(core_index, chip, slot):
        source = block.at[pl.ds(pl.multiple_of(core_index * piece_rows, piece_rows), piece_rows)]
        return remote(
            source,
            landing.at[me],
            gather_send.at[slot],
            gather_recv.at[me],
            device(core_index, chip),
        )

    sends = [piece(core, far_chip, 0), piece(1 - core, far_chip, 1), piece(1 - core, near_chip, 2)]
    for send in sends:
        send.start()

    @pl.when(jnp.logical_not(stays))
    def _():
        piece(core, near_chip, 3).start()

    channel_copy = remote(
        own_channel, other_channel, channel_sem.at[0], channel_sem.at[1], other
    )
    channel_copy.start()

    unit = fields[split_spin]
    inv_unit = jnp.max(1.0 / jnp.full((8, LANES), unit, jnp.float32))
    crossed = lax.broadcasted_iota(jnp.int32, (BLOCK, BLOCK), 0)
    crossed = crossed ^ lax.broadcasted_iota(jnp.int32, (BLOCK, BLOCK), 1)
    for table, spins, axis in (
        (row_table, [LANE_BITS + b for b in range(BLOCK_BITS)], 1),
        (lane_table, [*range(LANE_BITS), side_spin], 0),
    ):
        value = jnp.zeros((BLOCK, BLOCK), jnp.float32)
        for bit, spin in enumerate(spins):
            value = jnp.where(crossed == 1 << bit, fields[spin] * inv_unit, value)
        hi, lo = split(value)
        table[...] = jnp.concatenate([hi, hi, lo], axis=axis)

    core_bit = core.astype(jnp.float32)
    core_sign = 1.0 - 2.0 * core_bit
    bond = [couplings[spin] * inv_unit for spin in range(SPINS - 1)]
    loss = [0.5 * decays[spin] * inv_unit for spin in range(SPINS)]
    for side in range(2):
        low_shape = (BLOCK, LANES)
        low_pos = lax.broadcasted_iota(jnp.int32, low_shape, 0) * LANES
        low_pos = low_pos + lax.broadcasted_iota(jnp.int32, low_shape, 1)
        side_sign = 1.0 - 2.0 * side
        low_real = jnp.zeros(low_shape, jnp.float32)
        low_imag = jnp.zeros(low_shape, jnp.float32)
        before = None
        for spin in range(side_spin):
            occupied = (lax.shift_right_logical(low_pos, spin) & 1).astype(jnp.float32)
            sign = 1.0 - 2.0 * occupied
            low_imag = low_imag - loss[spin] * occupied
            if spin > 0:
                low_real = low_real - bond[spin - 1] * (before * sign)
            before = sign
        low_real = low_real - bond[side_spin - 1] * side_sign * before
        low_real = low_real - bond[side_spin] * side_sign * core_sign
        low_imag = low_imag - side * loss[side_spin] - core_bit * loss[split_spin]
        for q in range(quarters):
            bits = [(q >> b) & 1 for b in range(SPINS - 1 - split_spin)]
            signs = [core_sign] + [1.0 - 2.0 * bit for bit in bits]
            real, imag = low_real, low_imag
            for b, bit in enumerate(bits):
                real = real - bond[split_spin + b] * (signs[b] * signs[b + 1])
                imag = imag - bit * loss[split_spin + 1 + b]
            diagonal[q, 0, side] = real
            diagonal[q, 1, side] = imag

    def window(ref, lead, part, s, side):
        return ref.at[(*lead, part, pl.ds(s * TILE, TILE), pl.ds(side * LANES, LANES))]

    def sums_copy(count, slot):
        return remote(
            own_sums.at[slot, pl.ds(0, 8 * count)],
            other_sums.at[slot, pl.ds(0, 8 * count)],
            sums_send.at[slot],
            sums_recv.at[slot],
            other,
        )

    def start_sums(values, slot):
        for k, value in enumerate(values):
            own_sums[slot, 8 * k : 8 * k + 8] = value
        sums_copy(len(values), slot).start()

    def finish_sums(count, slot):
        sums_copy(count, slot).wait()
        both = [ref[slot, : 8 * count] for ref in (own_sums, other_sums)]
        both = both[0] + both[1]
        return [jnp.sum(both[8 * k : 8 * k + 8]) for k in range(count)]

    def work_copy(slot, n):
        pair = (pl.ds(2 * (n // 2), 2), slice(None), pl.ds(n % 2 * half, half))
        return remote(
            work.at[(slot, *pair)],
            mate_work.at[(slot, *pair)],
            work_send.at[slot, n],
            work_recv.at[slot, n],
            other,
        )

    @pl.when(stays)
    def _():
        def keep(i, carry):
            rows = pl.multiple_of(i * SUB, SUB)
            landing[me, pl.ds(rows, SUB), :] = block[
                pl.ds(pl.multiple_of(core * piece_rows, piece_rows) + rows, SUB), :
            ]
            return carry

        lax.fori_loop(0, piece_rows // SUB, keep, 0)

    mate[1, pl.ds(2, 2)] = jnp.zeros((2, 2, BLOCK, BLOCK), jnp.float32)

    def arrival(chip):
        return remote(
            block.at[pl.ds(0, piece_rows)],
            landing.at[chip],
            gather_send.at[0],
            gather_recv.at[chip],
            other,
        )

    def forward(chip):
        return remote(
            landing.at[chip],
            mate_landing.at[chip],
            forward_send.at[chip],
            forward_recv.at[chip],
            other,
        )

    @pl.when(jnp.logical_not(stays))
    def _():
        arrival(me).wait_recv()

    def square(ref, q, acc):
        def add(i, acc):
            x = ref[q, pl.ds(pl.multiple_of(i * 128, 128), 128), :]
            return acc + fold(x * x)

        return lax.fori_loop(0, piece_rows // 128, add, acc)

    own_sq = zero_tile
    for flip_chip in range(quarters):
        q = me ^ flip_chip
        if flip_chip:
            arrival(q).wait_recv()
        forward(q).start()
        own_sq = square(landing, q, own_sq)
    mate_sq = zero_tile
    for flip_chip in range(quarters):
        q = me ^ flip_chip
        forward(q).wait()
        mate_sq = square(mate_landing, q, mate_sq)
    beta, inv_beta = scalar_sqrt(jnp.sum(own_sq + mate_sq))

    def put_split(q, part, s, side, x):
        for n, term in enumerate(split(x)):
            window(splits, (q, part), n, s, side)[...] = term

    def start_vector(q, carry):
        for s, side in tiles:
            for part in range(2):
                rows = pl.ds((side * BLOCK + s * TILE) * 2 + part, TILE, stride=2)
                x = landing[q, rows, :] * inv_beta
                window(basis, (0, q), part, s, side)[...] = x
                put_split(q, part, s, side, x)
                window(mate, (0, q), part, s, side)[...] = mate_landing[q, rows, :] * inv_beta
        return carry

    lax.fori_loop(0, quarters, start_vector, 0)

    high_fields = [fields[split_spin + 1 + b] * inv_unit for b in range(SPINS - 1 - split_spin)]

    def issue(q):
        for part in range(2):
            hi, lo = splits[q, part, 0], splits[q, part, 1]
            flips[q, part] = dot(
                jnp.concatenate([row_table[...], hi, lo, hi], axis=1),
                jnp.concatenate([hi, lo, hi, lane_table[...]], axis=0),
            )

    def pairing(v, w):
        return fold(v[0] * w[0] + v[1] * w[1]), fold(v[0] * w[1] - v[1] * w[0])

    def load(ref, lead, s, side):
        return [window(ref, lead, part, s, side)[...] for part in range(2)]

    def consume(j, pair, acc, before, norm, send):
        slot = j % 2
        for s, side in tiles:
            chosen = (2 * pair, 2 * pair + 1)
            x = [load(basis, (j, q), s, side) for q in chosen]
            for n, q in enumerate(chosen):
                made = load(flips, (q,), s, side)
                near = load(mate, (slot, q), s, side)
                cross = load(basis, (j, q ^ 2), s, side)
                f = [
                    made[part]
                    + near[part]
                    + high_fields[0] * x[1 - n][part]
                    + high_fields[1] * cross[part]
                    for part in range(2)
                ]
                dr = window(diagonal, (q, 0), side, s, 0)[...]
                di = window(diagonal, (q, 1), side, s, 0)[...]
                xr, xi = x[n]
                w = (dr * xr - di * xi - f[0], dr * xi + di * xr - f[1])
                more = pairing(x[n], w)
                if before:
                    more = more + pairing(load(basis, (j - 1, q), s, side), w)
                if norm:
                    more = more + (fold(w[0] * w[0] + w[1] * w[1]),)
                for m, value in enumerate(more):
                    acc[m] = acc[m] + value
                for part in range(2):
                    window(work, (slot, q), part, s, side)[...] = w[part]
            if send and side == 1 and (s + 1) % (half // TILE) == 0:
                work_copy(slot, 2 * pair + (s + 1) // (half // TILE) - 1).start()

    def take(q, w_ref, u_ref, slot, now, before, after, coeffs, inverse, both, own):
        for s, side in tiles:
            rr, ri = load(w_ref, (slot, q), s, side)
            for n, lead in enumerate([now, before] if both else [now]):
                vr, vi = load(u_ref, (lead, q), s, side)
                hr, hm = coeffs[2 * n], coeffs[2 * n + 1]
                rr = rr - (hr * vr - hm * vi)
                ri = ri - (hr * vi + hm * vr)
            for part, value in enumerate((rr * inverse, ri * inverse)):
                window(u_ref, (after, q), part, s, side)[...] = value
                if own:
                    put_split(q, part, s, side, value)

    def apply(j, first, last):
        slot = j % 2
        acc = [zero_tile] * (2 + 2 * (not first) + (not last))
        issue(2)
        issue(3)
        consume(j, 0, acc, not first, not last, not last)
        if not first:
            known = [scalars[j - 1, n] for n in range(6)]
            for n in range(2, 4):
                work_copy(1 - slot, n).wait()
            for q in range(2, 4):
                take(
                    q, mate_work, mate, 1 - slot, 1 - slot, slot, slot, known[:4], known[5],
                    True, False,
                )
        consume(j, 1, acc, not first, not last, False)
        return acc

    def rest_inner(j, count):
        slot = j % 2

        def one(k, carry):
            def add(q, acc):
                real, imag = acc
                for s, side in tiles:
                    v = load(basis, (k, q), s, side)
                    w = load(work, (slot, q), s, side)
                    more = pairing(v, w)
                    real, imag = real + more[0], imag + more[1]
                return real, imag

            real, imag = lax.fori_loop(0, quarters, add, (zero_tile, zero_tile))
            own_rest[j, k, 0] = real
            own_rest[j, k, 1] = imag
            return carry

        lax.fori_loop(0, count, one, 0)

    def step(j, first):
        slot = j % 2
        sums = apply(j, first, False)
        start_sums(sums, slot)
        for n in range(2, 4):
            work_copy(slot, n).start()
        if not first:
            rest_inner(j, j - 1)
        coeffs = finish_sums(len(sums), slot)
        left = coeffs[-1]
        for value in coeffs[:-1]:
            left = left - value * value
        norm, inv_norm = scalar_sqrt(left)
        for n in range(4):
            scalars[j, n] = coeffs[n] if n < len(coeffs) - 1 else jnp.float32(0.0)
        scalars[j, 4] = norm
        scalars[j, 5] = inv_norm
        for n in range(2):
            work_copy(slot, n).wait()
        for q in range(quarters):
            take(q, work, basis, slot, j, j - 1, j + 1, coeffs, inv_norm, not first, True)
            if q < 2:
                issue(q)
        for q in range(2):
            take(
                q, mate_work, mate, slot, slot, 1 - slot, 1 - slot, coeffs, inv_norm,
                not first, False,
            )

    final = KRYLOV - 1
    issue(0)
    issue(1)
    step(0, True)

    def later(j, carry):
        step(j, False)
        return carry

    lax.fori_loop(1, final, later, 0)
    rest_copy = remote(
        own_rest.at[pl.ds(0, final)],
        other_rest.at[pl.ds(0, final)],
        rest_sem.at[0],
        rest_sem.at[1],
        other,
    )
    last_copy = remote(
        own_rest.at[final], other_rest.at[final], rest_sem.at[2], rest_sem.at[3], other
    )
    rest_copy.start()
    start_sums(apply(final, False, True), final % 2)
    rest_inner(final, final - 1)
    last_copy.start()
    rest_copy.wait()
    sub = lax.broadcasted_iota(jnp.int32, (8, LANES), 0)
    lane = lax.broadcasted_iota(jnp.int32, (8, LANES), 1)

    def put(tile, where, value):
        return jnp.where(where, value, tile)

    gram = [jnp.where(sub == lane, 1.0, 0.0).astype(jnp.float32), zero_tile]
    projected = [zero_tile, zero_tile]
    column = {j: [zero_tile, zero_tile] for j in range(3)}
    across = {j: [zero_tile, zero_tile] for j in range(3)}
    for j in range(final):
        here = lane == j
        alpha = [scalars[j, 0], scalars[j, 1]]
        bravo = [scalars[j, 2], scalars[j, 3]]
        for part in range(2):
            projected[part] = put(projected[part], here & (sub == j), alpha[part])
            if j > 0:
                projected[part] = put(projected[part], here & (sub == j - 1), bravo[part])
        projected[0] = put(projected[0], here & (sub == j + 1), scalars[j, 4])
        if j < 2:
            continue
        down = [zero_tile, zero_tile]
        along = [zero_tile, zero_tile]
        for k in range(j - 1):
            for part in range(2):
                value = jnp.sum(own_rest[j, k, part] + other_rest[j, k, part])
                down[part] = put(down[part], sub == k, value)
                along[part] = put(along[part], lane == k, value)
        for made, new in ((column, down), (across, along)):
            for value, old in ((alpha, made[j]), (bravo, made[j - 1])):
                new[0] = new[0] - (value[0] * old[0] - value[1] * old[1])
                new[1] = new[1] - (value[0] * old[1] + value[1] * old[0])
            made[j + 1] = [part * scalars[j, 5] for part in new]
        gram[0] = gram[0] + jnp.where(lane == j + 1, column[j + 1][0], 0.0)
        gram[0] = gram[0] + jnp.where(sub == j + 1, across[j + 1][0], 0.0)
        gram[1] = gram[1] + jnp.where(lane == j + 1, column[j + 1][1], 0.0)
        gram[1] = gram[1] - jnp.where(sub == j + 1, across[j + 1][1], 0.0)

    near_targets = finish_sums(4, final % 2)
    last_copy.wait()
    targets = []
    for k in range(final - 1):
        for part in range(2):
            targets.append(jnp.sum(own_rest[final, k, part] + other_rest[final, k, part]))
    targets = targets + near_targets[2:4] + near_targets[:2]
    for k in range(KRYLOV):
        for part in range(2):
            gram[part] = put(gram[part], (lane == KRYLOV) & (sub == k), targets[2 * k + part])

    def column_of(tile, k):
        return jnp.broadcast_to(tile[:, k : k + 1], tile.shape)

    def row_of(tile, k):
        return jnp.broadcast_to(tile[k : k + 1, :], tile.shape)

    for p in range(KRYLOV):
        row = [row_of(tile, p) for tile in gram]
        factor = [column_of(tile, p) for tile in gram]
        inverse = 1.0 / row_of(factor[0], p)
        row = [tile * inverse for tile in row]
        less = (
            factor[0] * row[0] - factor[1] * row[1],
            factor[0] * row[1] + factor[1] * row[0],
        )
        gram = [jnp.where(sub == p, row[n], gram[n] - less[n]) for n in range(2)]
    for part in range(2):
        projected[part] = put(projected[part], lane == final, column_of(gram[part], KRYLOV))

    def product(a, b):
        real, imag = zero_tile, zero_tile
        for k in range(KRYLOV):
            ar, ai = column_of(a[0], k), column_of(a[1], k)
            br, bi = row_of(b[0], k), row_of(b[1], k)
            real = real + (ar * br - ai * bi)
            imag = imag + (ar * bi + ai * br)
        return real, imag

    inside = lane < KRYLOV
    pace = unit * (time_step / 2.0**squarings)
    first = (
        jnp.where(inside, projected[1] * pace, 0.0),
        jnp.where(inside, projected[0] * -pace, 0.0),
    )
    second = product(first, first)
    third = product(second, first)
    identity = jnp.where(sub == lane, 1.0, 0.0).astype(jnp.float32)
    series = None
    for low in range(taylor_order // 3 * 3, -1, -3):
        terms = [identity * (1.0 / math.factorial(low)), zero_tile]
        for n, power in ((low + 1, first), (low + 2, second)):
            if n <= taylor_order:
                terms = [t + p * (1.0 / math.factorial(n)) for t, p in zip(terms, power)]
        if series is not None:
            terms = [t + p for t, p in zip(terms, product(third, series))]
        series = terms
    for repeat in range(squarings):
        series = product(series, series)
    weights = [
        jnp.sum(jnp.where((sub == k) & (lane == 0), tile * beta, 0.0))
        for tile in series
        for k in range(KRYLOV)
    ]
    channel_copy.wait()
    channel = jnp.where(stays, own_channel[...], other_channel[...])
    sub_pos = lax.broadcasted_iota(jnp.int32, (TILE, LANES), 0) * LANES
    sub_pos = sub_pos + lax.broadcasted_iota(jnp.int32, (TILE, LANES), 1)

    def combine(q, acc):
        high = (core << split_spin) + (q << (split_spin + 1))
        for s, side in tiles:
            pr = jnp.zeros((TILE, LANES), jnp.float32)
            pi = jnp.zeros((TILE, LANES), jnp.float32)
            for k in range(KRYLOV):
                vr = window(basis, (k, q), 0, s, side)[...]
                vi = window(basis, (k, q), 1, s, side)[...]
                cr, ci = weights[k], weights[k + KRYLOV]
                pr = pr + (cr * vr - ci * vi)
                pi = pi + (cr * vi + ci * vr)
            window(work, (0, q), 0, s, side)[...] = pr
            window(work, (0, q), 1, s, side)[...] = pi
            position = sub_pos + (high + (side << side_spin) + s * TILE * LANES)
            occupied = lax.shift_right_logical(position, channel) & 1
            acc = acc + fold(jnp.where(occupied == 1, pr * pr + pi * pi, 0.0))
        return acc

    jumped_sq = lax.fori_loop(0, quarters, combine, zero_tile)

    start_sums([jumped_sq], 0)

    def pack(target, q, part):
        for s, side in tiles:
            value = window(work, (0, q), part, s, side)[...]
            for b in range(SPINS - 1 - split_spin):
                flipped = window(work, (0, q | (1 << b)), part, s, side)[...]
                value = jnp.where(channel == split_spin + 1 + b, flipped, value)
            target[s * TILE : (s + 1) * TILE, side * LANES : (side + 1) * LANES] = value

    parcels = []
    for part in range(2):
        q = me ^ (1 << part)
        pack(parcel.at[part], q, part)
        copy = remote(
            parcel.at[part],
            pieces.at[core, part],
            parcel_send.at[part],
            parcel_recv.at[core, part],
            device(held, q),
        )
        copy.start()
        parcels.append(copy)
    for part in range(2):
        pack(parcel.at[2 + part], me, part)
    home = remote(
        parcel.at[pl.ds(2, 2)], pieces.at[core], parcel_send.at[2], parcel_recv.at[2, 0], other
    )

    @pl.when(jnp.logical_not(stays))
    def _():
        home.start()

    @pl.when(stays)
    def _():
        for part in range(2):
            pieces[core, part] = parcel[2 + part]

    all_sq = finish_sums(1, 0)[0]
    size = jnp.float32(quarters * 2 * piece_rows // 2 * LANES)
    ratio = jnp.where(channel[:8] < SPINS, size / jnp.full((8, LANES), all_sq, jnp.float32), 1.0)
    own_scale = jnp.sqrt(ratio)
    own_sums[1, 0:8] = own_scale
    scale_copy = remote(
        own_sums.at[1, pl.ds(0, 8)], scale_out, scale_sem.at[0], scale_sem.at[1],
        device(core, me ^ 1),
    )

    @pl.when(stays)
    def _():
        scale_copy.start()
        scale_out[...] = own_scale
        remote(
            parcel.at[pl.ds(2, 2)], pieces.at[1 - core], parcel_send.at[2],
            parcel_recv.at[2, 0], other,
        ).wait_recv()
        scale_copy.wait_send()

    @pl.when(jnp.logical_not(stays))
    def _():
        for sender in range(2):
            for part in range(2):
                remote(
                    parcel.at[part], pieces.at[sender, part], parcel_send.at[part],
                    parcel_recv.at[sender, part], other,
                ).wait_recv()
        scale_copy.wait_recv()
        home.wait_send()
        piece(core, near_chip, 3).wait_send()

    for copy in parcels:
        copy.wait_send()
    for send in sends:
        send.wait_send()


def lower_kernel(channel_ref, pieces, scale, out):
    channel = channel_ref[0]
    me = lax.axis_index("amp")
    side_spin = LANE_BITS + BLOCK_BITS
    in_lanes = channel < LANE_BITS
    in_rows = jnp.logical_not(in_lanes) & (channel < side_spin)
    lane_shift = jnp.where(in_lanes, lax.shift_left(1, channel), 0)
    row_shift = jnp.where(in_rows, lax.shift_left(1, jnp.maximum(channel - LANE_BITS, 0)), 0)
    near = jnp.where(row_shift < 8, row_shift, 0)
    far = jnp.where(row_shift < 8, 0, row_shift)
    lane_turn = (LANES - lane_shift) % LANES
    row_turn = (8 - near) % 8
    sub_pos = lax.broadcasted_iota(jnp.int32, (8, LANES), 0) * LANES
    sub_pos = sub_pos + lax.broadcasted_iota(jnp.int32, (8, LANES), 1)
    own = me * (4 * BLOCK * LANES)
    factor = scale[...]

    for half in range(2):
        from_half = jnp.where(channel == side_spin + 1, 1, half)
        for side in range(2):
            from_side = jnp.where(channel == side_spin, 1, side)
            columns = pl.ds(pl.multiple_of(from_side * LANES, LANES), LANES)

            def lower(i, carry, half=half, side=side, from_half=from_half, columns=columns):
                for t in range(8):
                    local = i * 64 + t * 8
                    base = (half * 2 + side) * BLOCK + local
                    rows = pl.ds(pl.multiple_of(local | far, 8), 8)
                    position = sub_pos + (own + base * LANES)
                    vacant = (lax.shift_right_logical(position, channel) & 1) == 0
                    for part in range(2):
                        x = pieces[from_half, part, rows, columns]
                        x = pltpu.roll(x, row_turn, 0)
                        x = pltpu.roll(x, lane_turn, 1)
                        x = jnp.where(vacant, x * factor, 0.0)
                        out[pl.ds(base * 2 + part, 8, stride=2), :] = x
                return carry

            lax.fori_loop(0, BLOCK // 64, lower, 0)


def paired_body(amplitudes, couplings, fields, decays, channel):
    quarters = lax.axis_size("amp")
    local_len = amplitudes.shape[2]
    block_rows = local_len // LANES
    vmem = pl.BlockSpec(memory_space=pltpu.VMEM)
    smem = pl.BlockSpec(memory_space=pltpu.SMEM)
    f32 = jnp.float32
    dma = pltpu.SemaphoreType.DMA
    sums_rows = 8 * (2 * KRYLOV + 1)
    state = amplitudes.reshape(2, block_rows, LANES).transpose(1, 0, 2)
    state = state.reshape(2 * block_rows, LANES)
    pieces, scale = pl.pallas_call(
        pair_kernel,
        out_shape=(
            jax.ShapeDtypeStruct((2, 2, BLOCK, BLOCK), f32),
            jax.ShapeDtypeStruct((8, LANES), f32),
        ),
        in_specs=[smem] * 4 + [vmem],
        out_specs=(vmem, vmem),
        scratch_shapes=[
            pltpu.VMEM((quarters, block_rows, LANES), f32),
            pltpu.VMEM((quarters, block_rows, LANES), f32),
            pltpu.VMEM((KRYLOV, quarters, 2, BLOCK, BLOCK), f32),
            pltpu.VMEM((2, quarters, 2, BLOCK, BLOCK), f32),
            pltpu.VMEM((2, quarters, 2, BLOCK, BLOCK), f32),
            pltpu.VMEM((2, quarters, 2, BLOCK, BLOCK), f32),
            pltpu.VMEM((quarters, 2, BLOCK, BLOCK), f32),
            pltpu.VMEM((quarters, 2, 2, BLOCK, BLOCK), jnp.bfloat16),
            pltpu.VMEM((BLOCK, 3 * BLOCK), jnp.bfloat16),
            pltpu.VMEM((3 * BLOCK, BLOCK), jnp.bfloat16),
            pltpu.VMEM((quarters, 2, 2, BLOCK, LANES), f32),
            pltpu.VMEM((2, sums_rows, LANES), f32),
            pltpu.VMEM((2, sums_rows, LANES), f32),
            pltpu.VMEM((KRYLOV, KRYLOV - 2, 2, 8, LANES), f32),
            pltpu.VMEM((KRYLOV, KRYLOV - 2, 2, 8, LANES), f32),
            pltpu.SMEM((KRYLOV - 1, 6), f32),
            pltpu.VMEM((TILE, LANES), jnp.int32),
            pltpu.VMEM((TILE, LANES), jnp.int32),
            pltpu.VMEM((4, BLOCK, BLOCK), f32),
            dma((4,)),
            dma((quarters,)),
            dma((quarters,)),
            dma((quarters,)),
            dma((2,)),
            dma((2,)),
            dma((4,)),
            dma((2, quarters)),
            dma((2, quarters)),
            dma((2,)),
            dma((3,)),
            dma((3, 2)),
            dma((2,)),
        ],
        compiler_params=pltpu.CompilerParams(
            collective_id=1, has_side_effects=True, vmem_limit_bytes=62 * 1024 * 1024
        ),
        name="pair",
    )(channel, couplings, fields, decays, state)
    lowered = pl.pallas_call(
        lower_kernel,
        out_shape=jax.ShapeDtypeStruct((2 * block_rows, LANES), f32),
        in_specs=[smem, vmem, vmem],
        out_specs=vmem,
        name="lower",
    )(channel, pieces, scale)
    lowered = lowered.reshape(block_rows, 2, LANES).transpose(1, 0, 2)
    return lowered.reshape(amplitudes.shape)


def solution(mesh):
    placed = (P("traj", None, "amp"), P(), P(), P(), P("traj"))

    def step(amplitudes, *rest):
        trajectories = mesh.shape["traj"]
        low_rows = amplitudes.shape[2] // mesh.shape["amp"] // LANES
        paired = (
            mesh.shape["amp"] == 4
            and trajectories % 2 == 0
            and amplitudes.shape[0] == trajectories
            and low_rows == 4 * BLOCK
        )
        return jax.shard_map(
            paired_body if paired else body,
            mesh=mesh,
            in_specs=placed,
            out_specs=P("traj", None, "amp"),
            check_vma=False,
        )(amplitudes, *rest)

    return step
```

```python
import math

import jax
import jax.numpy as jnp
from jax import lax
from jax.experimental import pallas as pl
from jax.experimental.pallas import tpu as pltpu
from jax.sharding import PartitionSpec as P

SPINS = 19
KRYLOV = 8
LANES = 128
LANE_BITS = 7

time_step = 0.7
squarings = 8
taylor_order = 10
highest = lax.Precision.HIGHEST

CHUNK_BITS = 8
CHUNK = 1 << CHUNK_BITS
SUB = 32


def split(x):
    hi = x.astype(jnp.bfloat16)
    lo = (x - hi.astype(jnp.float32)).astype(jnp.bfloat16)
    return hi, lo


def dot(a, b):
    return jnp.dot(a, b, preferred_element_type=jnp.float32)


def fold(x):
    return jnp.sum(x.reshape(x.shape[0] // 8, 8, x.shape[1]), axis=0)


def scalar_sqrt(value):
    root = jnp.sqrt(jnp.full((8, LANES), value, jnp.float32))
    return jnp.max(root), jnp.max(1.0 / root)


def krylov_weights(a_matrix):
    size = a_matrix.shape[0]
    pad = jnp.zeros((LANES - size, LANES), jnp.float32)
    scaled = jnp.concatenate([a_matrix, pad], axis=0) * (1.0 / 2.0**squarings)
    rows = lax.broadcasted_iota(jnp.int32, (LANES, LANES), 0)
    cols = lax.broadcasted_iota(jnp.int32, (LANES, LANES), 1)
    identity = jnp.where(rows == cols, 1.0, 0.0).astype(jnp.float32)
    series = identity
    for degree in range(taylor_order, 0, -1):
        product = jnp.dot(
            scaled, series, precision=highest, preferred_element_type=jnp.float32
        )
        series = identity + product * (1.0 / degree)
    for repeat in range(squarings):
        series = jnp.dot(
            series, series, precision=highest, preferred_element_type=jnp.float32
        )
    return series


def kernel(
    channel_ref,
    couplings,
    fields,
    decays,
    state,
    out,
    basis,
    work,
    flips,
    row_table,
    lane_table,
    diag_low,
):
    node_count, _, block_rows, _ = state.shape
    rows = node_count * block_rows
    chunks = rows // CHUNK
    subs = CHUNK // SUB
    channel = channel_ref[0]
    device = lax.axis_index("amp")
    zero_tile = jnp.zeros((8, LANES), jnp.float32)
    per_block = block_rows // CHUNK

    table_shape = (CHUNK, CHUNK)
    crossed = lax.broadcasted_iota(jnp.int32, table_shape, 0)
    crossed = crossed ^ lax.broadcasted_iota(jnp.int32, table_shape, 1)
    for table, first_spin, bits in (
        (row_table, LANE_BITS, CHUNK_BITS),
        (lane_table, 0, LANE_BITS),
    ):
        value = jnp.zeros(table_shape, jnp.float32)
        for bit in range(bits):
            value = jnp.where(crossed == 1 << bit, fields[first_spin + bit], value)
        table[0], table[1] = split(value)

    low_shape = (CHUNK, LANES)
    low_pos = lax.broadcasted_iota(jnp.int32, low_shape, 0) * LANES
    low_pos = low_pos + lax.broadcasted_iota(jnp.int32, low_shape, 1)
    low_bits = LANE_BITS + CHUNK_BITS
    before = None
    low_real = jnp.zeros(low_shape, jnp.float32)
    low_imag = jnp.zeros(low_shape, jnp.float32)
    for spin in range(low_bits):
        occupied = (lax.shift_right_logical(low_pos, spin) & 1).astype(jnp.float32)
        sign = 1.0 - 2.0 * occupied
        low_imag = low_imag - 0.5 * decays[spin] * occupied
        if spin > 0:
            low_real = low_real - couplings[spin - 1] * (before * sign)
        before = sign
    diag_low[0] = low_real
    diag_low[1] = low_imag

    def high_diagonal(i):
        bits = [
            (lax.shift_right_logical(i, b) & 1).astype(jnp.float32)
            for b in range(SPINS - low_bits)
        ]
        signs = [1.0 - 2.0 * bit for bit in bits]
        real = jnp.float32(0.0)
        imag = jnp.float32(0.0)
        for b in range(len(bits)):
            imag = imag - 0.5 * decays[low_bits + b] * bits[b]
            if b > 0:
                real = real - couplings[low_bits + b - 1] * signs[b - 1] * signs[b]
        edge = couplings[low_bits - 1] * signs[0]
        return real - edge, real + edge, imag

    def start_norm(i, acc):
        node = i // per_block
        first = (i % per_block) * CHUNK
        for part in range(2):
            x = state[node, part, pl.ds(first, CHUNK), :]
            acc = acc + fold(x * x)
        return acc

    start_sq = jnp.sum(lax.fori_loop(0, chunks, start_norm, zero_tile))
    beta, inv_beta = scalar_sqrt(start_sq)

    def start_vector(i, carry):
        node = i // per_block
        first = (i % per_block) * CHUNK
        for part in range(2):
            basis[0, pl.ds(i * CHUNK, CHUNK), part * LANES : (part + 1) * LANES] = (
                state[node, part, pl.ds(first, CHUNK), :] * inv_beta
            )
        return carry

    lax.fori_loop(0, chunks, start_vector, 0)

    mat_rows = lax.broadcasted_iota(jnp.int32, (2 * KRYLOV, LANES), 0)
    mat_cols = lax.broadcasted_iota(jnp.int32, (2 * KRYLOV, LANES), 1)
    a_matrix = jnp.zeros((2 * KRYLOV, LANES), jnp.float32)

    def put(matrix, k, j, real, imag):
        a_real = time_step * imag
        a_imag = -time_step * real
        for r, c, value in (
            (k, j, a_real),
            (k, j + KRYLOV, -a_imag),
            (k + KRYLOV, j, a_imag),
            (k + KRYLOV, j + KRYLOV, a_real),
        ):
            matrix = jnp.where((mat_rows == r) & (mat_cols == c), value, matrix)
        return matrix

    high_fields = [
        fields[LANE_BITS + CHUNK_BITS + b] for b in range(SPINS - LANE_BITS - CHUNK_BITS)
    ]

    for j in range(KRYLOV):
        last = j + 1 == KRYLOV

        def apply_chunk(i, acc, j=j):
            base = pl.multiple_of(i * CHUNK, CHUNK)
            hi, lo = split(basis[j, pl.ds(base, CHUNK), :])
            flips[...] = (
                dot(row_table[0], hi)
                + dot(row_table[1], hi)
                + dot(row_table[0], lo)
                + dot(hi, lane_table[0])
                + dot(lo, lane_table[0])
                + dot(hi, lane_table[1])
            )
            acc = list(acc)
            real_vacant, real_occupied, imag_high = high_diagonal(i)
            for s in range(subs):
                here = pl.ds(base + s * SUB, SUB)
                x = basis[j, here, :]
                f = flips[s * SUB : (s + 1) * SUB, :]
                for b, field in enumerate(high_fields):
                    there = pl.multiple_of((i ^ (1 << b)) * CHUNK, CHUNK)
                    f = f + field * basis[j, pl.ds(there + s * SUB, SUB), :]
                part = slice(s * SUB, (s + 1) * SUB)
                dr = diag_low[0, part, :] + (real_vacant if s < subs // 2 else real_occupied)
                di = diag_low[1, part, :] + imag_high
                xr, xi = x[:, :LANES], x[:, LANES:]
                wr = dr * xr - di * xi - f[:, :LANES]
                wi = dr * xi + di * xr - f[:, LANES:]
                work[here, :LANES] = wr
                work[here, LANES:] = wi
                for k in range(j + 1):
                    vr = basis[k, here, :LANES]
                    vi = basis[k, here, LANES:]
                    acc[2 * k] = acc[2 * k] + fold(vr * wr + vi * wi)
                    acc[2 * k + 1] = acc[2 * k + 1] + fold(vr * wi - vi * wr)
                acc[-1] = acc[-1] + fold(wr * wr + wi * wi)
            return tuple(acc)

        sums = lax.fori_loop(0, chunks, apply_chunk, (zero_tile,) * (2 * j + 3))
        coeffs = [jnp.sum(t) for t in sums]
        for k in range(j + 1):
            a_matrix = put(a_matrix, k, j, coeffs[2 * k], coeffs[2 * k + 1])
        if last:
            break
        left = coeffs[-1]
        for value in coeffs[:-1]:
            left = left - value * value
        norm, inv_norm = scalar_sqrt(left)
        a_matrix = put(a_matrix, j + 1, j, norm, jnp.float32(0.0))

        def subtract_chunk(i, carry, j=j, coeffs=coeffs, inv_norm=inv_norm):
            base = pl.multiple_of(i * CHUNK, CHUNK)
            for s in range(subs):
                here = pl.ds(base + s * SUB, SUB)
                rr = work[here, :LANES]
                ri = work[here, LANES:]
                for k in range(j + 1):
                    vr = basis[k, here, :LANES]
                    vi = basis[k, here, LANES:]
                    hr, hm = coeffs[2 * k], coeffs[2 * k + 1]
                    rr = rr - (hr * vr - hm * vi)
                    ri = ri - (hr * vi + hm * vr)
                basis[j + 1, here, :LANES] = rr * inv_norm
                basis[j + 1, here, LANES:] = ri * inv_norm
            return carry

        lax.fori_loop(0, chunks, subtract_chunk, 0)

    series = krylov_weights(a_matrix)
    first = series[: 2 * KRYLOV, :] * beta
    weights = [
        jnp.sum(jnp.where((mat_rows == k) & (mat_cols == 0), first, 0.0))
        for k in range(2 * KRYLOV)
    ]
    sub_pos = lax.broadcasted_iota(jnp.int32, (SUB, LANES), 0) * LANES
    sub_pos = sub_pos + lax.broadcasted_iota(jnp.int32, (SUB, LANES), 1)

    def combine(i, acc):
        base = pl.multiple_of(i * CHUNK, CHUNK)
        for s in range(subs):
            here = pl.ds(base + s * SUB, SUB)
            pr = jnp.zeros((SUB, LANES), jnp.float32)
            pi = jnp.zeros((SUB, LANES), jnp.float32)
            for k in range(KRYLOV):
                vr = basis[k, here, :LANES]
                vi = basis[k, here, LANES:]
                cr, ci = weights[k], weights[k + KRYLOV]
                pr = pr + (cr * vr - ci * vi)
                pi = pi + (cr * vi + ci * vr)
            work[here, :LANES] = pr
            work[here, LANES:] = pi
            position = sub_pos + (base + s * SUB) * LANES
            occupied = lax.shift_right_logical(position, channel) & 1
            acc = acc + fold(jnp.where(occupied == 1, pr * pr + pi * pi, 0.0))
        return acc

    total = jnp.sum(lax.fori_loop(0, chunks, combine, zero_tile))
    jumped = channel < SPINS
    size = jnp.float32(rows * LANES)
    total = jnp.where(jumped, total, size)
    root = jnp.sqrt(size / jnp.full((8, LANES), total, jnp.float32))
    scale = jnp.max(root)
    in_lanes = channel < LANE_BITS
    lane_shift = jnp.where(in_lanes, lax.shift_left(1, channel), 0)
    row_shift = jnp.where(
        in_lanes | (channel >= SPINS),
        0,
        lax.shift_left(1, jnp.maximum(channel - LANE_BITS, 0)),
    )
    in_sublanes = row_shift < 8
    near = jnp.where(in_sublanes, row_shift, 0)
    far = jnp.where(in_sublanes, 0, row_shift)
    lane_turn = (LANES - lane_shift) % LANES
    row_turn = (SUB - near) % SUB

    def jump(i, carry):
        local = pl.multiple_of(i * SUB, SUB)
        base = device * block_rows + local
        source = pl.multiple_of(base + far, 8)
        position = sub_pos + base * LANES
        vacant = (lax.shift_right_logical(position, channel) & 1) == 0
        for part in range(2):
            x = work[pl.ds(source, SUB), part * LANES : (part + 1) * LANES]
            x = pltpu.roll(x, row_turn, 0)
            x = pltpu.roll(x, lane_turn, 1)
            out[part, pl.ds(local, SUB), :] = jnp.where(vacant, x * scale, 0.0)
        return carry

    lax.fori_loop(0, block_rows // SUB, jump, 0)


def gather_kernel(block, out, send_sem, recv_sem):
    me = lax.axis_index("amp")
    near = (me ^ 1, me ^ 2)
    barrier = pltpu.get_barrier_semaphore()
    for partner in near:
        pl.semaphore_signal(
            barrier, inc=1, device_id={"amp": partner}, device_id_type=pl.DeviceIdType.MESH
        )
    pl.semaphore_wait(barrier, 2)

    def copy(source, owner, part, axis, slot):
        return pltpu.make_async_remote_copy(
            src_ref=source,
            dst_ref=out.at[owner, part],
            send_sem=send_sem.at[slot],
            recv_sem=recv_sem.at[slot],
            device_id={"amp": near[axis]},
            device_id_type=pl.DeviceIdType.MESH,
        )

    direct = {}
    for turn in range(2):
        for axis in range(2):
            part = axis ^ turn
            direct[axis, part] = copy(block.at[part], me, part, axis, 2 * axis + part)
            direct[axis, part].start()
    out[me] = block[...]
    forwards = []
    for axis in range(2):
        direct[axis, axis].wait_recv()
        owner = near[axis]
        forward = copy(out.at[owner, axis], owner, axis, 1 - axis, 4 + axis)
        forward.start()
        forwards.append(forward)
    for axis in range(2):
        direct[axis, 1 - axis].wait_recv()
    for forward in forwards:
        forward.wait_recv()
    for sent in list(direct.values()) + forwards:
        sent.wait_send()


def gather(block):
    node_count = lax.axis_size("amp")
    if node_count != 4:
        return lax.all_gather(block, "amp")
    vmem = pl.BlockSpec(memory_space=pltpu.VMEM)
    return pl.pallas_call(
        gather_kernel,
        out_shape=jax.ShapeDtypeStruct((node_count,) + block.shape, block.dtype),
        in_specs=[vmem],
        out_specs=vmem,
        scratch_shapes=[pltpu.SemaphoreType.DMA((6,)), pltpu.SemaphoreType.DMA((6,))],
        compiler_params=pltpu.CompilerParams(collective_id=0, has_side_effects=True),
        name="gather",
    )(block)


def body(amplitudes, couplings, fields, decays, channel):
    node_count = lax.axis_size("amp")
    local_len = amplitudes.shape[2]
    block_rows = local_len // LANES
    rows = node_count * block_rows
    vmem = pl.BlockSpec(memory_space=pltpu.VMEM)
    smem = pl.BlockSpec(memory_space=pltpu.SMEM)
    call = pl.pallas_call(
        kernel,
        out_shape=jax.ShapeDtypeStruct((2, block_rows, LANES), jnp.float32),
        in_specs=[smem] * 4 + [vmem],
        out_specs=vmem,
        scratch_shapes=[
            pltpu.VMEM((KRYLOV, rows, 2 * LANES), jnp.float32),
            pltpu.VMEM((rows + rows // 2, 2 * LANES), jnp.float32),
            pltpu.VMEM((CHUNK, 2 * LANES), jnp.float32),
            pltpu.VMEM((2, CHUNK, CHUNK), jnp.bfloat16),
            pltpu.VMEM((2, CHUNK, CHUNK), jnp.bfloat16),
            pltpu.VMEM((2, CHUNK, LANES), jnp.float32),
        ],
        compiler_params=pltpu.CompilerParams(vmem_limit_bytes=62 * 1024 * 1024),
        name="trajectory",
    )
    results = []
    for t in range(amplitudes.shape[0]):
        block = amplitudes[t].reshape(2, block_rows, LANES)
        state = gather(block)
        results.append(call(channel[t : t + 1], couplings, fields, decays, state))
    return jnp.stack(results).reshape(amplitudes.shape)


BLOCK = 256
BLOCK_BITS = 8
TILE = 16


def pair_kernel(
    channel_ref,
    couplings,
    fields,
    decays,
    block,
    pieces,
    scale_out,
    landing,
    mate_landing,
    basis,
    mate,
    work,
    mate_work,
    flips,
    splits,
    row_table,
    lane_table,
    diagonal,
    own_sums,
    other_sums,
    own_rest,
    other_rest,
    scalars,
    own_channel,
    other_channel,
    parcel,
    gather_send,
    gather_recv,
    forward_send,
    forward_recv,
    sums_send,
    sums_recv,
    rest_sem,
    work_send,
    work_recv,
    channel_sem,
    parcel_send,
    parcel_recv,
    scale_sem,
):
    quarters = landing.shape[0]
    piece_rows = landing.shape[1]
    traj = lax.axis_index("traj")
    me = lax.axis_index("amp")
    core = traj & 1
    first_traj = traj - core
    held = (me ^ (me >> 1)) & 1
    stays = core == held
    split_spin = LANE_BITS + BLOCK_BITS + 1
    side_spin = split_spin - 1
    zero_tile = jnp.zeros((8, LANES), jnp.float32)
    tiles = [(s, side) for s in range(BLOCK // TILE) for side in range(2)]
    half = BLOCK // 2

    def device(core_index, chip):
        return {"traj": first_traj + core_index, "amp": chip}

    def remote(source, target, send, recv, where):
        return pltpu.make_async_remote_copy(
            src_ref=source,
            dst_ref=target,
            send_sem=send,
            recv_sem=recv,
            device_id=where,
            device_id_type=pl.DeviceIdType.MESH,
        )

    other = device(1 - core, me)
    barrier = pltpu.get_barrier_semaphore()
    for flip_core in range(2):
        for flip_chip in range(quarters):
            if flip_core or flip_chip:
                pl.semaphore_signal(
                    barrier,
                    inc=1,
                    device_id=device(core ^ flip_core, me ^ flip_chip),
                    device_id_type=pl.DeviceIdType.MESH,
                )
    own_channel[...] = jnp.full(own_channel.shape, channel_ref[0], jnp.int32)
    pl.semaphore_wait(barrier, 2 * quarters - 1)

    near_chip = me ^ (held ^ core)
    far_chip = near_chip ^ 3

    def piece(core_index, chip, slot):
        source = block.at[pl.ds(pl.multiple_of(core_index * piece_rows, piece_rows), piece_rows)]
        return remote(
            source,
            landing.at[me],
            gather_send.at[slot],
            gather_recv.at[me],
            device(core_index, chip),
        )

    sends = [piece(core, far_chip, 0), piece(1 - core, far_chip, 1), piece(1 - core, near_chip, 2)]
    for send in sends:
        send.start()

    @pl.when(jnp.logical_not(stays))
    def _():
        piece(core, near_chip, 3).start()

    channel_copy = remote(
        own_channel, other_channel, channel_sem.at[0], channel_sem.at[1], other
    )
    channel_copy.start()

    unit = fields[split_spin]
    inv_unit = jnp.max(1.0 / jnp.full((8, LANES), unit, jnp.float32))
    crossed = lax.broadcasted_iota(jnp.int32, (BLOCK, BLOCK), 0)
    crossed = crossed ^ lax.broadcasted_iota(jnp.int32, (BLOCK, BLOCK), 1)
    for table, spins, axis in (
        (row_table, [LANE_BITS + b for b in range(BLOCK_BITS)], 1),
        (lane_table, [*range(LANE_BITS), side_spin], 0),
    ):
        value = jnp.zeros((BLOCK, BLOCK), jnp.float32)
        for bit, spin in enumerate(spins):
            value = jnp.where(crossed == 1 << bit, fields[spin] * inv_unit, value)
        hi, lo = split(value)
        table[...] = jnp.concatenate([hi, hi, lo], axis=axis)

    core_bit = core.astype(jnp.float32)
    core_sign = 1.0 - 2.0 * core_bit
    bond = [couplings[spin] * inv_unit for spin in range(SPINS - 1)]
    loss = [0.5 * decays[spin] * inv_unit for spin in range(SPINS)]
    for side in range(2):
        low_shape = (BLOCK, LANES)
        low_pos = lax.broadcasted_iota(jnp.int32, low_shape, 0) * LANES
        low_pos = low_pos + lax.broadcasted_iota(jnp.int32, low_shape, 1)
        side_sign = 1.0 - 2.0 * side
        low_real = jnp.zeros(low_shape, jnp.float32)
        low_imag = jnp.zeros(low_shape, jnp.float32)
        before = None
        for spin in range(side_spin):
            occupied = (lax.shift_right_logical(low_pos, spin) & 1).astype(jnp.float32)
            sign = 1.0 - 2.0 * occupied
            low_imag = low_imag - loss[spin] * occupied
            if spin > 0:
                low_real = low_real - bond[spin - 1] * (before * sign)
            before = sign
        low_real = low_real - bond[side_spin - 1] * side_sign * before
        low_real = low_real - bond[side_spin] * side_sign * core_sign
        low_imag = low_imag - side * loss[side_spin] - core_bit * loss[split_spin]
        for q in range(quarters):
            bits = [(q >> b) & 1 for b in range(SPINS - 1 - split_spin)]
            signs = [core_sign] + [1.0 - 2.0 * bit for bit in bits]
            real, imag = low_real, low_imag
            for b, bit in enumerate(bits):
                real = real - bond[split_spin + b] * (signs[b] * signs[b + 1])
                imag = imag - bit * loss[split_spin + 1 + b]
            diagonal[q, 0, side] = real
            diagonal[q, 1, side] = imag

    def window(ref, lead, part, s, side):
        return ref.at[(*lead, part, pl.ds(s * TILE, TILE), pl.ds(side * LANES, LANES))]

    def sums_copy(count, slot):
        return remote(
            own_sums.at[slot, pl.ds(0, 8 * count)],
            other_sums.at[slot, pl.ds(0, 8 * count)],
            sums_send.at[slot],
            sums_recv.at[slot],
            other,
        )

    def start_sums(values, slot):
        for k, value in enumerate(values):
            own_sums[slot, 8 * k : 8 * k + 8] = value
        sums_copy(len(values), slot).start()

    def finish_sums(count, slot):
        sums_copy(count, slot).wait()
        both = [ref[slot, : 8 * count] for ref in (own_sums, other_sums)]
        both = both[0] + both[1]
        return [jnp.sum(both[8 * k : 8 * k + 8]) for k in range(count)]

    def work_copy(slot, n):
        pair = (pl.ds(2 * (n // 2), 2), slice(None), pl.ds(n % 2 * half, half))
        return remote(
            work.at[(slot, *pair)],
            mate_work.at[(slot, *pair)],
            work_send.at[slot, n],
            work_recv.at[slot, n],
            other,
        )

    @pl.when(stays)
    def _():
        def keep(i, carry):
            rows = pl.multiple_of(i * SUB, SUB)
            landing[me, pl.ds(rows, SUB), :] = block[
                pl.ds(pl.multiple_of(core * piece_rows, piece_rows) + rows, SUB), :
            ]
            return carry

        lax.fori_loop(0, piece_rows // SUB, keep, 0)

    mate[1, pl.ds(2, 2)] = jnp.zeros((2, 2, BLOCK, BLOCK), jnp.float32)

    def arrival(chip):
        return remote(
            block.at[pl.ds(0, piece_rows)],
            landing.at[chip],
            gather_send.at[0],
            gather_recv.at[chip],
            other,
        )

    def forward(chip):
        return remote(
            landing.at[chip],
            mate_landing.at[chip],
            forward_send.at[chip],
            forward_recv.at[chip],
            other,
        )

    @pl.when(jnp.logical_not(stays))
    def _():
        arrival(me).wait_recv()

    def square(ref, q, acc):
        def add(i, acc):
            x = ref[q, pl.ds(pl.multiple_of(i * 128, 128), 128), :]
            return acc + fold(x * x)

        return lax.fori_loop(0, piece_rows // 128, add, acc)

    own_sq = zero_tile
    for flip_chip in range(quarters):
        q = me ^ flip_chip
        if flip_chip:
            arrival(q).wait_recv()
        forward(q).start()
        own_sq = square(landing, q, own_sq)
    mate_sq = zero_tile
    for flip_chip in range(quarters):
        q = me ^ flip_chip
        forward(q).wait()
        mate_sq = square(mate_landing, q, mate_sq)
    beta, inv_beta = scalar_sqrt(jnp.sum(own_sq + mate_sq))

    def put_split(q, part, s, side, x):
        for n, term in enumerate(split(x)):
            window(splits, (q, part), n, s, side)[...] = term

    def start_vector(q, carry):
        for s, side in tiles:
            for part in range(2):
                rows = pl.ds((side * BLOCK + s * TILE) * 2 + part, TILE, stride=2)
                x = landing[q, rows, :] * inv_beta
                window(basis, (0, q), part, s, side)[...] = x
                put_split(q, part, s, side, x)
                window(mate, (0, q), part, s, side)[...] = mate_landing[q, rows, :] * inv_beta
        return carry

    lax.fori_loop(0, quarters, start_vector, 0)

    high_fields = [fields[split_spin + 1 + b] * inv_unit for b in range(SPINS - 1 - split_spin)]

    def issue(q, part):
        hi, lo = splits[q, part, 0], splits[q, part, 1]
        flips[q, part] = dot(
            jnp.concatenate([row_table[...], hi, lo, hi], axis=1),
            jnp.concatenate([hi, lo, hi, lane_table[...]], axis=0),
        )

    def pairing(v, w):
        return fold(v[0] * w[0] + v[1] * w[1]), fold(v[0] * w[1] - v[1] * w[0])

    def load(ref, lead, s, side):
        return [window(ref, lead, part, s, side)[...] for part in range(2)]

    def consume(j, pair, acc, before, norm, send, between=()):
        slot = j % 2
        for t, (s, side) in enumerate(tiles):
            if t % 8 == 0 and between:
                issue(*between[t // 8])
            chosen = (2 * pair, 2 * pair + 1)
            x = [load(basis, (j, q), s, side) for q in chosen]
            for n, q in enumerate(chosen):
                made = load(flips, (q,), s, side)
                near = load(mate, (slot, q), s, side)
                cross = load(basis, (j, q ^ 2), s, side)
                f = [
                    made[part]
                    + near[part]
                    + high_fields[0] * x[1 - n][part]
                    + high_fields[1] * cross[part]
                    for part in range(2)
                ]
                dr = window(diagonal, (q, 0), side, s, 0)[...]
                di = window(diagonal, (q, 1), side, s, 0)[...]
                xr, xi = x[n]
                w = (dr * xr - di * xi - f[0], dr * xi + di * xr - f[1])
                more = pairing(x[n], w)
                if before:
                    more = more + pairing(load(basis, (j - 1, q), s, side), w)
                if norm:
                    more = more + (fold(w[0] * w[0] + w[1] * w[1]),)
                for m, value in enumerate(more):
                    acc[m] = acc[m] + value
                for part in range(2):
                    window(work, (slot, q), part, s, side)[...] = w[part]
            if send and side == 1 and (s + 1) % (half // TILE) == 0:
                work_copy(slot, 2 * pair + (s + 1) // (half // TILE) - 1).start()

    def take(q, w_ref, u_ref, slot, now, before, after, coeffs, inverse, both, own, between=()):
        for t, (s, side) in enumerate(tiles):
            if t % 16 == 0 and between:
                issue(*between[t // 16])
            rr, ri = load(w_ref, (slot, q), s, side)
            for n, lead in enumerate([now, before] if both else [now]):
                vr, vi = load(u_ref, (lead, q), s, side)
                hr, hm = coeffs[2 * n], coeffs[2 * n + 1]
                rr = rr - (hr * vr - hm * vi)
                ri = ri - (hr * vi + hm * vr)
            for part, value in enumerate((rr * inverse, ri * inverse)):
                window(u_ref, (after, q), part, s, side)[...] = value
                if own:
                    put_split(q, part, s, side, value)

    def apply(j, first, last):
        slot = j % 2
        acc = [zero_tile] * (2 + 2 * (not first) + (not last))
        if not first:
            known = [scalars[j - 1, n] for n in range(6)]
            for n in range(2, 4):
                work_copy(1 - slot, n).wait()
        products = [(q, part) for q in (2, 3) for part in range(2)]
        consume(j, 0, acc, not first, not last, not last, products)
        if not first:
            for q in range(2, 4):
                take(
                    q, mate_work, mate, 1 - slot, 1 - slot, slot, slot, known[:4], known[5],
                    True, False,
                )
        consume(j, 1, acc, not first, not last, False)
        return acc

    def rest_inner(j, count):
        slot = j % 2

        def one(k, carry):
            def add(q, acc):
                real, imag = acc
                for s, side in tiles:
                    v = load(basis, (k, q), s, side)
                    w = load(work, (slot, q), s, side)
                    more = pairing(v, w)
                    real, imag = real + more[0], imag + more[1]
                return real, imag

            real, imag = lax.fori_loop(0, quarters, add, (zero_tile, zero_tile))
            own_rest[j, k, 0] = real
            own_rest[j, k, 1] = imag
            return carry

        lax.fori_loop(0, count, one, 0)

    def step(j, first):
        slot = j % 2
        sums = apply(j, first, False)
        start_sums(sums, slot)
        for n in range(2, 4):
            work_copy(slot, n).start()
        if not first:
            rest_inner(j, j - 1)
        coeffs = finish_sums(len(sums), slot)
        left = coeffs[-1]
        for value in coeffs[:-1]:
            left = left - value * value
        norm, inv_norm = scalar_sqrt(left)
        for n in range(4):
            scalars[j, n] = coeffs[n] if n < len(coeffs) - 1 else jnp.float32(0.0)
        scalars[j, 4] = norm
        scalars[j, 5] = inv_norm
        for n in range(2):
            work_copy(slot, n).wait()
        for q in range(quarters):
            between = [(q - 1, part) for part in range(2)] if 0 < q < 3 else ()
            take(
                q, work, basis, slot, j, j - 1, j + 1, coeffs, inv_norm, not first, True, between
            )
        for q in range(2):
            take(
                q, mate_work, mate, slot, slot, 1 - slot, 1 - slot, coeffs, inv_norm,
                not first, False,
            )

    final = KRYLOV - 1
    for q in range(2):
        for part in range(2):
            issue(q, part)
    step(0, True)

    def later(j, carry):
        step(j, False)
        return carry

    lax.fori_loop(1, final, later, 0)
    rest_copy = remote(
        own_rest.at[pl.ds(0, final)],
        other_rest.at[pl.ds(0, final)],
        rest_sem.at[0],
        rest_sem.at[1],
        other,
    )
    last_copy = remote(
        own_rest.at[final], other_rest.at[final], rest_sem.at[2], rest_sem.at[3], other
    )
    rest_copy.start()
    start_sums(apply(final, False, True), final % 2)
    rest_inner(final, final - 1)
    last_copy.start()
    rest_copy.wait()
    sub = lax.broadcasted_iota(jnp.int32, (8, LANES), 0)
    lane = lax.broadcasted_iota(jnp.int32, (8, LANES), 1)

    def put(tile, where, value):
        return jnp.where(where, value, tile)

    gram = [jnp.where(sub == lane, 1.0, 0.0).astype(jnp.float32), zero_tile]
    projected = [zero_tile, zero_tile]
    column = {j: [zero_tile, zero_tile] for j in range(3)}
    across = {j: [zero_tile, zero_tile] for j in range(3)}
    for j in range(final):
        here = lane == j
        alpha = [scalars[j, 0], scalars[j, 1]]
        bravo = [scalars[j, 2], scalars[j, 3]]
        for part in range(2):
            projected[part] = put(projected[part], here & (sub == j), alpha[part])
            if j > 0:
                projected[part] = put(projected[part], here & (sub == j - 1), bravo[part])
        projected[0] = put(projected[0], here & (sub == j + 1), scalars[j, 4])
        if j < 2:
            continue
        down = [zero_tile, zero_tile]
        along = [zero_tile, zero_tile]
        for k in range(j - 1):
            for part in range(2):
                value = jnp.sum(own_rest[j, k, part] + other_rest[j, k, part])
                down[part] = put(down[part], sub == k, value)
                along[part] = put(along[part], lane == k, value)
        for made, new in ((column, down), (across, along)):
            for value, old in ((alpha, made[j]), (bravo, made[j - 1])):
                new[0] = new[0] - (value[0] * old[0] - value[1] * old[1])
                new[1] = new[1] - (value[0] * old[1] + value[1] * old[0])
            made[j + 1] = [part * scalars[j, 5] for part in new]
        gram[0] = gram[0] + jnp.where(lane == j + 1, column[j + 1][0], 0.0)
        gram[0] = gram[0] + jnp.where(sub == j + 1, across[j + 1][0], 0.0)
        gram[1] = gram[1] + jnp.where(lane == j + 1, column[j + 1][1], 0.0)
        gram[1] = gram[1] - jnp.where(sub == j + 1, across[j + 1][1], 0.0)

    near_targets = finish_sums(4, final % 2)
    last_copy.wait()
    targets = []
    for k in range(final - 1):
        for part in range(2):
            targets.append(jnp.sum(own_rest[final, k, part] + other_rest[final, k, part]))
    targets = targets + near_targets[2:4] + near_targets[:2]
    for k in range(KRYLOV):
        for part in range(2):
            gram[part] = put(gram[part], (lane == KRYLOV) & (sub == k), targets[2 * k + part])

    def column_of(tile, k):
        return jnp.broadcast_to(tile[:, k : k + 1], tile.shape)

    def row_of(tile, k):
        return jnp.broadcast_to(tile[k : k + 1, :], tile.shape)

    for p in range(KRYLOV):
        row = [row_of(tile, p) for tile in gram]
        factor = [column_of(tile, p) for tile in gram]
        inverse = 1.0 / row_of(factor[0], p)
        row = [tile * inverse for tile in row]
        less = (
            factor[0] * row[0] - factor[1] * row[1],
            factor[0] * row[1] + factor[1] * row[0],
        )
        gram = [jnp.where(sub == p, row[n], gram[n] - less[n]) for n in range(2)]
    for part in range(2):
        projected[part] = put(projected[part], lane == final, column_of(gram[part], KRYLOV))

    def product(a, b):
        real, imag = zero_tile, zero_tile
        for k in range(KRYLOV):
            ar, ai = column_of(a[0], k), column_of(a[1], k)
            br, bi = row_of(b[0], k), row_of(b[1], k)
            real = real + (ar * br - ai * bi)
            imag = imag + (ar * bi + ai * br)
        return real, imag

    inside = lane < KRYLOV
    pace = unit * (time_step / 2.0**squarings)
    first = (
        jnp.where(inside, projected[1] * pace, 0.0),
        jnp.where(inside, projected[0] * -pace, 0.0),
    )
    second = product(first, first)
    third = product(second, first)
    identity = jnp.where(sub == lane, 1.0, 0.0).astype(jnp.float32)
    series = None
    for low in range(taylor_order // 3 * 3, -1, -3):
        terms = [identity * (1.0 / math.factorial(low)), zero_tile]
        for n, power in ((low + 1, first), (low + 2, second)):
            if n <= taylor_order:
                terms = [t + p * (1.0 / math.factorial(n)) for t, p in zip(terms, power)]
        if series is not None:
            terms = [t + p for t, p in zip(terms, product(third, series))]
        series = terms
    for repeat in range(squarings):
        series = product(series, series)
    weights = [
        jnp.sum(jnp.where((sub == k) & (lane == 0), tile * beta, 0.0))
        for tile in series
        for k in range(KRYLOV)
    ]
    channel_copy.wait()
    channel = jnp.where(stays, own_channel[...], other_channel[...])
    sub_pos = lax.broadcasted_iota(jnp.int32, (TILE, LANES), 0) * LANES
    sub_pos = sub_pos + lax.broadcasted_iota(jnp.int32, (TILE, LANES), 1)

    def combine(q, acc):
        high = (core << split_spin) + (q << (split_spin + 1))
        for s, side in tiles:
            pr = jnp.zeros((TILE, LANES), jnp.float32)
            pi = jnp.zeros((TILE, LANES), jnp.float32)
            for k in range(KRYLOV):
                vr = window(basis, (k, q), 0, s, side)[...]
                vi = window(basis, (k, q), 1, s, side)[...]
                cr, ci = weights[k], weights[k + KRYLOV]
                pr = pr + (cr * vr - ci * vi)
                pi = pi + (cr * vi + ci * vr)
            window(work, (0, q), 0, s, side)[...] = pr
            window(work, (0, q), 1, s, side)[...] = pi
            position = sub_pos + (high + (side << side_spin) + s * TILE * LANES)
            occupied = lax.shift_right_logical(position, channel) & 1
            acc = acc + fold(jnp.where(occupied == 1, pr * pr + pi * pi, 0.0))
        return acc

    jumped_sq = lax.fori_loop(0, quarters, combine, zero_tile)

    start_sums([jumped_sq], 0)

    def pack(target, q, part):
        for s, side in tiles:
            value = window(work, (0, q), part, s, side)[...]
            for b in range(SPINS - 1 - split_spin):
                flipped = window(work, (0, q | (1 << b)), part, s, side)[...]
                value = jnp.where(channel == split_spin + 1 + b, flipped, value)
            target[s * TILE : (s + 1) * TILE, side * LANES : (side + 1) * LANES] = value

    parcels = []
    for part in range(2):
        q = me ^ (1 << part)
        pack(parcel.at[part], q, part)
        copy = remote(
            parcel.at[part],
            pieces.at[core, part],
            parcel_send.at[part],
            parcel_recv.at[core, part],
            device(held, q),
        )
        copy.start()
        parcels.append(copy)
    for part in range(2):
        pack(parcel.at[2 + part], me, part)
    home = remote(
        parcel.at[pl.ds(2, 2)], pieces.at[core], parcel_send.at[2], parcel_recv.at[2, 0], other
    )

    @pl.when(jnp.logical_not(stays))
    def _():
        home.start()

    @pl.when(stays)
    def _():
        for part in range(2):
            pieces[core, part] = parcel[2 + part]

    all_sq = finish_sums(1, 0)[0]
    size = jnp.float32(quarters * 2 * piece_rows // 2 * LANES)
    ratio = jnp.where(channel[:8] < SPINS, size / jnp.full((8, LANES), all_sq, jnp.float32), 1.0)
    own_scale = jnp.sqrt(ratio)
    own_sums[1, 0:8] = own_scale
    scale_copy = remote(
        own_sums.at[1, pl.ds(0, 8)], scale_out, scale_sem.at[0], scale_sem.at[1],
        device(core, me ^ 1),
    )

    @pl.when(stays)
    def _():
        scale_copy.start()
        scale_out[...] = own_scale
        remote(
            parcel.at[pl.ds(2, 2)], pieces.at[1 - core], parcel_send.at[2],
            parcel_recv.at[2, 0], other,
        ).wait_recv()
        scale_copy.wait_send()

    @pl.when(jnp.logical_not(stays))
    def _():
        for sender in range(2):
            for part in range(2):
                remote(
                    parcel.at[part], pieces.at[sender, part], parcel_send.at[part],
                    parcel_recv.at[sender, part], other,
                ).wait_recv()
        scale_copy.wait_recv()
        home.wait_send()
        piece(core, near_chip, 3).wait_send()

    for copy in parcels:
        copy.wait_send()
    for send in sends:
        send.wait_send()


def lower_kernel(channel_ref, pieces, scale, out):
    channel = channel_ref[0]
    me = lax.axis_index("amp")
    side_spin = LANE_BITS + BLOCK_BITS
    in_lanes = channel < LANE_BITS
    in_rows = jnp.logical_not(in_lanes) & (channel < side_spin)
    lane_shift = jnp.where(in_lanes, lax.shift_left(1, channel), 0)
    row_shift = jnp.where(in_rows, lax.shift_left(1, jnp.maximum(channel - LANE_BITS, 0)), 0)
    near = jnp.where(row_shift < 8, row_shift, 0)
    far = jnp.where(row_shift < 8, 0, row_shift)
    lane_turn = (LANES - lane_shift) % LANES
    row_turn = (8 - near) % 8
    sub_pos = lax.broadcasted_iota(jnp.int32, (8, LANES), 0) * LANES
    sub_pos = sub_pos + lax.broadcasted_iota(jnp.int32, (8, LANES), 1)
    own = me * (4 * BLOCK * LANES)
    factor = scale[...]

    for half in range(2):
        from_half = jnp.where(channel == side_spin + 1, 1, half)
        for side in range(2):
            from_side = jnp.where(channel == side_spin, 1, side)
            columns = pl.ds(pl.multiple_of(from_side * LANES, LANES), LANES)

            def lower(i, carry, half=half, side=side, from_half=from_half, columns=columns):
                for t in range(8):
                    local = i * 64 + t * 8
                    base = (half * 2 + side) * BLOCK + local
                    rows = pl.ds(pl.multiple_of(local | far, 8), 8)
                    position = sub_pos + (own + base * LANES)
                    vacant = (lax.shift_right_logical(position, channel) & 1) == 0
                    for part in range(2):
                        x = pieces[from_half, part, rows, columns]
                        x = pltpu.roll(x, row_turn, 0)
                        x = pltpu.roll(x, lane_turn, 1)
                        x = jnp.where(vacant, x * factor, 0.0)
                        out[pl.ds(base * 2 + part, 8, stride=2), :] = x
                return carry

            lax.fori_loop(0, BLOCK // 64, lower, 0)


def paired_body(amplitudes, couplings, fields, decays, channel):
    quarters = lax.axis_size("amp")
    local_len = amplitudes.shape[2]
    block_rows = local_len // LANES
    vmem = pl.BlockSpec(memory_space=pltpu.VMEM)
    smem = pl.BlockSpec(memory_space=pltpu.SMEM)
    f32 = jnp.float32
    dma = pltpu.SemaphoreType.DMA
    sums_rows = 8 * (2 * KRYLOV + 1)
    state = amplitudes.reshape(2, block_rows, LANES).transpose(1, 0, 2)
    state = state.reshape(2 * block_rows, LANES)
    pieces, scale = pl.pallas_call(
        pair_kernel,
        out_shape=(
            jax.ShapeDtypeStruct((2, 2, BLOCK, BLOCK), f32),
            jax.ShapeDtypeStruct((8, LANES), f32),
        ),
        in_specs=[smem] * 4 + [vmem],
        out_specs=(vmem, vmem),
        scratch_shapes=[
            pltpu.VMEM((quarters, block_rows, LANES), f32),
            pltpu.VMEM((quarters, block_rows, LANES), f32),
            pltpu.VMEM((KRYLOV, quarters, 2, BLOCK, BLOCK), f32),
            pltpu.VMEM((2, quarters, 2, BLOCK, BLOCK), f32),
            pltpu.VMEM((2, quarters, 2, BLOCK, BLOCK), f32),
            pltpu.VMEM((2, quarters, 2, BLOCK, BLOCK), f32),
            pltpu.VMEM((quarters, 2, BLOCK, BLOCK), f32),
            pltpu.VMEM((quarters, 2, 2, BLOCK, BLOCK), jnp.bfloat16),
            pltpu.VMEM((BLOCK, 3 * BLOCK), jnp.bfloat16),
            pltpu.VMEM((3 * BLOCK, BLOCK), jnp.bfloat16),
            pltpu.VMEM((quarters, 2, 2, BLOCK, LANES), f32),
            pltpu.VMEM((2, sums_rows, LANES), f32),
            pltpu.VMEM((2, sums_rows, LANES), f32),
            pltpu.VMEM((KRYLOV, KRYLOV - 2, 2, 8, LANES), f32),
            pltpu.VMEM((KRYLOV, KRYLOV - 2, 2, 8, LANES), f32),
            pltpu.SMEM((KRYLOV - 1, 6), f32),
            pltpu.VMEM((TILE, LANES), jnp.int32),
            pltpu.VMEM((TILE, LANES), jnp.int32),
            pltpu.VMEM((4, BLOCK, BLOCK), f32),
            dma((4,)),
            dma((quarters,)),
            dma((quarters,)),
            dma((quarters,)),
            dma((2,)),
            dma((2,)),
            dma((4,)),
            dma((2, quarters)),
            dma((2, quarters)),
            dma((2,)),
            dma((3,)),
            dma((3, 2)),
            dma((2,)),
        ],
        compiler_params=pltpu.CompilerParams(
            collective_id=1, has_side_effects=True, vmem_limit_bytes=48 * 1024 * 1024
        ),
        name="pair",
    )(channel, couplings, fields, decays, state)
    lowered = pl.pallas_call(
        lower_kernel,
        out_shape=jax.ShapeDtypeStruct((2 * block_rows, LANES), f32),
        in_specs=[smem, vmem, vmem],
        out_specs=vmem,
        compiler_params=pltpu.CompilerParams(vmem_limit_bytes=8 * 1024 * 1024),
        name="lower",
    )(channel, pieces, scale)
    lowered = lowered.reshape(block_rows, 2, LANES).transpose(1, 0, 2)
    return lowered.reshape(amplitudes.shape)


def solution(mesh):
    placed = (P("traj", None, "amp"), P(), P(), P(), P("traj"))

    def step(amplitudes, *rest):
        trajectories = mesh.shape["traj"]
        low_rows = amplitudes.shape[2] // mesh.shape["amp"] // LANES
        paired = (
            mesh.shape["amp"] == 4
            and trajectories % 2 == 0
            and amplitudes.shape[0] == trajectories
            and low_rows == 4 * BLOCK
        )
        return jax.shard_map(
            paired_body if paired else body,
            mesh=mesh,
            in_specs=placed,
            out_specs=P("traj", None, "amp"),
            check_vma=False,
        )(amplitudes, *rest)

    return step
```

```python
import math

import jax
import jax.numpy as jnp
from jax import lax
from jax.experimental import pallas as pl
from jax.experimental.pallas import tpu as pltpu
from jax.sharding import PartitionSpec as P

SPINS = 19
KRYLOV = 8
LANES = 128
LANE_BITS = 7

time_step = 0.7
squarings = 8
taylor_order = 10
highest = lax.Precision.HIGHEST

CHUNK_BITS = 8
CHUNK = 1 << CHUNK_BITS
SUB = 32


def split(x):
    hi = x.astype(jnp.bfloat16)
    lo = (x - hi.astype(jnp.float32)).astype(jnp.bfloat16)
    return hi, lo


def dot(a, b):
    return jnp.dot(a, b, preferred_element_type=jnp.float32)


def fold(x):
    return jnp.sum(x.reshape(x.shape[0] // 8, 8, x.shape[1]), axis=0)


def scalar_sqrt(value):
    root = jnp.sqrt(jnp.full((8, LANES), value, jnp.float32))
    return jnp.max(root), jnp.max(1.0 / root)


def krylov_weights(a_matrix):
    size = a_matrix.shape[0]
    pad = jnp.zeros((LANES - size, LANES), jnp.float32)
    scaled = jnp.concatenate([a_matrix, pad], axis=0) * (1.0 / 2.0**squarings)
    rows = lax.broadcasted_iota(jnp.int32, (LANES, LANES), 0)
    cols = lax.broadcasted_iota(jnp.int32, (LANES, LANES), 1)
    identity = jnp.where(rows == cols, 1.0, 0.0).astype(jnp.float32)
    series = identity
    for degree in range(taylor_order, 0, -1):
        product = jnp.dot(
            scaled, series, precision=highest, preferred_element_type=jnp.float32
        )
        series = identity + product * (1.0 / degree)
    for repeat in range(squarings):
        series = jnp.dot(
            series, series, precision=highest, preferred_element_type=jnp.float32
        )
    return series


def kernel(
    channel_ref,
    couplings,
    fields,
    decays,
    state,
    out,
    basis,
    work,
    flips,
    row_table,
    lane_table,
    diag_low,
):
    node_count, _, block_rows, _ = state.shape
    rows = node_count * block_rows
    chunks = rows // CHUNK
    subs = CHUNK // SUB
    channel = channel_ref[0]
    device = lax.axis_index("amp")
    zero_tile = jnp.zeros((8, LANES), jnp.float32)
    per_block = block_rows // CHUNK

    table_shape = (CHUNK, CHUNK)
    crossed = lax.broadcasted_iota(jnp.int32, table_shape, 0)
    crossed = crossed ^ lax.broadcasted_iota(jnp.int32, table_shape, 1)
    for table, first_spin, bits in (
        (row_table, LANE_BITS, CHUNK_BITS),
        (lane_table, 0, LANE_BITS),
    ):
        value = jnp.zeros(table_shape, jnp.float32)
        for bit in range(bits):
            value = jnp.where(crossed == 1 << bit, fields[first_spin + bit], value)
        table[0], table[1] = split(value)

    low_shape = (CHUNK, LANES)
    low_pos = lax.broadcasted_iota(jnp.int32, low_shape, 0) * LANES
    low_pos = low_pos + lax.broadcasted_iota(jnp.int32, low_shape, 1)
    low_bits = LANE_BITS + CHUNK_BITS
    before = None
    low_real = jnp.zeros(low_shape, jnp.float32)
    low_imag = jnp.zeros(low_shape, jnp.float32)
    for spin in range(low_bits):
        occupied = (lax.shift_right_logical(low_pos, spin) & 1).astype(jnp.float32)
        sign = 1.0 - 2.0 * occupied
        low_imag = low_imag - 0.5 * decays[spin] * occupied
        if spin > 0:
            low_real = low_real - couplings[spin - 1] * (before * sign)
        before = sign
    diag_low[0] = low_real
    diag_low[1] = low_imag

    def high_diagonal(i):
        bits = [
            (lax.shift_right_logical(i, b) & 1).astype(jnp.float32)
            for b in range(SPINS - low_bits)
        ]
        signs = [1.0 - 2.0 * bit for bit in bits]
        real = jnp.float32(0.0)
        imag = jnp.float32(0.0)
        for b in range(len(bits)):
            imag = imag - 0.5 * decays[low_bits + b] * bits[b]
            if b > 0:
                real = real - couplings[low_bits + b - 1] * signs[b - 1] * signs[b]
        edge = couplings[low_bits - 1] * signs[0]
        return real - edge, real + edge, imag

    def start_norm(i, acc):
        node = i // per_block
        first = (i % per_block) * CHUNK
        for part in range(2):
            x = state[node, part, pl.ds(first, CHUNK), :]
            acc = acc + fold(x * x)
        return acc

    start_sq = jnp.sum(lax.fori_loop(0, chunks, start_norm, zero_tile))
    beta, inv_beta = scalar_sqrt(start_sq)

    def start_vector(i, carry):
        node = i // per_block
        first = (i % per_block) * CHUNK
        for part in range(2):
            basis[0, pl.ds(i * CHUNK, CHUNK), part * LANES : (part + 1) * LANES] = (
                state[node, part, pl.ds(first, CHUNK), :] * inv_beta
            )
        return carry

    lax.fori_loop(0, chunks, start_vector, 0)

    mat_rows = lax.broadcasted_iota(jnp.int32, (2 * KRYLOV, LANES), 0)
    mat_cols = lax.broadcasted_iota(jnp.int32, (2 * KRYLOV, LANES), 1)
    a_matrix = jnp.zeros((2 * KRYLOV, LANES), jnp.float32)

    def put(matrix, k, j, real, imag):
        a_real = time_step * imag
        a_imag = -time_step * real
        for r, c, value in (
            (k, j, a_real),
            (k, j + KRYLOV, -a_imag),
            (k + KRYLOV, j, a_imag),
            (k + KRYLOV, j + KRYLOV, a_real),
        ):
            matrix = jnp.where((mat_rows == r) & (mat_cols == c), value, matrix)
        return matrix

    high_fields = [
        fields[LANE_BITS + CHUNK_BITS + b] for b in range(SPINS - LANE_BITS - CHUNK_BITS)
    ]

    for j in range(KRYLOV):
        last = j + 1 == KRYLOV

        def apply_chunk(i, acc, j=j):
            base = pl.multiple_of(i * CHUNK, CHUNK)
            hi, lo = split(basis[j, pl.ds(base, CHUNK), :])
            flips[...] = (
                dot(row_table[0], hi)
                + dot(row_table[1], hi)
                + dot(row_table[0], lo)
                + dot(hi, lane_table[0])
                + dot(lo, lane_table[0])
                + dot(hi, lane_table[1])
            )
            acc = list(acc)
            real_vacant, real_occupied, imag_high = high_diagonal(i)
            for s in range(subs):
                here = pl.ds(base + s * SUB, SUB)
                x = basis[j, here, :]
                f = flips[s * SUB : (s + 1) * SUB, :]
                for b, field in enumerate(high_fields):
                    there = pl.multiple_of((i ^ (1 << b)) * CHUNK, CHUNK)
                    f = f + field * basis[j, pl.ds(there + s * SUB, SUB), :]
                part = slice(s * SUB, (s + 1) * SUB)
                dr = diag_low[0, part, :] + (real_vacant if s < subs // 2 else real_occupied)
                di = diag_low[1, part, :] + imag_high
                xr, xi = x[:, :LANES], x[:, LANES:]
                wr = dr * xr - di * xi - f[:, :LANES]
                wi = dr * xi + di * xr - f[:, LANES:]
                work[here, :LANES] = wr
                work[here, LANES:] = wi
                for k in range(j + 1):
                    vr = basis[k, here, :LANES]
                    vi = basis[k, here, LANES:]
                    acc[2 * k] = acc[2 * k] + fold(vr * wr + vi * wi)
                    acc[2 * k + 1] = acc[2 * k + 1] + fold(vr * wi - vi * wr)
                acc[-1] = acc[-1] + fold(wr * wr + wi * wi)
            return tuple(acc)

        sums = lax.fori_loop(0, chunks, apply_chunk, (zero_tile,) * (2 * j + 3))
        coeffs = [jnp.sum(t) for t in sums]
        for k in range(j + 1):
            a_matrix = put(a_matrix, k, j, coeffs[2 * k], coeffs[2 * k + 1])
        if last:
            break
        left = coeffs[-1]
        for value in coeffs[:-1]:
            left = left - value * value
        norm, inv_norm = scalar_sqrt(left)
        a_matrix = put(a_matrix, j + 1, j, norm, jnp.float32(0.0))

        def subtract_chunk(i, carry, j=j, coeffs=coeffs, inv_norm=inv_norm):
            base = pl.multiple_of(i * CHUNK, CHUNK)
            for s in range(subs):
                here = pl.ds(base + s * SUB, SUB)
                rr = work[here, :LANES]
                ri = work[here, LANES:]
                for k in range(j + 1):
                    vr = basis[k, here, :LANES]
                    vi = basis[k, here, LANES:]
                    hr, hm = coeffs[2 * k], coeffs[2 * k + 1]
                    rr = rr - (hr * vr - hm * vi)
                    ri = ri - (hr * vi + hm * vr)
                basis[j + 1, here, :LANES] = rr * inv_norm
                basis[j + 1, here, LANES:] = ri * inv_norm
            return carry

        lax.fori_loop(0, chunks, subtract_chunk, 0)

    series = krylov_weights(a_matrix)
    first = series[: 2 * KRYLOV, :] * beta
    weights = [
        jnp.sum(jnp.where((mat_rows == k) & (mat_cols == 0), first, 0.0))
        for k in range(2 * KRYLOV)
    ]
    sub_pos = lax.broadcasted_iota(jnp.int32, (SUB, LANES), 0) * LANES
    sub_pos = sub_pos + lax.broadcasted_iota(jnp.int32, (SUB, LANES), 1)

    def combine(i, acc):
        base = pl.multiple_of(i * CHUNK, CHUNK)
        for s in range(subs):
            here = pl.ds(base + s * SUB, SUB)
            pr = jnp.zeros((SUB, LANES), jnp.float32)
            pi = jnp.zeros((SUB, LANES), jnp.float32)
            for k in range(KRYLOV):
                vr = basis[k, here, :LANES]
                vi = basis[k, here, LANES:]
                cr, ci = weights[k], weights[k + KRYLOV]
                pr = pr + (cr * vr - ci * vi)
                pi = pi + (cr * vi + ci * vr)
            work[here, :LANES] = pr
            work[here, LANES:] = pi
            position = sub_pos + (base + s * SUB) * LANES
            occupied = lax.shift_right_logical(position, channel) & 1
            acc = acc + fold(jnp.where(occupied == 1, pr * pr + pi * pi, 0.0))
        return acc

    total = jnp.sum(lax.fori_loop(0, chunks, combine, zero_tile))
    jumped = channel < SPINS
    size = jnp.float32(rows * LANES)
    total = jnp.where(jumped, total, size)
    root = jnp.sqrt(size / jnp.full((8, LANES), total, jnp.float32))
    scale = jnp.max(root)
    in_lanes = channel < LANE_BITS
    lane_shift = jnp.where(in_lanes, lax.shift_left(1, channel), 0)
    row_shift = jnp.where(
        in_lanes | (channel >= SPINS),
        0,
        lax.shift_left(1, jnp.maximum(channel - LANE_BITS, 0)),
    )
    in_sublanes = row_shift < 8
    near = jnp.where(in_sublanes, row_shift, 0)
    far = jnp.where(in_sublanes, 0, row_shift)
    lane_turn = (LANES - lane_shift) % LANES
    row_turn = (SUB - near) % SUB

    def jump(i, carry):
        local = pl.multiple_of(i * SUB, SUB)
        base = device * block_rows + local
        source = pl.multiple_of(base + far, 8)
        position = sub_pos + base * LANES
        vacant = (lax.shift_right_logical(position, channel) & 1) == 0
        for part in range(2):
            x = work[pl.ds(source, SUB), part * LANES : (part + 1) * LANES]
            x = pltpu.roll(x, row_turn, 0)
            x = pltpu.roll(x, lane_turn, 1)
            out[part, pl.ds(local, SUB), :] = jnp.where(vacant, x * scale, 0.0)
        return carry

    lax.fori_loop(0, block_rows // SUB, jump, 0)


def gather_kernel(block, out, send_sem, recv_sem):
    me = lax.axis_index("amp")
    near = (me ^ 1, me ^ 2)
    barrier = pltpu.get_barrier_semaphore()
    for partner in near:
        pl.semaphore_signal(
            barrier, inc=1, device_id={"amp": partner}, device_id_type=pl.DeviceIdType.MESH
        )
    pl.semaphore_wait(barrier, 2)

    def copy(source, owner, part, axis, slot):
        return pltpu.make_async_remote_copy(
            src_ref=source,
            dst_ref=out.at[owner, part],
            send_sem=send_sem.at[slot],
            recv_sem=recv_sem.at[slot],
            device_id={"amp": near[axis]},
            device_id_type=pl.DeviceIdType.MESH,
        )

    direct = {}
    for turn in range(2):
        for axis in range(2):
            part = axis ^ turn
            direct[axis, part] = copy(block.at[part], me, part, axis, 2 * axis + part)
            direct[axis, part].start()
    out[me] = block[...]
    forwards = []
    for axis in range(2):
        direct[axis, axis].wait_recv()
        owner = near[axis]
        forward = copy(out.at[owner, axis], owner, axis, 1 - axis, 4 + axis)
        forward.start()
        forwards.append(forward)
    for axis in range(2):
        direct[axis, 1 - axis].wait_recv()
    for forward in forwards:
        forward.wait_recv()
    for sent in list(direct.values()) + forwards:
        sent.wait_send()


def gather(block):
    node_count = lax.axis_size("amp")
    if node_count != 4:
        return lax.all_gather(block, "amp")
    vmem = pl.BlockSpec(memory_space=pltpu.VMEM)
    return pl.pallas_call(
        gather_kernel,
        out_shape=jax.ShapeDtypeStruct((node_count,) + block.shape, block.dtype),
        in_specs=[vmem],
        out_specs=vmem,
        scratch_shapes=[pltpu.SemaphoreType.DMA((6,)), pltpu.SemaphoreType.DMA((6,))],
        compiler_params=pltpu.CompilerParams(collective_id=0, has_side_effects=True),
        name="gather",
    )(block)


def body(amplitudes, couplings, fields, decays, channel):
    node_count = lax.axis_size("amp")
    local_len = amplitudes.shape[2]
    block_rows = local_len // LANES
    rows = node_count * block_rows
    vmem = pl.BlockSpec(memory_space=pltpu.VMEM)
    smem = pl.BlockSpec(memory_space=pltpu.SMEM)
    call = pl.pallas_call(
        kernel,
        out_shape=jax.ShapeDtypeStruct((2, block_rows, LANES), jnp.float32),
        in_specs=[smem] * 4 + [vmem],
        out_specs=vmem,
        scratch_shapes=[
            pltpu.VMEM((KRYLOV, rows, 2 * LANES), jnp.float32),
            pltpu.VMEM((rows + rows // 2, 2 * LANES), jnp.float32),
            pltpu.VMEM((CHUNK, 2 * LANES), jnp.float32),
            pltpu.VMEM((2, CHUNK, CHUNK), jnp.bfloat16),
            pltpu.VMEM((2, CHUNK, CHUNK), jnp.bfloat16),
            pltpu.VMEM((2, CHUNK, LANES), jnp.float32),
        ],
        compiler_params=pltpu.CompilerParams(vmem_limit_bytes=62 * 1024 * 1024),
        name="trajectory",
    )
    results = []
    for t in range(amplitudes.shape[0]):
        block = amplitudes[t].reshape(2, block_rows, LANES)
        state = gather(block)
        results.append(call(channel[t : t + 1], couplings, fields, decays, state))
    return jnp.stack(results).reshape(amplitudes.shape)


BLOCK = 256
BLOCK_BITS = 8
TILE = 16


def pair_kernel(
    channel_ref,
    couplings,
    fields,
    decays,
    block,
    pieces,
    scale_out,
    landing,
    mate_landing,
    basis,
    mate,
    work,
    mate_work,
    flips,
    splits,
    row_table,
    lane_table,
    diagonal,
    own_sums,
    other_sums,
    own_rest,
    other_rest,
    scalars,
    own_channel,
    other_channel,
    parcel,
    gather_send,
    gather_recv,
    forward_send,
    forward_recv,
    sums_send,
    sums_recv,
    rest_sem,
    work_send,
    work_recv,
    channel_sem,
    parcel_send,
    parcel_recv,
    scale_sem,
):
    quarters = landing.shape[0]
    piece_rows = landing.shape[1]
    traj = lax.axis_index("traj")
    me = lax.axis_index("amp")
    core = traj & 1
    first_traj = traj - core
    held = (me ^ (me >> 1)) & 1
    stays = core == held
    split_spin = LANE_BITS + BLOCK_BITS + 1
    side_spin = split_spin - 1
    zero_tile = jnp.zeros((8, LANES), jnp.float32)
    tiles = [(s, side) for s in range(BLOCK // TILE) for side in range(2)]
    half = BLOCK // 2

    def device(core_index, chip):
        return {"traj": first_traj + core_index, "amp": chip}

    def remote(source, target, send, recv, where):
        return pltpu.make_async_remote_copy(
            src_ref=source,
            dst_ref=target,
            send_sem=send,
            recv_sem=recv,
            device_id=where,
            device_id_type=pl.DeviceIdType.MESH,
        )

    other = device(1 - core, me)
    barrier = pltpu.get_barrier_semaphore()
    for flip_core in range(2):
        for flip_chip in range(quarters):
            if flip_core or flip_chip:
                pl.semaphore_signal(
                    barrier,
                    inc=1,
                    device_id=device(core ^ flip_core, me ^ flip_chip),
                    device_id_type=pl.DeviceIdType.MESH,
                )
    own_channel[...] = jnp.full(own_channel.shape, channel_ref[0], jnp.int32)
    pl.semaphore_wait(barrier, 2 * quarters - 1)

    near_chip = me ^ (held ^ core)
    far_chip = near_chip ^ 3

    def piece(core_index, chip, slot):
        source = block.at[pl.ds(pl.multiple_of(core_index * piece_rows, piece_rows), piece_rows)]
        return remote(
            source,
            landing.at[me],
            gather_send.at[slot],
            gather_recv.at[me],
            device(core_index, chip),
        )

    sends = [piece(core, far_chip, 0), piece(1 - core, far_chip, 1), piece(1 - core, near_chip, 2)]
    for send in sends:
        send.start()

    @pl.when(jnp.logical_not(stays))
    def _():
        piece(core, near_chip, 3).start()

    channel_copy = remote(
        own_channel, other_channel, channel_sem.at[0], channel_sem.at[1], other
    )
    channel_copy.start()

    unit = fields[split_spin]
    inv_unit = jnp.max(1.0 / jnp.full((8, LANES), unit, jnp.float32))
    crossed = lax.broadcasted_iota(jnp.int32, (BLOCK, BLOCK), 0)
    crossed = crossed ^ lax.broadcasted_iota(jnp.int32, (BLOCK, BLOCK), 1)
    for table, spins, axis in (
        (row_table, [LANE_BITS + b for b in range(BLOCK_BITS)], 1),
        (lane_table, [*range(LANE_BITS), side_spin], 0),
    ):
        value = jnp.zeros((BLOCK, BLOCK), jnp.float32)
        for bit, spin in enumerate(spins):
            value = jnp.where(crossed == 1 << bit, fields[spin] * inv_unit, value)
        hi, lo = split(value)
        table[...] = jnp.concatenate([hi, hi, lo], axis=axis)

    core_bit = core.astype(jnp.float32)
    core_sign = 1.0 - 2.0 * core_bit
    bond = [couplings[spin] * inv_unit for spin in range(SPINS - 1)]
    loss = [0.5 * decays[spin] * inv_unit for spin in range(SPINS)]
    for side in range(2):
        low_shape = (BLOCK, LANES)
        low_pos = lax.broadcasted_iota(jnp.int32, low_shape, 0) * LANES
        low_pos = low_pos + lax.broadcasted_iota(jnp.int32, low_shape, 1)
        side_sign = 1.0 - 2.0 * side
        low_real = jnp.zeros(low_shape, jnp.float32)
        low_imag = jnp.zeros(low_shape, jnp.float32)
        before = None
        for spin in range(side_spin):
            occupied = (lax.shift_right_logical(low_pos, spin) & 1).astype(jnp.float32)
            sign = 1.0 - 2.0 * occupied
            low_imag = low_imag - loss[spin] * occupied
            if spin > 0:
                low_real = low_real - bond[spin - 1] * (before * sign)
            before = sign
        low_real = low_real - bond[side_spin - 1] * side_sign * before
        low_real = low_real - bond[side_spin] * side_sign * core_sign
        low_imag = low_imag - side * loss[side_spin] - core_bit * loss[split_spin]
        for q in range(quarters):
            bits = [(q >> b) & 1 for b in range(SPINS - 1 - split_spin)]
            signs = [core_sign] + [1.0 - 2.0 * bit for bit in bits]
            real, imag = low_real, low_imag
            for b, bit in enumerate(bits):
                real = real - bond[split_spin + b] * (signs[b] * signs[b + 1])
                imag = imag - bit * loss[split_spin + 1 + b]
            diagonal[q, 0, side] = real
            diagonal[q, 1, side] = imag

    def window(ref, lead, part, s, side):
        return ref.at[(*lead, part, pl.ds(s * TILE, TILE), pl.ds(side * LANES, LANES))]

    def sums_copy(count, slot):
        return remote(
            own_sums.at[slot, pl.ds(0, 8 * count)],
            other_sums.at[slot, pl.ds(0, 8 * count)],
            sums_send.at[slot],
            sums_recv.at[slot],
            other,
        )

    def start_sums(values, slot):
        for k, value in enumerate(values):
            own_sums[slot, 8 * k : 8 * k + 8] = value
        sums_copy(len(values), slot).start()

    def finish_sums(count, slot):
        sums_copy(count, slot).wait()
        both = [ref[slot, : 8 * count] for ref in (own_sums, other_sums)]
        both = both[0] + both[1]
        return [jnp.sum(both[8 * k : 8 * k + 8]) for k in range(count)]

    def work_copy(slot, n):
        pair = (pl.ds(2 * (n // 2), 2), slice(None), pl.ds(n % 2 * half, half))
        return remote(
            work.at[(slot, *pair)],
            mate_work.at[(slot, *pair)],
            work_send.at[slot, n],
            work_recv.at[slot, n],
            other,
        )

    @pl.when(stays)
    def _():
        def keep(i, carry):
            rows = pl.multiple_of(i * SUB, SUB)
            landing[me, pl.ds(rows, SUB), :] = block[
                pl.ds(pl.multiple_of(core * piece_rows, piece_rows) + rows, SUB), :
            ]
            return carry

        lax.fori_loop(0, piece_rows // SUB, keep, 0)

    mate[1, pl.ds(2, 2)] = jnp.zeros((2, 2, BLOCK, BLOCK), jnp.float32)

    def arrival(chip):
        return remote(
            block.at[pl.ds(0, piece_rows)],
            landing.at[chip],
            gather_send.at[0],
            gather_recv.at[chip],
            other,
        )

    def forward(chip):
        return remote(
            landing.at[chip],
            mate_landing.at[chip],
            forward_send.at[chip],
            forward_recv.at[chip],
            other,
        )

    @pl.when(jnp.logical_not(stays))
    def _():
        arrival(me).wait_recv()

    def square(ref, q, acc):
        def add(i, acc):
            x = ref[q, pl.ds(pl.multiple_of(i * 128, 128), 128), :]
            return acc + fold(x * x)

        return lax.fori_loop(0, piece_rows // 128, add, acc)

    own_sq = zero_tile
    for flip_chip in range(quarters):
        q = me ^ flip_chip
        if flip_chip:
            arrival(q).wait_recv()
        forward(q).start()
        own_sq = square(landing, q, own_sq)
    mate_sq = zero_tile
    for flip_chip in range(quarters):
        q = me ^ flip_chip
        forward(q).wait()
        mate_sq = square(mate_landing, q, mate_sq)
    beta, inv_beta = scalar_sqrt(jnp.sum(own_sq + mate_sq))

    def put_split(q, part, s, side, x):
        for n, term in enumerate(split(x)):
            window(splits, (q, part), n, s, side)[...] = term

    def start_vector(q, carry):
        for s, side in tiles:
            for part in range(2):
                rows = pl.ds((side * BLOCK + s * TILE) * 2 + part, TILE, stride=2)
                x = landing[q, rows, :] * inv_beta
                window(basis, (0, q), part, s, side)[...] = x
                put_split(q, part, s, side, x)
                window(mate, (0, q), part, s, side)[...] = mate_landing[q, rows, :] * inv_beta
        return carry

    lax.fori_loop(0, quarters, start_vector, 0)

    high_fields = [fields[split_spin + 1 + b] * inv_unit for b in range(SPINS - 1 - split_spin)]

    def issue(q, part):
        hi, lo = splits[q, part, 0], splits[q, part, 1]
        flips[q, part] = dot(
            jnp.concatenate([row_table[...], hi, lo, hi], axis=1),
            jnp.concatenate([hi, lo, hi, lane_table[...]], axis=0),
        )

    def pairing(v, w):
        return fold(v[0] * w[0] + v[1] * w[1]), fold(v[0] * w[1] - v[1] * w[0])

    def load(ref, lead, s, side):
        return [window(ref, lead, part, s, side)[...] for part in range(2)]

    def consume(j, slot, pair, acc, before, norm, h, between=()):
        count = len(tiles) // 2
        for t, (s, side) in enumerate(tiles[h * count : (h + 1) * count]):
            if t % 8 == 0 and between:
                issue(*between[t // 8])
            chosen = (2 * pair, 2 * pair + 1)
            x = [load(basis, (j, q), s, side) for q in chosen]
            for n, q in enumerate(chosen):
                made = load(flips, (q,), s, side)
                near = load(mate, (slot, q), s, side)
                cross = load(basis, (j, q ^ 2), s, side)
                f = [
                    made[part]
                    + near[part]
                    + high_fields[0] * x[1 - n][part]
                    + high_fields[1] * cross[part]
                    for part in range(2)
                ]
                dr = window(diagonal, (q, 0), side, s, 0)[...]
                di = window(diagonal, (q, 1), side, s, 0)[...]
                xr, xi = x[n]
                w = (dr * xr - di * xi - f[0], dr * xi + di * xr - f[1])
                more = pairing(x[n], w)
                if before:
                    more = more + pairing(load(basis, (j - 1, q), s, side), w)
                if norm:
                    more = more + (fold(w[0] * w[0] + w[1] * w[1]),)
                for m, value in enumerate(more):
                    acc[m] = acc[m] + value
                for part in range(2):
                    window(work, (slot, q), part, s, side)[...] = w[part]

    def take(q, w_ref, u_ref, slot, now, before, after, coeffs, inverse, both, own, between=()):
        group = 4
        leads = [now, before] if both else [now]
        for t in range(0, len(tiles), group):
            if t % 16 == 0 and between:
                issue(*between[t // 16])
            made = []
            for s, side in tiles[t : t + group]:
                rr, ri = load(w_ref, (slot, q), s, side)
                vs = [load(u_ref, (lead, q), s, side) for lead in leads]
                made.append((rr, ri, vs))
            for (s, side), (rr, ri, vs) in zip(tiles[t : t + group], made):
                for n, (vr, vi) in enumerate(vs):
                    hr, hm = coeffs[2 * n], coeffs[2 * n + 1]
                    rr = rr - (hr * vr - hm * vi)
                    ri = ri - (hr * vi + hm * vr)
                for part, value in enumerate((rr * inverse, ri * inverse)):
                    window(u_ref, (after, q), part, s, side)[...] = value
                    if own:
                        put_split(q, part, s, side, value)

    def apply(j, slot, first, last):
        acc = [zero_tile] * (2 + 2 * (not first) + (not last))
        middle = None
        if not first:
            known = [scalars[j - 1, n] for n in range(6)]
            for n in range(2, 4):
                work_copy(1 - slot, n).wait()

            def middle(q):
                take(
                    q, mate_work, mate, 1 - slot, 1 - slot, slot, slot, known[:4], known[5],
                    True, False,
                )

        for h in range(2):
            products = [(2 + h, part) for part in range(2)]
            consume(j, slot, 0, acc, not first, not last, h, products)
            if not last:
                work_copy(slot, h).start()
        if middle:
            middle(2)
            middle(3)
        for h in range(2):
            consume(j, slot, 1, acc, not first, not last, h)
        return acc

    def rest_inner(j, slot, count):

        def one(k, carry):
            def add(q, acc):
                real, imag = acc
                for s, side in tiles:
                    v = load(basis, (k, q), s, side)
                    w = load(work, (slot, q), s, side)
                    more = pairing(v, w)
                    real, imag = real + more[0], imag + more[1]
                return real, imag

            real, imag = lax.fori_loop(0, quarters, add, (zero_tile, zero_tile))
            own_rest[j, k, 0] = real
            own_rest[j, k, 1] = imag
            return carry

        lax.fori_loop(0, count, one, 0)

    def step(j, slot, first):
        sums = apply(j, slot, first, False)
        start_sums(sums, slot)
        for n in range(2, 4):
            work_copy(slot, n).start()
        if not first:
            rest_inner(j, slot, j - 1)
        coeffs = finish_sums(len(sums), slot)
        left = coeffs[-1]
        for value in coeffs[:-1]:
            left = left - value * value
        norm, inv_norm = scalar_sqrt(left)
        for n in range(4):
            scalars[j, n] = coeffs[n] if n < len(coeffs) - 1 else jnp.float32(0.0)
        scalars[j, 4] = norm
        scalars[j, 5] = inv_norm
        for q in range(quarters):
            if q == 2:
                for n in range(2):
                    work_copy(slot, n).wait()
            between = [(q - 2, part) for part in range(2)] if q > 1 else ()
            take(
                q, work, basis, slot, j, j - 1, j + 1, coeffs, inv_norm, not first, True, between
            )
        for q in range(2):
            take(
                q, mate_work, mate, slot, slot, 1 - slot, 1 - slot, coeffs, inv_norm,
                not first, False,
            )

    final = KRYLOV - 1
    for q in range(2):
        for part in range(2):
            issue(q, part)
    step(0, 0, True)

    def later(i, carry):
        step(2 * i + 1, 1, False)
        step(2 * i + 2, 0, False)
        return carry

    lax.fori_loop(0, final // 2, later, 0)
    rest_copy = remote(
        own_rest.at[pl.ds(0, final)],
        other_rest.at[pl.ds(0, final)],
        rest_sem.at[0],
        rest_sem.at[1],
        other,
    )
    last_copy = remote(
        own_rest.at[final], other_rest.at[final], rest_sem.at[2], rest_sem.at[3], other
    )
    rest_copy.start()
    start_sums(apply(final, final % 2, False, True), final % 2)
    rest_inner(final, final % 2, final - 1)
    last_copy.start()
    rest_copy.wait()
    sub = lax.broadcasted_iota(jnp.int32, (8, LANES), 0)
    lane = lax.broadcasted_iota(jnp.int32, (8, LANES), 1)

    def put(tile, where, value):
        return jnp.where(where, value, tile)

    gram = [jnp.where(sub == lane, 1.0, 0.0).astype(jnp.float32), zero_tile]
    projected = [zero_tile, zero_tile]
    column = {j: [zero_tile, zero_tile] for j in range(3)}
    across = {j: [zero_tile, zero_tile] for j in range(3)}
    for j in range(final):
        here = lane == j
        alpha = [scalars[j, 0], scalars[j, 1]]
        bravo = [scalars[j, 2], scalars[j, 3]]
        for part in range(2):
            projected[part] = put(projected[part], here & (sub == j), alpha[part])
            if j > 0:
                projected[part] = put(projected[part], here & (sub == j - 1), bravo[part])
        projected[0] = put(projected[0], here & (sub == j + 1), scalars[j, 4])
        if j < 2:
            continue
        down = [zero_tile, zero_tile]
        along = [zero_tile, zero_tile]
        for k in range(j - 1):
            for part in range(2):
                value = jnp.sum(own_rest[j, k, part] + other_rest[j, k, part])
                down[part] = put(down[part], sub == k, value)
                along[part] = put(along[part], lane == k, value)
        for made, new in ((column, down), (across, along)):
            for value, old in ((alpha, made[j]), (bravo, made[j - 1])):
                new[0] = new[0] - (value[0] * old[0] - value[1] * old[1])
                new[1] = new[1] - (value[0] * old[1] + value[1] * old[0])
            made[j + 1] = [part * scalars[j, 5] for part in new]
        gram[0] = gram[0] + jnp.where(lane == j + 1, column[j + 1][0], 0.0)
        gram[0] = gram[0] + jnp.where(sub == j + 1, across[j + 1][0], 0.0)
        gram[1] = gram[1] + jnp.where(lane == j + 1, column[j + 1][1], 0.0)
        gram[1] = gram[1] - jnp.where(sub == j + 1, across[j + 1][1], 0.0)

    near_targets = finish_sums(4, final % 2)
    last_copy.wait()
    targets = []
    for k in range(final - 1):
        for part in range(2):
            targets.append(jnp.sum(own_rest[final, k, part] + other_rest[final, k, part]))
    targets = targets + near_targets[2:4] + near_targets[:2]
    for k in range(KRYLOV):
        for part in range(2):
            gram[part] = put(gram[part], (lane == KRYLOV) & (sub == k), targets[2 * k + part])

    def column_of(tile, k):
        return jnp.broadcast_to(tile[:, k : k + 1], tile.shape)

    def row_of(tile, k):
        return jnp.broadcast_to(tile[k : k + 1, :], tile.shape)

    for p in range(KRYLOV):
        row = [row_of(tile, p) for tile in gram]
        factor = [column_of(tile, p) for tile in gram]
        inverse = 1.0 / row_of(factor[0], p)
        row = [tile * inverse for tile in row]
        less = (
            factor[0] * row[0] - factor[1] * row[1],
            factor[0] * row[1] + factor[1] * row[0],
        )
        gram = [jnp.where(sub == p, row[n], gram[n] - less[n]) for n in range(2)]
    for part in range(2):
        projected[part] = put(projected[part], lane == final, column_of(gram[part], KRYLOV))

    def product(a, b):
        real, imag = zero_tile, zero_tile
        for k in range(KRYLOV):
            ar, ai = column_of(a[0], k), column_of(a[1], k)
            br, bi = row_of(b[0], k), row_of(b[1], k)
            real = real + (ar * br - ai * bi)
            imag = imag + (ar * bi + ai * br)
        return real, imag

    inside = lane < KRYLOV
    pace = unit * (time_step / 2.0**squarings)
    first = (
        jnp.where(inside, projected[1] * pace, 0.0),
        jnp.where(inside, projected[0] * -pace, 0.0),
    )
    second = product(first, first)
    third = product(second, first)
    identity = jnp.where(sub == lane, 1.0, 0.0).astype(jnp.float32)
    series = None
    for low in range(taylor_order // 3 * 3, -1, -3):
        terms = [identity * (1.0 / math.factorial(low)), zero_tile]
        for n, power in ((low + 1, first), (low + 2, second)):
            if n <= taylor_order:
                terms = [t + p * (1.0 / math.factorial(n)) for t, p in zip(terms, power)]
        if series is not None:
            terms = [t + p for t, p in zip(terms, product(third, series))]
        series = terms
    for repeat in range(squarings):
        series = product(series, series)
    weights = [
        jnp.sum(jnp.where((sub == k) & (lane == 0), tile * beta, 0.0))
        for tile in series
        for k in range(KRYLOV)
    ]
    channel_copy.wait()
    channel = jnp.where(stays, own_channel[...], other_channel[...])
    sub_pos = lax.broadcasted_iota(jnp.int32, (TILE, LANES), 0) * LANES
    sub_pos = sub_pos + lax.broadcasted_iota(jnp.int32, (TILE, LANES), 1)

    def combine(q, acc):
        high = (core << split_spin) + (q << (split_spin + 1))
        for s, side in tiles:
            pr = jnp.zeros((TILE, LANES), jnp.float32)
            pi = jnp.zeros((TILE, LANES), jnp.float32)
            for k in range(KRYLOV):
                vr = window(basis, (k, q), 0, s, side)[...]
                vi = window(basis, (k, q), 1, s, side)[...]
                cr, ci = weights[k], weights[k + KRYLOV]
                pr = pr + (cr * vr - ci * vi)
                pi = pi + (cr * vi + ci * vr)
            window(work, (0, q), 0, s, side)[...] = pr
            window(work, (0, q), 1, s, side)[...] = pi
            position = sub_pos + (high + (side << side_spin) + s * TILE * LANES)
            occupied = lax.shift_right_logical(position, channel) & 1
            acc = acc + fold(jnp.where(occupied == 1, pr * pr + pi * pi, 0.0))
        return acc

    jumped_sq = lax.fori_loop(0, quarters, combine, zero_tile)

    start_sums([jumped_sq], 0)

    def pack(target, q, part):
        for s, side in tiles:
            value = window(work, (0, q), part, s, side)[...]
            for b in range(SPINS - 1 - split_spin):
                flipped = window(work, (0, q | (1 << b)), part, s, side)[...]
                value = jnp.where(channel == split_spin + 1 + b, flipped, value)
            target[s * TILE : (s + 1) * TILE, side * LANES : (side + 1) * LANES] = value

    parcels = []
    for part in range(2):
        q = me ^ (1 << part)
        pack(parcel.at[part], q, part)
        copy = remote(
            parcel.at[part],
            pieces.at[core, part],
            parcel_send.at[part],
            parcel_recv.at[core, part],
            device(held, q),
        )
        copy.start()
        parcels.append(copy)
    for part in range(2):
        pack(parcel.at[2 + part], me, part)
    home = remote(
        parcel.at[pl.ds(2, 2)], pieces.at[core], parcel_send.at[2], parcel_recv.at[2, 0], other
    )

    @pl.when(jnp.logical_not(stays))
    def _():
        home.start()

    @pl.when(stays)
    def _():
        for part in range(2):
            pieces[core, part] = parcel[2 + part]

    all_sq = finish_sums(1, 0)[0]
    size = jnp.float32(quarters * 2 * piece_rows // 2 * LANES)
    ratio = jnp.where(channel[:8] < SPINS, size / jnp.full((8, LANES), all_sq, jnp.float32), 1.0)
    own_scale = jnp.sqrt(ratio)
    own_sums[1, 0:8] = own_scale
    scale_copy = remote(
        own_sums.at[1, pl.ds(0, 8)], scale_out, scale_sem.at[0], scale_sem.at[1],
        device(core, me ^ 1),
    )

    @pl.when(stays)
    def _():
        scale_copy.start()
        scale_out[...] = own_scale
        remote(
            parcel.at[pl.ds(2, 2)], pieces.at[1 - core], parcel_send.at[2],
            parcel_recv.at[2, 0], other,
        ).wait_recv()
        scale_copy.wait_send()

    @pl.when(jnp.logical_not(stays))
    def _():
        for sender in range(2):
            for part in range(2):
                remote(
                    parcel.at[part], pieces.at[sender, part], parcel_send.at[part],
                    parcel_recv.at[sender, part], other,
                ).wait_recv()
        scale_copy.wait_recv()
        home.wait_send()
        piece(core, near_chip, 3).wait_send()

    for copy in parcels:
        copy.wait_send()
    for send in sends:
        send.wait_send()


def lower_kernel(channel_ref, pieces, scale, out):
    channel = channel_ref[0]
    me = lax.axis_index("amp")
    side_spin = LANE_BITS + BLOCK_BITS
    in_lanes = channel < LANE_BITS
    in_rows = jnp.logical_not(in_lanes) & (channel < side_spin)
    lane_shift = jnp.where(in_lanes, lax.shift_left(1, channel), 0)
    row_shift = jnp.where(in_rows, lax.shift_left(1, jnp.maximum(channel - LANE_BITS, 0)), 0)
    near = jnp.where(row_shift < 8, row_shift, 0)
    far = jnp.where(row_shift < 8, 0, row_shift)
    lane_turn = (LANES - lane_shift) % LANES
    row_turn = (8 - near) % 8
    sub_pos = lax.broadcasted_iota(jnp.int32, (8, LANES), 0) * LANES
    sub_pos = sub_pos + lax.broadcasted_iota(jnp.int32, (8, LANES), 1)
    own = me * (4 * BLOCK * LANES)
    factor = scale[...]

    for half in range(2):
        from_half = jnp.where(channel == side_spin + 1, 1, half)
        for side in range(2):
            from_side = jnp.where(channel == side_spin, 1, side)
            columns = pl.ds(pl.multiple_of(from_side * LANES, LANES), LANES)

            def lower(i, carry, half=half, side=side, from_half=from_half, columns=columns):
                for t in range(8):
                    local = i * 64 + t * 8
                    base = (half * 2 + side) * BLOCK + local
                    rows = pl.ds(pl.multiple_of(local | far, 8), 8)
                    position = sub_pos + (own + base * LANES)
                    vacant = (lax.shift_right_logical(position, channel) & 1) == 0
                    for part in range(2):
                        x = pieces[from_half, part, rows, columns]
                        x = pltpu.roll(x, row_turn, 0)
                        x = pltpu.roll(x, lane_turn, 1)
                        x = jnp.where(vacant, x * factor, 0.0)
                        out[pl.ds(base * 2 + part, 8, stride=2), :] = x
                return carry

            lax.fori_loop(0, BLOCK // 64, lower, 0)


def paired_body(amplitudes, couplings, fields, decays, channel):
    quarters = lax.axis_size("amp")
    local_len = amplitudes.shape[2]
    block_rows = local_len // LANES
    vmem = pl.BlockSpec(memory_space=pltpu.VMEM)
    smem = pl.BlockSpec(memory_space=pltpu.SMEM)
    f32 = jnp.float32
    dma = pltpu.SemaphoreType.DMA
    sums_rows = 8 * (2 * KRYLOV + 1)
    state = amplitudes.reshape(2, block_rows, LANES).transpose(1, 0, 2)
    state = state.reshape(2 * block_rows, LANES)
    pieces, scale = pl.pallas_call(
        pair_kernel,
        out_shape=(
            jax.ShapeDtypeStruct((2, 2, BLOCK, BLOCK), f32),
            jax.ShapeDtypeStruct((8, LANES), f32),
        ),
        in_specs=[smem] * 4 + [vmem],
        out_specs=(vmem, vmem),
        scratch_shapes=[
            pltpu.VMEM((quarters, block_rows, LANES), f32),
            pltpu.VMEM((quarters, block_rows, LANES), f32),
            pltpu.VMEM((KRYLOV, quarters, 2, BLOCK, BLOCK), f32),
            pltpu.VMEM((2, quarters, 2, BLOCK, BLOCK), f32),
            pltpu.VMEM((2, quarters, 2, BLOCK, BLOCK), f32),
            pltpu.VMEM((2, quarters, 2, BLOCK, BLOCK), f32),
            pltpu.VMEM((quarters, 2, BLOCK, BLOCK), f32),
            pltpu.VMEM((quarters, 2, 2, BLOCK, BLOCK), jnp.bfloat16),
            pltpu.VMEM((BLOCK, 3 * BLOCK), jnp.bfloat16),
            pltpu.VMEM((3 * BLOCK, BLOCK), jnp.bfloat16),
            pltpu.VMEM((quarters, 2, 2, BLOCK, LANES), f32),
            pltpu.VMEM((2, sums_rows, LANES), f32),
            pltpu.VMEM((2, sums_rows, LANES), f32),
            pltpu.VMEM((KRYLOV, KRYLOV - 2, 2, 8, LANES), f32),
            pltpu.VMEM((KRYLOV, KRYLOV - 2, 2, 8, LANES), f32),
            pltpu.SMEM((KRYLOV - 1, 6), f32),
            pltpu.VMEM((TILE, LANES), jnp.int32),
            pltpu.VMEM((TILE, LANES), jnp.int32),
            pltpu.VMEM((4, BLOCK, BLOCK), f32),
            dma((4,)),
            dma((quarters,)),
            dma((quarters,)),
            dma((quarters,)),
            dma((2,)),
            dma((2,)),
            dma((4,)),
            dma((2, quarters)),
            dma((2, quarters)),
            dma((2,)),
            dma((3,)),
            dma((3, 2)),
            dma((2,)),
        ],
        compiler_params=pltpu.CompilerParams(
            collective_id=1, has_side_effects=True, vmem_limit_bytes=48 * 1024 * 1024
        ),
        name="pair",
    )(channel, couplings, fields, decays, state)
    lowered = pl.pallas_call(
        lower_kernel,
        out_shape=jax.ShapeDtypeStruct((2 * block_rows, LANES), f32),
        in_specs=[smem, vmem, vmem],
        out_specs=vmem,
        compiler_params=pltpu.CompilerParams(vmem_limit_bytes=8 * 1024 * 1024),
        name="lower",
    )(channel, pieces, scale)
    lowered = lowered.reshape(block_rows, 2, LANES).transpose(1, 0, 2)
    return lowered.reshape(amplitudes.shape)


def solution(mesh):
    placed = (P("traj", None, "amp"), P(), P(), P(), P("traj"))

    def step(amplitudes, *rest):
        trajectories = mesh.shape["traj"]
        low_rows = amplitudes.shape[2] // mesh.shape["amp"] // LANES
        paired = (
            mesh.shape["amp"] == 4
            and trajectories % 2 == 0
            and amplitudes.shape[0] == trajectories
            and low_rows == 4 * BLOCK
        )
        return jax.shard_map(
            paired_body if paired else body,
            mesh=mesh,
            in_specs=placed,
            out_specs=P("traj", None, "amp"),
            check_vma=False,
        )(amplitudes, *rest)

    return step
```

```python
import math

import jax
import jax.numpy as jnp
from jax import lax
from jax.experimental import pallas as pl
from jax.experimental.pallas import tpu as pltpu
from jax.sharding import PartitionSpec as P

SPINS = 19
KRYLOV = 8
LANES = 128
LANE_BITS = 7

time_step = 0.7
squarings = 8
taylor_order = 10
highest = lax.Precision.HIGHEST

CHUNK_BITS = 8
CHUNK = 1 << CHUNK_BITS
SUB = 32


def split(x):
    hi = x.astype(jnp.bfloat16)
    lo = (x - hi.astype(jnp.float32)).astype(jnp.bfloat16)
    return hi, lo


def dot(a, b):
    return jnp.dot(a, b, preferred_element_type=jnp.float32)


def fold(x):
    return jnp.sum(x.reshape(x.shape[0] // 8, 8, x.shape[1]), axis=0)


def scalar_sqrt(value):
    root = jnp.sqrt(jnp.full((8, LANES), value, jnp.float32))
    return jnp.max(root), jnp.max(1.0 / root)


def krylov_weights(a_matrix):
    size = a_matrix.shape[0]
    pad = jnp.zeros((LANES - size, LANES), jnp.float32)
    scaled = jnp.concatenate([a_matrix, pad], axis=0) * (1.0 / 2.0**squarings)
    rows = lax.broadcasted_iota(jnp.int32, (LANES, LANES), 0)
    cols = lax.broadcasted_iota(jnp.int32, (LANES, LANES), 1)
    identity = jnp.where(rows == cols, 1.0, 0.0).astype(jnp.float32)
    series = identity
    for degree in range(taylor_order, 0, -1):
        product = jnp.dot(
            scaled, series, precision=highest, preferred_element_type=jnp.float32
        )
        series = identity + product * (1.0 / degree)
    for repeat in range(squarings):
        series = jnp.dot(
            series, series, precision=highest, preferred_element_type=jnp.float32
        )
    return series


def kernel(
    channel_ref,
    couplings,
    fields,
    decays,
    state,
    out,
    basis,
    work,
    flips,
    row_table,
    lane_table,
    diag_low,
):
    node_count, _, block_rows, _ = state.shape
    rows = node_count * block_rows
    chunks = rows // CHUNK
    subs = CHUNK // SUB
    channel = channel_ref[0]
    device = lax.axis_index("amp")
    zero_tile = jnp.zeros((8, LANES), jnp.float32)
    per_block = block_rows // CHUNK

    table_shape = (CHUNK, CHUNK)
    crossed = lax.broadcasted_iota(jnp.int32, table_shape, 0)
    crossed = crossed ^ lax.broadcasted_iota(jnp.int32, table_shape, 1)
    for table, first_spin, bits in (
        (row_table, LANE_BITS, CHUNK_BITS),
        (lane_table, 0, LANE_BITS),
    ):
        value = jnp.zeros(table_shape, jnp.float32)
        for bit in range(bits):
            value = jnp.where(crossed == 1 << bit, fields[first_spin + bit], value)
        table[0], table[1] = split(value)

    low_shape = (CHUNK, LANES)
    low_pos = lax.broadcasted_iota(jnp.int32, low_shape, 0) * LANES
    low_pos = low_pos + lax.broadcasted_iota(jnp.int32, low_shape, 1)
    low_bits = LANE_BITS + CHUNK_BITS
    before = None
    low_real = jnp.zeros(low_shape, jnp.float32)
    low_imag = jnp.zeros(low_shape, jnp.float32)
    for spin in range(low_bits):
        occupied = (lax.shift_right_logical(low_pos, spin) & 1).astype(jnp.float32)
        sign = 1.0 - 2.0 * occupied
        low_imag = low_imag - 0.5 * decays[spin] * occupied
        if spin > 0:
            low_real = low_real - couplings[spin - 1] * (before * sign)
        before = sign
    diag_low[0] = low_real
    diag_low[1] = low_imag

    def high_diagonal(i):
        bits = [
            (lax.shift_right_logical(i, b) & 1).astype(jnp.float32)
            for b in range(SPINS - low_bits)
        ]
        signs = [1.0 - 2.0 * bit for bit in bits]
        real = jnp.float32(0.0)
        imag = jnp.float32(0.0)
        for b in range(len(bits)):
            imag = imag - 0.5 * decays[low_bits + b] * bits[b]
            if b > 0:
                real = real - couplings[low_bits + b - 1] * signs[b - 1] * signs[b]
        edge = couplings[low_bits - 1] * signs[0]
        return real - edge, real + edge, imag

    def start_norm(i, acc):
        node = i // per_block
        first = (i % per_block) * CHUNK
        for part in range(2):
            x = state[node, part, pl.ds(first, CHUNK), :]
            acc = acc + fold(x * x)
        return acc

    start_sq = jnp.sum(lax.fori_loop(0, chunks, start_norm, zero_tile))
    beta, inv_beta = scalar_sqrt(start_sq)

    def start_vector(i, carry):
        node = i // per_block
        first = (i % per_block) * CHUNK
        for part in range(2):
            basis[0, pl.ds(i * CHUNK, CHUNK), part * LANES : (part + 1) * LANES] = (
                state[node, part, pl.ds(first, CHUNK), :] * inv_beta
            )
        return carry

    lax.fori_loop(0, chunks, start_vector, 0)

    mat_rows = lax.broadcasted_iota(jnp.int32, (2 * KRYLOV, LANES), 0)
    mat_cols = lax.broadcasted_iota(jnp.int32, (2 * KRYLOV, LANES), 1)
    a_matrix = jnp.zeros((2 * KRYLOV, LANES), jnp.float32)

    def put(matrix, k, j, real, imag):
        a_real = time_step * imag
        a_imag = -time_step * real
        for r, c, value in (
            (k, j, a_real),
            (k, j + KRYLOV, -a_imag),
            (k + KRYLOV, j, a_imag),
            (k + KRYLOV, j + KRYLOV, a_real),
        ):
            matrix = jnp.where((mat_rows == r) & (mat_cols == c), value, matrix)
        return matrix

    high_fields = [
        fields[LANE_BITS + CHUNK_BITS + b] for b in range(SPINS - LANE_BITS - CHUNK_BITS)
    ]

    for j in range(KRYLOV):
        last = j + 1 == KRYLOV

        def apply_chunk(i, acc, j=j):
            base = pl.multiple_of(i * CHUNK, CHUNK)
            hi, lo = split(basis[j, pl.ds(base, CHUNK), :])
            flips[...] = (
                dot(row_table[0], hi)
                + dot(row_table[1], hi)
                + dot(row_table[0], lo)
                + dot(hi, lane_table[0])
                + dot(lo, lane_table[0])
                + dot(hi, lane_table[1])
            )
            acc = list(acc)
            real_vacant, real_occupied, imag_high = high_diagonal(i)
            for s in range(subs):
                here = pl.ds(base + s * SUB, SUB)
                x = basis[j, here, :]
                f = flips[s * SUB : (s + 1) * SUB, :]
                for b, field in enumerate(high_fields):
                    there = pl.multiple_of((i ^ (1 << b)) * CHUNK, CHUNK)
                    f = f + field * basis[j, pl.ds(there + s * SUB, SUB), :]
                part = slice(s * SUB, (s + 1) * SUB)
                dr = diag_low[0, part, :] + (real_vacant if s < subs // 2 else real_occupied)
                di = diag_low[1, part, :] + imag_high
                xr, xi = x[:, :LANES], x[:, LANES:]
                wr = dr * xr - di * xi - f[:, :LANES]
                wi = dr * xi + di * xr - f[:, LANES:]
                work[here, :LANES] = wr
                work[here, LANES:] = wi
                for k in range(j + 1):
                    vr = basis[k, here, :LANES]
                    vi = basis[k, here, LANES:]
                    acc[2 * k] = acc[2 * k] + fold(vr * wr + vi * wi)
                    acc[2 * k + 1] = acc[2 * k + 1] + fold(vr * wi - vi * wr)
                acc[-1] = acc[-1] + fold(wr * wr + wi * wi)
            return tuple(acc)

        sums = lax.fori_loop(0, chunks, apply_chunk, (zero_tile,) * (2 * j + 3))
        coeffs = [jnp.sum(t) for t in sums]
        for k in range(j + 1):
            a_matrix = put(a_matrix, k, j, coeffs[2 * k], coeffs[2 * k + 1])
        if last:
            break
        left = coeffs[-1]
        for value in coeffs[:-1]:
            left = left - value * value
        norm, inv_norm = scalar_sqrt(left)
        a_matrix = put(a_matrix, j + 1, j, norm, jnp.float32(0.0))

        def subtract_chunk(i, carry, j=j, coeffs=coeffs, inv_norm=inv_norm):
            base = pl.multiple_of(i * CHUNK, CHUNK)
            for s in range(subs):
                here = pl.ds(base + s * SUB, SUB)
                rr = work[here, :LANES]
                ri = work[here, LANES:]
                for k in range(j + 1):
                    vr = basis[k, here, :LANES]
                    vi = basis[k, here, LANES:]
                    hr, hm = coeffs[2 * k], coeffs[2 * k + 1]
                    rr = rr - (hr * vr - hm * vi)
                    ri = ri - (hr * vi + hm * vr)
                basis[j + 1, here, :LANES] = rr * inv_norm
                basis[j + 1, here, LANES:] = ri * inv_norm
            return carry

        lax.fori_loop(0, chunks, subtract_chunk, 0)

    series = krylov_weights(a_matrix)
    first = series[: 2 * KRYLOV, :] * beta
    weights = [
        jnp.sum(jnp.where((mat_rows == k) & (mat_cols == 0), first, 0.0))
        for k in range(2 * KRYLOV)
    ]
    sub_pos = lax.broadcasted_iota(jnp.int32, (SUB, LANES), 0) * LANES
    sub_pos = sub_pos + lax.broadcasted_iota(jnp.int32, (SUB, LANES), 1)

    def combine(i, acc):
        base = pl.multiple_of(i * CHUNK, CHUNK)
        for s in range(subs):
            here = pl.ds(base + s * SUB, SUB)
            pr = jnp.zeros((SUB, LANES), jnp.float32)
            pi = jnp.zeros((SUB, LANES), jnp.float32)
            for k in range(KRYLOV):
                vr = basis[k, here, :LANES]
                vi = basis[k, here, LANES:]
                cr, ci = weights[k], weights[k + KRYLOV]
                pr = pr + (cr * vr - ci * vi)
                pi = pi + (cr * vi + ci * vr)
            work[here, :LANES] = pr
            work[here, LANES:] = pi
            position = sub_pos + (base + s * SUB) * LANES
            occupied = lax.shift_right_logical(position, channel) & 1
            acc = acc + fold(jnp.where(occupied == 1, pr * pr + pi * pi, 0.0))
        return acc

    total = jnp.sum(lax.fori_loop(0, chunks, combine, zero_tile))
    jumped = channel < SPINS
    size = jnp.float32(rows * LANES)
    total = jnp.where(jumped, total, size)
    root = jnp.sqrt(size / jnp.full((8, LANES), total, jnp.float32))
    scale = jnp.max(root)
    in_lanes = channel < LANE_BITS
    lane_shift = jnp.where(in_lanes, lax.shift_left(1, channel), 0)
    row_shift = jnp.where(
        in_lanes | (channel >= SPINS),
        0,
        lax.shift_left(1, jnp.maximum(channel - LANE_BITS, 0)),
    )
    in_sublanes = row_shift < 8
    near = jnp.where(in_sublanes, row_shift, 0)
    far = jnp.where(in_sublanes, 0, row_shift)
    lane_turn = (LANES - lane_shift) % LANES
    row_turn = (SUB - near) % SUB

    def jump(i, carry):
        local = pl.multiple_of(i * SUB, SUB)
        base = device * block_rows + local
        source = pl.multiple_of(base + far, 8)
        position = sub_pos + base * LANES
        vacant = (lax.shift_right_logical(position, channel) & 1) == 0
        for part in range(2):
            x = work[pl.ds(source, SUB), part * LANES : (part + 1) * LANES]
            x = pltpu.roll(x, row_turn, 0)
            x = pltpu.roll(x, lane_turn, 1)
            out[part, pl.ds(local, SUB), :] = jnp.where(vacant, x * scale, 0.0)
        return carry

    lax.fori_loop(0, block_rows // SUB, jump, 0)


def gather_kernel(block, out, send_sem, recv_sem):
    me = lax.axis_index("amp")
    near = (me ^ 1, me ^ 2)
    barrier = pltpu.get_barrier_semaphore()
    for partner in near:
        pl.semaphore_signal(
            barrier, inc=1, device_id={"amp": partner}, device_id_type=pl.DeviceIdType.MESH
        )
    pl.semaphore_wait(barrier, 2)

    def copy(source, owner, part, axis, slot):
        return pltpu.make_async_remote_copy(
            src_ref=source,
            dst_ref=out.at[owner, part],
            send_sem=send_sem.at[slot],
            recv_sem=recv_sem.at[slot],
            device_id={"amp": near[axis]},
            device_id_type=pl.DeviceIdType.MESH,
        )

    direct = {}
    for turn in range(2):
        for axis in range(2):
            part = axis ^ turn
            direct[axis, part] = copy(block.at[part], me, part, axis, 2 * axis + part)
            direct[axis, part].start()
    out[me] = block[...]
    forwards = []
    for axis in range(2):
        direct[axis, axis].wait_recv()
        owner = near[axis]
        forward = copy(out.at[owner, axis], owner, axis, 1 - axis, 4 + axis)
        forward.start()
        forwards.append(forward)
    for axis in range(2):
        direct[axis, 1 - axis].wait_recv()
    for forward in forwards:
        forward.wait_recv()
    for sent in list(direct.values()) + forwards:
        sent.wait_send()


def gather(block):
    node_count = lax.axis_size("amp")
    if node_count != 4:
        return lax.all_gather(block, "amp")
    vmem = pl.BlockSpec(memory_space=pltpu.VMEM)
    return pl.pallas_call(
        gather_kernel,
        out_shape=jax.ShapeDtypeStruct((node_count,) + block.shape, block.dtype),
        in_specs=[vmem],
        out_specs=vmem,
        scratch_shapes=[pltpu.SemaphoreType.DMA((6,)), pltpu.SemaphoreType.DMA((6,))],
        compiler_params=pltpu.CompilerParams(collective_id=0, has_side_effects=True),
        name="gather",
    )(block)


def body(amplitudes, couplings, fields, decays, channel):
    node_count = lax.axis_size("amp")
    local_len = amplitudes.shape[2]
    block_rows = local_len // LANES
    rows = node_count * block_rows
    vmem = pl.BlockSpec(memory_space=pltpu.VMEM)
    smem = pl.BlockSpec(memory_space=pltpu.SMEM)
    call = pl.pallas_call(
        kernel,
        out_shape=jax.ShapeDtypeStruct((2, block_rows, LANES), jnp.float32),
        in_specs=[smem] * 4 + [vmem],
        out_specs=vmem,
        scratch_shapes=[
            pltpu.VMEM((KRYLOV, rows, 2 * LANES), jnp.float32),
            pltpu.VMEM((rows + rows // 2, 2 * LANES), jnp.float32),
            pltpu.VMEM((CHUNK, 2 * LANES), jnp.float32),
            pltpu.VMEM((2, CHUNK, CHUNK), jnp.bfloat16),
            pltpu.VMEM((2, CHUNK, CHUNK), jnp.bfloat16),
            pltpu.VMEM((2, CHUNK, LANES), jnp.float32),
        ],
        compiler_params=pltpu.CompilerParams(vmem_limit_bytes=62 * 1024 * 1024),
        name="trajectory",
    )
    results = []
    for t in range(amplitudes.shape[0]):
        block = amplitudes[t].reshape(2, block_rows, LANES)
        state = gather(block)
        results.append(call(channel[t : t + 1], couplings, fields, decays, state))
    return jnp.stack(results).reshape(amplitudes.shape)


BLOCK = 256
BLOCK_BITS = 8
TILE = 16


def pair_kernel(
    channel_ref,
    couplings,
    fields,
    decays,
    block,
    pieces,
    scale_out,
    landing,
    mate_landing,
    basis,
    mate,
    work,
    mate_work,
    flips,
    splits,
    row_table,
    lane_table,
    diagonal,
    own_sums,
    other_sums,
    own_rest,
    other_rest,
    scalars,
    own_channel,
    other_channel,
    parcel,
    gather_send,
    gather_recv,
    forward_send,
    forward_recv,
    sums_send,
    sums_recv,
    rest_sem,
    work_send,
    work_recv,
    channel_sem,
    parcel_send,
    parcel_recv,
    scale_sem,
):
    quarters = landing.shape[0]
    piece_rows = landing.shape[1]
    traj = lax.axis_index("traj")
    me = lax.axis_index("amp")
    core = traj & 1
    first_traj = traj - core
    held = (me ^ (me >> 1)) & 1
    stays = core == held
    split_spin = LANE_BITS + BLOCK_BITS + 1
    side_spin = split_spin - 1
    zero_tile = jnp.zeros((8, LANES), jnp.float32)
    tiles = [(s, side) for s in range(BLOCK // TILE) for side in range(2)]
    half = BLOCK // 2

    def device(core_index, chip):
        return {"traj": first_traj + core_index, "amp": chip}

    def remote(source, target, send, recv, where):
        return pltpu.make_async_remote_copy(
            src_ref=source,
            dst_ref=target,
            send_sem=send,
            recv_sem=recv,
            device_id=where,
            device_id_type=pl.DeviceIdType.MESH,
        )

    other = device(1 - core, me)
    barrier = pltpu.get_barrier_semaphore()
    for flip_core in range(2):
        for flip_chip in range(quarters):
            if flip_core or flip_chip:
                pl.semaphore_signal(
                    barrier,
                    inc=1,
                    device_id=device(core ^ flip_core, me ^ flip_chip),
                    device_id_type=pl.DeviceIdType.MESH,
                )
    own_channel[...] = jnp.full(own_channel.shape, channel_ref[0], jnp.int32)
    pl.semaphore_wait(barrier, 2 * quarters - 1)

    near_chip = me ^ (held ^ core)
    far_chip = near_chip ^ 3

    def piece(core_index, chip, slot):
        source = block.at[pl.ds(pl.multiple_of(core_index * piece_rows, piece_rows), piece_rows)]
        return remote(
            source,
            landing.at[me],
            gather_send.at[slot],
            gather_recv.at[me],
            device(core_index, chip),
        )

    sends = [piece(core, far_chip, 0), piece(1 - core, far_chip, 1), piece(1 - core, near_chip, 2)]
    for send in sends:
        send.start()

    @pl.when(jnp.logical_not(stays))
    def _():
        piece(core, near_chip, 3).start()

    channel_copy = remote(
        own_channel, other_channel, channel_sem.at[0], channel_sem.at[1], other
    )
    channel_copy.start()

    unit = fields[split_spin]
    inv_unit = jnp.max(1.0 / jnp.full((8, LANES), unit, jnp.float32))
    crossed = lax.broadcasted_iota(jnp.int32, (BLOCK, BLOCK), 0)
    crossed = crossed ^ lax.broadcasted_iota(jnp.int32, (BLOCK, BLOCK), 1)
    for table, spins, axis in (
        (row_table, [LANE_BITS + b for b in range(BLOCK_BITS)], 1),
        (lane_table, [*range(LANE_BITS), side_spin], 0),
    ):
        value = jnp.zeros((BLOCK, BLOCK), jnp.float32)
        for bit, spin in enumerate(spins):
            value = jnp.where(crossed == 1 << bit, fields[spin] * inv_unit, value)
        hi, lo = split(value)
        table[...] = jnp.concatenate([hi, hi, lo], axis=axis)

    core_bit = core.astype(jnp.float32)
    core_sign = 1.0 - 2.0 * core_bit
    bond = [couplings[spin] * inv_unit for spin in range(SPINS - 1)]
    loss = [0.5 * decays[spin] * inv_unit for spin in range(SPINS)]
    for side in range(2):
        low_shape = (BLOCK, LANES)
        low_pos = lax.broadcasted_iota(jnp.int32, low_shape, 0) * LANES
        low_pos = low_pos + lax.broadcasted_iota(jnp.int32, low_shape, 1)
        side_sign = 1.0 - 2.0 * side
        low_real = jnp.zeros(low_shape, jnp.float32)
        low_imag = jnp.zeros(low_shape, jnp.float32)
        before = None
        for spin in range(side_spin):
            occupied = (lax.shift_right_logical(low_pos, spin) & 1).astype(jnp.float32)
            sign = 1.0 - 2.0 * occupied
            low_imag = low_imag - loss[spin] * occupied
            if spin > 0:
                low_real = low_real - bond[spin - 1] * (before * sign)
            before = sign
        low_real = low_real - bond[side_spin - 1] * side_sign * before
        low_real = low_real - bond[side_spin] * side_sign * core_sign
        low_imag = low_imag - side * loss[side_spin] - core_bit * loss[split_spin]
        for q in range(quarters):
            bits = [(q >> b) & 1 for b in range(SPINS - 1 - split_spin)]
            signs = [core_sign] + [1.0 - 2.0 * bit for bit in bits]
            real, imag = low_real, low_imag
            for b, bit in enumerate(bits):
                real = real - bond[split_spin + b] * (signs[b] * signs[b + 1])
                imag = imag - bit * loss[split_spin + 1 + b]
            diagonal[q, 0, side] = real
            diagonal[q, 1, side] = imag

    def window(ref, lead, part, s, side):
        return ref.at[(*lead, part, pl.ds(s * TILE, TILE), pl.ds(side * LANES, LANES))]

    def sums_copy(count, slot):
        return remote(
            own_sums.at[slot, pl.ds(0, 8 * count)],
            other_sums.at[slot, pl.ds(0, 8 * count)],
            sums_send.at[slot],
            sums_recv.at[slot],
            other,
        )

    def start_sums(values, slot):
        for k, value in enumerate(values):
            own_sums[slot, 8 * k : 8 * k + 8] = value
        sums_copy(len(values), slot).start()

    def finish_sums(count, slot):
        sums_copy(count, slot).wait()
        both = [ref[slot, : 8 * count] for ref in (own_sums, other_sums)]
        both = both[0] + both[1]
        return [jnp.sum(both[8 * k : 8 * k + 8]) for k in range(count)]

    def work_copy(slot, n):
        pair = (pl.ds(2 * (n // 2), 2), slice(None), pl.ds(n % 2 * half, half))
        return remote(
            work.at[(slot, *pair)],
            mate_work.at[(slot, *pair)],
            work_send.at[slot, n],
            work_recv.at[slot, n],
            other,
        )

    @pl.when(stays)
    def _():
        def keep(i, carry):
            rows = pl.multiple_of(i * SUB, SUB)
            landing[me, pl.ds(rows, SUB), :] = block[
                pl.ds(pl.multiple_of(core * piece_rows, piece_rows) + rows, SUB), :
            ]
            return carry

        lax.fori_loop(0, piece_rows // SUB, keep, 0)

    mate[1, pl.ds(2, 2)] = jnp.zeros((2, 2, BLOCK, BLOCK), jnp.float32)

    def arrival(chip):
        return remote(
            block.at[pl.ds(0, piece_rows)],
            landing.at[chip],
            gather_send.at[0],
            gather_recv.at[chip],
            other,
        )

    def forward(chip):
        return remote(
            landing.at[chip],
            mate_landing.at[chip],
            forward_send.at[chip],
            forward_recv.at[chip],
            other,
        )

    @pl.when(jnp.logical_not(stays))
    def _():
        arrival(me).wait_recv()

    def square(ref, q, acc):
        def add(i, acc):
            x = ref[q, pl.ds(pl.multiple_of(i * 128, 128), 128), :]
            return acc + fold(x * x)

        return lax.fori_loop(0, piece_rows // 128, add, acc)

    own_sq = zero_tile
    for flip_chip in range(quarters):
        q = me ^ flip_chip
        if flip_chip:
            arrival(q).wait_recv()
        forward(q).start()
        own_sq = square(landing, q, own_sq)
    mate_sq = zero_tile
    for flip_chip in range(quarters):
        q = me ^ flip_chip
        forward(q).wait()
        mate_sq = square(mate_landing, q, mate_sq)
    beta, inv_beta = scalar_sqrt(jnp.sum(own_sq + mate_sq))

    def put_split(q, part, s, side, x):
        for n, term in enumerate(split(x)):
            window(splits, (q, part), n, s, side)[...] = term

    def start_vector(q, carry):
        for s, side in tiles:
            for part in range(2):
                rows = pl.ds((side * BLOCK + s * TILE) * 2 + part, TILE, stride=2)
                x = landing[q, rows, :] * inv_beta
                window(basis, (0, q), part, s, side)[...] = x
                put_split(q, part, s, side, x)
                window(mate, (0, q), part, s, side)[...] = mate_landing[q, rows, :] * inv_beta
        return carry

    lax.fori_loop(0, quarters, start_vector, 0)

    high_fields = [fields[split_spin + 1 + b] * inv_unit for b in range(SPINS - 1 - split_spin)]

    def issue(q, part):
        hi, lo = splits[q, part, 0], splits[q, part, 1]
        flips[q, part] = dot(
            jnp.concatenate([row_table[...], hi, lo, hi], axis=1),
            jnp.concatenate([hi, lo, hi, lane_table[...]], axis=0),
        )

    def pairing(v, w):
        return fold(v[0] * w[0] + v[1] * w[1]), fold(v[0] * w[1] - v[1] * w[0])

    def load(ref, lead, s, side):
        return [window(ref, lead, part, s, side)[...] for part in range(2)]

    def consume(j, slot, pair, acc, before, norm, h, between=()):
        count = len(tiles) // 2
        for t, (s, side) in enumerate(tiles[h * count : (h + 1) * count]):
            if t % 8 == 0 and between:
                issue(*between[t // 8])
            chosen = (2 * pair, 2 * pair + 1)
            x = [load(basis, (j, q), s, side) for q in chosen]
            for n, q in enumerate(chosen):
                made = load(flips, (q,), s, side)
                near = load(mate, (slot, q), s, side)
                cross = load(basis, (j, q ^ 2), s, side)
                f = [
                    made[part]
                    + near[part]
                    + high_fields[0] * x[1 - n][part]
                    + high_fields[1] * cross[part]
                    for part in range(2)
                ]
                dr = window(diagonal, (q, 0), side, s, 0)[...]
                di = window(diagonal, (q, 1), side, s, 0)[...]
                xr, xi = x[n]
                w = (dr * xr - di * xi - f[0], dr * xi + di * xr - f[1])
                more = pairing(x[n], w)
                if before:
                    more = more + pairing(load(basis, (j - 1, q), s, side), w)
                if norm:
                    more = more + (fold(w[0] * w[0] + w[1] * w[1]),)
                for m, value in enumerate(more):
                    acc[m] = acc[m] + value
                for part in range(2):
                    window(work, (slot, q), part, s, side)[...] = w[part]

    def take(q, w_ref, u_ref, slot, now, before, after, coeffs, inverse, both, own, between=()):
        group = 4
        leads = [now, before] if both else [now]
        for t in range(0, len(tiles), group):
            if t % 16 == 0 and between:
                issue(*between[t // 16])
            made = []
            for s, side in tiles[t : t + group]:
                rr, ri = load(w_ref, (slot, q), s, side)
                vs = [load(u_ref, (lead, q), s, side) for lead in leads]
                made.append((rr, ri, vs))
            for (s, side), (rr, ri, vs) in zip(tiles[t : t + group], made):
                for n, (vr, vi) in enumerate(vs):
                    hr, hm = coeffs[2 * n], coeffs[2 * n + 1]
                    rr = rr - (hr * vr - hm * vi)
                    ri = ri - (hr * vi + hm * vr)
                for part, value in enumerate((rr * inverse, ri * inverse)):
                    window(u_ref, (after, q), part, s, side)[...] = value
                    if own:
                        put_split(q, part, s, side, value)

    def apply(j, slot, first, last):
        acc = [zero_tile] * (2 + 2 * (not first) + (not last))
        middle = None
        if not first:
            known = [scalars[j - 1, n] for n in range(6)]

            def middle(q):
                take(
                    q, mate_work, mate, 1 - slot, 1 - slot, slot, slot, known[:4], known[5],
                    True, False,
                )

        for h in range(2):
            products = [(2 + h, part) for part in range(2)]
            consume(j, slot, 0, acc, not first, not last, h, products)
            if not last:
                work_copy(slot, h).start()
        if middle:
            for n in range(2, 4):
                work_copy(1 - slot, n).wait()
            middle(2)
            middle(3)
        for h in range(2):
            consume(j, slot, 1, acc, not first, not last, h)
        return acc

    def rest_inner(j, slot, count):

        def one(k, carry):
            def add(q, acc):
                real, imag = acc
                for s, side in tiles:
                    v = load(basis, (k, q), s, side)
                    w = load(work, (slot, q), s, side)
                    more = pairing(v, w)
                    real, imag = real + more[0], imag + more[1]
                return real, imag

            real, imag = lax.fori_loop(0, quarters, add, (zero_tile, zero_tile))
            own_rest[j, k, 0] = real
            own_rest[j, k, 1] = imag
            return carry

        lax.fori_loop(0, count, one, 0)

    def step(j, slot, first):
        sums = apply(j, slot, first, False)
        start_sums(sums, slot)
        for n in range(2, 4):
            work_copy(slot, n).start()
        if not first:
            rest_inner(j, slot, j - 1)
        coeffs = finish_sums(len(sums), slot)
        left = coeffs[-1]
        for value in coeffs[:-1]:
            left = left - value * value
        norm, inv_norm = scalar_sqrt(left)
        for n in range(4):
            scalars[j, n] = coeffs[n] if n < len(coeffs) - 1 else jnp.float32(0.0)
        scalars[j, 4] = norm
        scalars[j, 5] = inv_norm
        for q in range(quarters):
            if q == 2:
                for n in range(2):
                    work_copy(slot, n).wait()
            between = [(q - 2, part) for part in range(2)] if q > 1 else ()
            take(
                q, work, basis, slot, j, j - 1, j + 1, coeffs, inv_norm, not first, True, between
            )
        for q in range(2):
            take(
                q, mate_work, mate, slot, slot, 1 - slot, 1 - slot, coeffs, inv_norm,
                not first, False,
            )

    final = KRYLOV - 1
    for q in range(2):
        for part in range(2):
            issue(q, part)
    step(0, 0, True)

    def later(i, carry):
        step(2 * i + 1, 1, False)
        step(2 * i + 2, 0, False)
        return carry

    lax.fori_loop(0, final // 2, later, 0)
    rest_copy = remote(
        own_rest.at[pl.ds(0, final)],
        other_rest.at[pl.ds(0, final)],
        rest_sem.at[0],
        rest_sem.at[1],
        other,
    )
    last_copy = remote(
        own_rest.at[final], other_rest.at[final], rest_sem.at[2], rest_sem.at[3], other
    )
    rest_copy.start()
    start_sums(apply(final, final % 2, False, True), final % 2)
    rest_inner(final, final % 2, final - 1)
    last_copy.start()
    rest_copy.wait()
    sub = lax.broadcasted_iota(jnp.int32, (8, LANES), 0)
    lane = lax.broadcasted_iota(jnp.int32, (8, LANES), 1)

    def put(tile, where, value):
        return jnp.where(where, value, tile)

    gram = [jnp.where(sub == lane, 1.0, 0.0).astype(jnp.float32), zero_tile]
    projected = [zero_tile, zero_tile]
    column = {j: [zero_tile, zero_tile] for j in range(3)}
    across = {j: [zero_tile, zero_tile] for j in range(3)}
    for j in range(final):
        here = lane == j
        alpha = [scalars[j, 0], scalars[j, 1]]
        bravo = [scalars[j, 2], scalars[j, 3]]
        for part in range(2):
            projected[part] = put(projected[part], here & (sub == j), alpha[part])
            if j > 0:
                projected[part] = put(projected[part], here & (sub == j - 1), bravo[part])
        projected[0] = put(projected[0], here & (sub == j + 1), scalars[j, 4])
        if j < 2:
            continue
        down = [zero_tile, zero_tile]
        along = [zero_tile, zero_tile]
        for k in range(j - 1):
            for part in range(2):
                value = jnp.sum(own_rest[j, k, part] + other_rest[j, k, part])
                down[part] = put(down[part], sub == k, value)
                along[part] = put(along[part], lane == k, value)
        for made, new in ((column, down), (across, along)):
            for value, old in ((alpha, made[j]), (bravo, made[j - 1])):
                new[0] = new[0] - (value[0] * old[0] - value[1] * old[1])
                new[1] = new[1] - (value[0] * old[1] + value[1] * old[0])
            made[j + 1] = [part * scalars[j, 5] for part in new]
        gram[0] = gram[0] + jnp.where(lane == j + 1, column[j + 1][0], 0.0)
        gram[0] = gram[0] + jnp.where(sub == j + 1, across[j + 1][0], 0.0)
        gram[1] = gram[1] + jnp.where(lane == j + 1, column[j + 1][1], 0.0)
        gram[1] = gram[1] - jnp.where(sub == j + 1, across[j + 1][1], 0.0)

    near_targets = finish_sums(4, final % 2)
    last_copy.wait()
    targets = []
    for k in range(final - 1):
        for part in range(2):
            targets.append(jnp.sum(own_rest[final, k, part] + other_rest[final, k, part]))
    targets = targets + near_targets[2:4] + near_targets[:2]
    for k in range(KRYLOV):
        for part in range(2):
            gram[part] = put(gram[part], (lane == KRYLOV) & (sub == k), targets[2 * k + part])

    def column_of(tile, k):
        return jnp.broadcast_to(tile[:, k : k + 1], tile.shape)

    def row_of(tile, k):
        return jnp.broadcast_to(tile[k : k + 1, :], tile.shape)

    for p in range(KRYLOV):
        row = [row_of(tile, p) for tile in gram]
        factor = [column_of(tile, p) for tile in gram]
        inverse = 1.0 / row_of(factor[0], p)
        row = [tile * inverse for tile in row]
        less = (
            factor[0] * row[0] - factor[1] * row[1],
            factor[0] * row[1] + factor[1] * row[0],
        )
        gram = [jnp.where(sub == p, row[n], gram[n] - less[n]) for n in range(2)]
    for part in range(2):
        projected[part] = put(projected[part], lane == final, column_of(gram[part], KRYLOV))

    def product(a, b):
        real, imag = zero_tile, zero_tile
        for k in range(KRYLOV):
            ar, ai = column_of(a[0], k), column_of(a[1], k)
            br, bi = row_of(b[0], k), row_of(b[1], k)
            real = real + (ar * br - ai * bi)
            imag = imag + (ar * bi + ai * br)
        return real, imag

    inside = lane < KRYLOV
    pace = unit * (time_step / 2.0**squarings)
    first = (
        jnp.where(inside, projected[1] * pace, 0.0),
        jnp.where(inside, projected[0] * -pace, 0.0),
    )
    second = product(first, first)
    third = product(second, first)
    identity = jnp.where(sub == lane, 1.0, 0.0).astype(jnp.float32)
    series = None
    for low in range(taylor_order // 3 * 3, -1, -3):
        terms = [identity * (1.0 / math.factorial(low)), zero_tile]
        for n, power in ((low + 1, first), (low + 2, second)):
            if n <= taylor_order:
                terms = [t + p * (1.0 / math.factorial(n)) for t, p in zip(terms, power)]
        if series is not None:
            terms = [t + p for t, p in zip(terms, product(third, series))]
        series = terms
    for repeat in range(squarings):
        series = product(series, series)
    weights = [
        jnp.sum(jnp.where((sub == k) & (lane == 0), tile * beta, 0.0))
        for tile in series
        for k in range(KRYLOV)
    ]
    channel_copy.wait()
    channel = jnp.where(stays, own_channel[...], other_channel[...])
    sub_pos = lax.broadcasted_iota(jnp.int32, (TILE, LANES), 0) * LANES
    sub_pos = sub_pos + lax.broadcasted_iota(jnp.int32, (TILE, LANES), 1)

    def combine(q, acc):
        high = (core << split_spin) + (q << (split_spin + 1))
        for s, side in tiles:
            pr = jnp.zeros((TILE, LANES), jnp.float32)
            pi = jnp.zeros((TILE, LANES), jnp.float32)
            for k in range(KRYLOV):
                vr = window(basis, (k, q), 0, s, side)[...]
                vi = window(basis, (k, q), 1, s, side)[...]
                cr, ci = weights[k], weights[k + KRYLOV]
                pr = pr + (cr * vr - ci * vi)
                pi = pi + (cr * vi + ci * vr)
            window(work, (0, q), 0, s, side)[...] = pr
            window(work, (0, q), 1, s, side)[...] = pi
            position = sub_pos + (high + (side << side_spin) + s * TILE * LANES)
            occupied = lax.shift_right_logical(position, channel) & 1
            acc = acc + fold(jnp.where(occupied == 1, pr * pr + pi * pi, 0.0))
        return acc

    jumped_sq = lax.fori_loop(0, quarters, combine, zero_tile)

    start_sums([jumped_sq], 0)

    def pack(target, q, part):
        for s, side in tiles:
            value = window(work, (0, q), part, s, side)[...]
            for b in range(SPINS - 1 - split_spin):
                flipped = window(work, (0, q | (1 << b)), part, s, side)[...]
                value = jnp.where(channel == split_spin + 1 + b, flipped, value)
            target[s * TILE : (s + 1) * TILE, side * LANES : (side + 1) * LANES] = value

    parcels = []
    for part in range(2):
        q = me ^ (1 << part)
        pack(parcel.at[part], q, part)
        copy = remote(
            parcel.at[part],
            pieces.at[core, part],
            parcel_send.at[part],
            parcel_recv.at[core, part],
            device(held, q),
        )
        copy.start()
        parcels.append(copy)
    for part in range(2):
        pack(parcel.at[2 + part], me, part)
    home = remote(
        parcel.at[pl.ds(2, 2)], pieces.at[core], parcel_send.at[2], parcel_recv.at[2, 0], other
    )

    @pl.when(jnp.logical_not(stays))
    def _():
        home.start()

    @pl.when(stays)
    def _():
        for part in range(2):
            pieces[core, part] = parcel[2 + part]

    all_sq = finish_sums(1, 0)[0]
    size = jnp.float32(quarters * 2 * piece_rows // 2 * LANES)
    ratio = jnp.where(channel[:8] < SPINS, size / jnp.full((8, LANES), all_sq, jnp.float32), 1.0)
    own_scale = jnp.sqrt(ratio)
    own_sums[1, 0:8] = own_scale
    scale_copy = remote(
        own_sums.at[1, pl.ds(0, 8)], scale_out, scale_sem.at[0], scale_sem.at[1],
        device(core, me ^ 1),
    )

    @pl.when(stays)
    def _():
        scale_copy.start()
        scale_out[...] = own_scale
        remote(
            parcel.at[pl.ds(2, 2)], pieces.at[1 - core], parcel_send.at[2],
            parcel_recv.at[2, 0], other,
        ).wait_recv()
        scale_copy.wait_send()

    @pl.when(jnp.logical_not(stays))
    def _():
        for sender in range(2):
            for part in range(2):
                remote(
                    parcel.at[part], pieces.at[sender, part], parcel_send.at[part],
                    parcel_recv.at[sender, part], other,
                ).wait_recv()
        scale_copy.wait_recv()
        home.wait_send()
        piece(core, near_chip, 3).wait_send()

    for copy in parcels:
        copy.wait_send()
    for send in sends:
        send.wait_send()


def lower_kernel(channel_ref, pieces, scale, out):
    channel = channel_ref[0]
    me = lax.axis_index("amp")
    side_spin = LANE_BITS + BLOCK_BITS
    in_lanes = channel < LANE_BITS
    in_rows = jnp.logical_not(in_lanes) & (channel < side_spin)
    lane_shift = jnp.where(in_lanes, lax.shift_left(1, channel), 0)
    row_shift = jnp.where(in_rows, lax.shift_left(1, jnp.maximum(channel - LANE_BITS, 0)), 0)
    near = jnp.where(row_shift < 8, row_shift, 0)
    far = jnp.where(row_shift < 8, 0, row_shift)
    lane_turn = (LANES - lane_shift) % LANES
    row_turn = (8 - near) % 8
    sub_pos = lax.broadcasted_iota(jnp.int32, (8, LANES), 0) * LANES
    sub_pos = sub_pos + lax.broadcasted_iota(jnp.int32, (8, LANES), 1)
    own = me * (4 * BLOCK * LANES)
    factor = scale[...]

    for half in range(2):
        from_half = jnp.where(channel == side_spin + 1, 1, half)
        for side in range(2):
            from_side = jnp.where(channel == side_spin, 1, side)
            columns = pl.ds(pl.multiple_of(from_side * LANES, LANES), LANES)

            def lower(i, carry, half=half, side=side, from_half=from_half, columns=columns):
                for t in range(8):
                    local = i * 64 + t * 8
                    base = (half * 2 + side) * BLOCK + local
                    rows = pl.ds(pl.multiple_of(local | far, 8), 8)
                    position = sub_pos + (own + base * LANES)
                    vacant = (lax.shift_right_logical(position, channel) & 1) == 0
                    for part in range(2):
                        x = pieces[from_half, part, rows, columns]
                        x = pltpu.roll(x, row_turn, 0)
                        x = pltpu.roll(x, lane_turn, 1)
                        x = jnp.where(vacant, x * factor, 0.0)
                        out[pl.ds(base * 2 + part, 8, stride=2), :] = x
                return carry

            lax.fori_loop(0, BLOCK // 64, lower, 0)


def paired_body(amplitudes, couplings, fields, decays, channel):
    quarters = lax.axis_size("amp")
    local_len = amplitudes.shape[2]
    block_rows = local_len // LANES
    vmem = pl.BlockSpec(memory_space=pltpu.VMEM)
    smem = pl.BlockSpec(memory_space=pltpu.SMEM)
    f32 = jnp.float32
    dma = pltpu.SemaphoreType.DMA
    sums_rows = 8 * (2 * KRYLOV + 1)
    state = amplitudes.reshape(2, block_rows, LANES).transpose(1, 0, 2)
    state = state.reshape(2 * block_rows, LANES)
    pieces, scale = pl.pallas_call(
        pair_kernel,
        out_shape=(
            jax.ShapeDtypeStruct((2, 2, BLOCK, BLOCK), f32),
            jax.ShapeDtypeStruct((8, LANES), f32),
        ),
        in_specs=[smem] * 4 + [vmem],
        out_specs=(vmem, vmem),
        scratch_shapes=[
            pltpu.VMEM((quarters, block_rows, LANES), f32),
            pltpu.VMEM((quarters, block_rows, LANES), f32),
            pltpu.VMEM((KRYLOV, quarters, 2, BLOCK, BLOCK), f32),
            pltpu.VMEM((2, quarters, 2, BLOCK, BLOCK), f32),
            pltpu.VMEM((2, quarters, 2, BLOCK, BLOCK), f32),
            pltpu.VMEM((2, quarters, 2, BLOCK, BLOCK), f32),
            pltpu.VMEM((quarters, 2, BLOCK, BLOCK), f32),
            pltpu.VMEM((quarters, 2, 2, BLOCK, BLOCK), jnp.bfloat16),
            pltpu.VMEM((BLOCK, 3 * BLOCK), jnp.bfloat16),
            pltpu.VMEM((3 * BLOCK, BLOCK), jnp.bfloat16),
            pltpu.VMEM((quarters, 2, 2, BLOCK, LANES), f32),
            pltpu.VMEM((2, sums_rows, LANES), f32),
            pltpu.VMEM((2, sums_rows, LANES), f32),
            pltpu.VMEM((KRYLOV, KRYLOV - 2, 2, 8, LANES), f32),
            pltpu.VMEM((KRYLOV, KRYLOV - 2, 2, 8, LANES), f32),
            pltpu.SMEM((KRYLOV - 1, 6), f32),
            pltpu.VMEM((TILE, LANES), jnp.int32),
            pltpu.VMEM((TILE, LANES), jnp.int32),
            pltpu.VMEM((4, BLOCK, BLOCK), f32),
            dma((4,)),
            dma((quarters,)),
            dma((quarters,)),
            dma((quarters,)),
            dma((2,)),
            dma((2,)),
            dma((4,)),
            dma((2, quarters)),
            dma((2, quarters)),
            dma((2,)),
            dma((3,)),
            dma((3, 2)),
            dma((2,)),
        ],
        compiler_params=pltpu.CompilerParams(
            collective_id=1, has_side_effects=True, vmem_limit_bytes=48 * 1024 * 1024
        ),
        name="pair",
    )(channel, couplings, fields, decays, state)
    lowered = pl.pallas_call(
        lower_kernel,
        out_shape=jax.ShapeDtypeStruct((2 * block_rows, LANES), f32),
        in_specs=[smem, vmem, vmem],
        out_specs=vmem,
        compiler_params=pltpu.CompilerParams(vmem_limit_bytes=8 * 1024 * 1024),
        name="lower",
    )(channel, pieces, scale)
    lowered = lowered.reshape(block_rows, 2, LANES).transpose(1, 0, 2)
    return lowered.reshape(amplitudes.shape)


def solution(mesh):
    placed = (P("traj", None, "amp"), P(), P(), P(), P("traj"))

    def step(amplitudes, *rest):
        trajectories = mesh.shape["traj"]
        low_rows = amplitudes.shape[2] // mesh.shape["amp"] // LANES
        paired = (
            mesh.shape["amp"] == 4
            and trajectories % 2 == 0
            and amplitudes.shape[0] == trajectories
            and low_rows == 4 * BLOCK
        )
        return jax.shard_map(
            paired_body if paired else body,
            mesh=mesh,
            in_specs=placed,
            out_specs=P("traj", None, "amp"),
            check_vma=False,
        )(amplitudes, *rest)

    return step
```
